32 devices in a mesh: dp: 8 (over z, x), tensor: 4 (over y, core).
Axes of the slice: x: 2, y: 2, z: 4, core: 2. Of those that a mesh axis runs over, the one named last changes fastest.
Arguments:
- inputs: bfloat16 [8, 1024, 512], P('dp', 'tensor'), may hold values from -18 to 18, as said below
- lengths: int32 [8], P('dp'), may hold values from 256 to 1024
- cotangent: bfloat16 [8, 1024, 512], P('dp', 'tensor'), may hold values from -6 to 6
- ln_gains: float32 [2, 2, 512], replicated, may hold values from 0.5 to 1.5
- ln_biases: float32 [2, 2, 512], replicated, may hold values from -0.5 to 0.5
- w_query: bfloat16 [2, 512, 512], P(None, None, 'tensor'), may hold values from -0.25 to 0.25
- w_key: bfloat16 [2, 512, 512], P(None, None, 'tensor'), may hold values from -0.25 to 0.25
- w_value: bfloat16 [2, 512, 512], P(None, None, 'tensor'), may hold values from -0.25 to 0.25
- w_output: bfloat16 [2, 512, 512], P(None, 'tensor'), may hold values from -1.5 to 1.5
- w_in: bfloat16 [2, 512, 2048], P(None, None, 'tensor'), may hold values from -0.25 to 0.25
- b_in: bfloat16 [2, 2048], P(None, 'tensor'), may hold values from -1.5 to 1.5
- w_out: bfloat16 [2, 2048, 512], P(None, 'tensor'), may hold values from -0.125 to 0.125
- b_out: float32 [2, 512], replicated, may hold values from -1.5 to 1.5
Outputs:
- outputs: float32 [8, 1024, 512], P('dp', 'tensor')
- input_grad: float32 [8, 1024, 512], P('dp', 'tensor')
- grad_ln_gains: float32 [2, 2, 512], replicated
- grad_ln_biases: float32 [2, 2, 512], replicated
- grad_w_query: float32 [2, 512, 512], P(None, None, 'tensor')
- grad_w_key: float32 [2, 512, 512], P(None, None, 'tensor')
- grad_w_value: float32 [2, 512, 512], P(None, None, 'tensor')
- grad_w_output: float32 [2, 512, 512], P(None, 'tensor')
- grad_w_in: float32 [2, 512, 2048], P(None, None, 'tensor')
- grad_b_in: float32 [2, 2048], P(None, 'tensor')
- grad_w_out: float32 [2, 2048, 512], P(None, 'tensor')
- grad_b_out: float32 [2, 512], replicated
- norms: float32 [6], replicated
The draws below stay inside these ranges and needn't reach their ends.
Inputs may be any that keep to these rules, and one draw needn't show every extreme that they name: The first lengths[s] positions of sequence s are valid, the rest padding. `inputs`: the block's input.
All inputs are finite; a program needn't handle non-finite values.
Results may differ from the reference program's by a relative error of at most 0.023.
Values may be sent and summed in bfloat16 or wider, within the bound.
No kernel may reach another device: no remote copies, remote signals or barrier semaphores. Data moves between devices by JAX's collectives and lax.ppermute only.
A program may use at most 192 MiB of HBM per device.

```python
import math
import jax
import jax.numpy as jnp
import numpy as np
from jax import lax

D = 512
HEADS = 8
HEAD_DIM = 64
FF = 2048
BLOCK = 16
LEVELS = 5
LAYERS = 2
SEQ_LEN = 1024
SEQS = 8


def draw_inputs(key, part):
    ordinal = jnp.arange(SEQS, dtype=jnp.float32) / max(SEQS - 1, 1)
    scaling = 1.0 + 2.0 * ordinal
    baseline = jax.random.truncated_normal(key, -6.0, 6.0, (SEQS, SEQ_LEN, D), jnp.float32)
    return (baseline * scaling[:, None, None]).astype(jnp.bfloat16)


def with_ends(entries, own_key, least, high):
    shape = entries.shape
    spot = [jax.random.randint(jax.random.fold_in(own_key, axis), (), 0, shape[axis]) for axis in range(len(shape))]
    entries = entries.at[tuple(spot)].set(least)
    longest = shape.index(max(shape))
    spot[longest] = (spot[longest] + 1) % shape[longest]
    return entries.at[tuple(spot)].set(high)


def block_levels(rng, extent, cuts, smallest, high):
    level, own = 1.0, jax.random.fold_in(rng, 6)
    for position, blocks in cuts:
        draws = jnp.exp(jax.random.uniform(jax.random.fold_in(own, position), (blocks,), jnp.float32, smallest / len(cuts), high / len(cuts)))
        level = level * jnp.repeat(draws, extent[position] // blocks).reshape([-1 if axis == position else 1 for axis in range(len(extent))])
    return level


def centred(key, extent, scale, bound, pieces=(), held_as=jnp.bfloat16):
    entries = jax.random.normal(key, extent, jnp.float32) * scale
    if len(pieces) > 0:
        entries = block_levels(key, extent, pieces, -0.22, 0.18) * entries
    return jnp.clip(entries, min=-bound, max=bound).astype(held_as)


def setup_inputs(seed: int = 0) -> dict:
    key_list = jax.random.split(jax.random.key(seed), 14)
    inputs = draw_inputs(jax.random.fold_in(key_list[13], 71), 0)
    lengths = with_ends(jax.random.randint(key_list[1], (SEQS,), SEQ_LEN // 4, SEQ_LEN + 1), jax.random.fold_in(key_list[1], 1), SEQ_LEN // 4, SEQ_LEN).astype(jnp.int32)
    cotangent = centred(key_list[2], (SEQS, SEQ_LEN, D), 1.0, 6.0, ((0, 8), (1, 4)))
    ln_gains = jnp.clip(1.0 + 0.1 * jax.random.normal(key_list[3], (LAYERS, 2, D), jnp.float32), 0.5, 1.5)
    ln_biases = centred(key_list[4], (LAYERS, 2, D), 0.1, 0.5, (), jnp.float32)
    w_query = centred(key_list[5], (LAYERS, D, D), D ** -0.5, 0.25, ((2, 4),))
    w_key = centred(key_list[6], (LAYERS, D, D), D ** -0.5, 0.25, ((2, 4),))
    w_value = centred(key_list[7], (LAYERS, D, D), D ** -0.5, 0.25, ((2, 4),))
    w_output = centred(key_list[8], (LAYERS, D, D), (max(1, D // 32)) ** -0.5, 1.5, ((1, 4),))
    w_in = centred(key_list[9], (LAYERS, D, FF), D ** -0.5, 0.25, ((2, 4),))
    b_in = centred(key_list[10], (LAYERS, FF), 0.3, 1.5, ((1, 4),))
    w_out = centred(key_list[11], (LAYERS, FF, D), FF ** -0.5, 0.125, ((1, 4),))
    b_out = centred(key_list[12], (LAYERS, D), 0.3, 1.5, (), jnp.float32)
    return dict(inputs=inputs, lengths=lengths, cotangent=cotangent, ln_gains=ln_gains, ln_biases=ln_biases, w_query=w_query, w_key=w_key, w_value=w_value, w_output=w_output, w_in=w_in, b_in=b_in, w_out=w_out, b_out=b_out)


HIGHEST = lax.Precision.HIGHEST

@jax.custom_vjp
def low(v):
    return lax.optimization_barrier(v.astype(jnp.bfloat16)).astype(jnp.float32)

@jax.custom_vjp
def low_back(v):
    return v

def low_keep(v):
    return (low(v), None)

def low_pass(kept, grad):
    return (grad,)

def back_keep(v):
    return (v, None)

def back_low(kept, grad):
    return (low(grad),)
low.defvjp(low_keep, low_pass)
low_back.defvjp(back_keep, back_low)

def product(left_side, right_side):
    return jnp.dot(left_side, right_side, precision=HIGHEST, preferred_element_type=jnp.float32)

def layer_norm(values, norm_gain, norm_offset):
    center = values - lax.optimization_barrier(jnp.mean(values, axis=-1, keepdims=True))
    spread = lax.optimization_barrier(jnp.mean(center * center, axis=-1, keepdims=True))
    return center * lax.rsqrt(spread + 1e-05) * norm_gain + norm_offset

def cover_table(level_index):
    if level_index == 0:
        return jnp.ones((BLOCK, 3 * BLOCK), jnp.float32)
    half_block = BLOCK // 2
    query_part = np.arange(BLOCK)[:, None] // half_block
    key_part = np.arange(3 * BLOCK)[None, :] // half_block
    return jnp.asarray(np.abs(2 + query_part - key_part) >= 2).astype(jnp.float32)

def windows(values, blocks):
    padding = [(BLOCK, BLOCK)] + [(0, 0)] * (values.ndim - 1)
    padded = jnp.pad(values, padding).reshape((blocks + 2, BLOCK) + values.shape[1:])
    return jnp.concatenate([padded[:-2], padded[1:-1], padded[2:]], axis=1)

def level_terms(queries, keys, values, counts, cover_mask):
    length = counts.shape[0]
    blocks = length // BLOCK
    grouped = queries.reshape((blocks, BLOCK) + queries.shape[1:])
    key_win = windows(keys, blocks)
    value_win = windows(values, blocks)
    count_win = windows(counts, blocks)
    scores = jnp.einsum('bqhe,bkhe->bhqk', grouped, key_win, precision=HIGHEST) * (1.0 / math.sqrt(HEAD_DIM))
    scores = low_back(scores)
    weights = jnp.exp(scores) * cover_mask
    weights_low = low(weights)
    numerator = jnp.einsum('bhqk,bkhe->bqhe', weights_low, value_win, precision=HIGHEST)
    numerator = low_back(numerator).reshape(queries.shape)
    denominator = lax.optimization_barrier(jnp.sum(weights * count_win[:, None, None, :], axis=-1))
    denominator = jnp.transpose(denominator, (0, 2, 1)).reshape(length, queries.shape[1])
    return (numerator, denominator)

def hierarchy(queries, keys, values, mask):
    spread_mask = mask[:, None, None]
    query_avg = queries * spread_mask
    key_avg = keys * spread_mask
    value_sum = values * spread_mask
    counts = mask
    numerator = jnp.zeros(queries.shape, jnp.float32)
    denominator = jnp.zeros(queries.shape[:2], jnp.float32)
    for level_index in range(LEVELS + 1):
        if level_index > 0:
            query_avg = 0.5 * (query_avg[0::2] + query_avg[1::2])
            key_avg = 0.5 * (key_avg[0::2] + key_avg[1::2])
            value_sum = value_sum[0::2] + value_sum[1::2]
            counts = counts[0::2] + counts[1::2]
        level_num, level_den = level_terms(low(query_avg), low(key_avg), low(value_sum), counts, cover_table(level_index))
        factor = 2 ** level_index
        numerator = numerator + jnp.repeat(level_num, factor, axis=0)
        denominator = denominator + jnp.repeat(level_den, factor, axis=0)
    return numerator / denominator[:, :, None]

def sequence_forward(stream, mask, params):
    gains, offsets, wq_all, wk_all, wv_all, attention_output_weights, input_weight_stack, bias_in, output_weight_stack, bias_out = params
    weight_rows = mask[:, None]
    terms = []
    for layer_number in range(LAYERS):
        first = low(layer_norm(stream, gains[layer_number, 0], offsets[layer_number, 0]))
        queries = low(low_back(product(first, wq_all[layer_number]))).reshape(SEQ_LEN, HEADS, HEAD_DIM)
        keys = low(low_back(product(first, wk_all[layer_number]))).reshape(SEQ_LEN, HEADS, HEAD_DIM)
        values = low(low_back(product(first, wv_all[layer_number]))).reshape(SEQ_LEN, HEADS, HEAD_DIM)
        mixed = hierarchy(queries, keys, values, mask)
        blended_coarse = low(low_back(mixed)).reshape(SEQ_LEN, D)
        attn_out = low_back(product(blended_coarse, attention_output_weights[layer_number]))
        middle = stream + attn_out
        second = low(layer_norm(middle, gains[layer_number, 1], offsets[layer_number, 1]))
        hidden_pre = low_back(product(second, input_weight_stack[layer_number]) + bias_in[layer_number])
        hidden_activation = low(jax.nn.gelu(hidden_pre, approximate=False))
        ffn_out = low_back(product(hidden_activation, output_weight_stack[layer_number]) + bias_out[layer_number])
        stream = middle + ffn_out
        terms.append(jnp.sum(weight_rows * attn_out * attn_out))
        terms.append(jnp.sum(weight_rows * ffn_out * ffn_out))
        terms.append(jnp.sum(weight_rows * stream * stream))
    terms.append(jnp.sum(mask))
    return (stream, jnp.stack(terms))

def reference(inputs, lengths, cotangent, ln_gains, ln_biases, w_query, w_key, w_value, w_output, w_in, b_in, w_out, b_out):
    params = tuple((weight.astype(jnp.float32) for weight in (ln_gains, ln_biases, w_query, w_key, w_value, w_output, w_in, b_in, w_out, b_out)))
    states = inputs.astype(jnp.float32)
    positions = jnp.arange(SEQ_LEN, dtype=jnp.int32)
    masks = (positions[None, :] < lengths[:, None].astype(jnp.int32)).astype(jnp.float32)

    def whole(states_in, params_in):

        def stepper(carry, item):
            return (carry, sequence_forward(item[0], item[1], params_in))
        _, (outs_all, terms_all) = lax.scan(jax.checkpoint(stepper), jnp.float32(0.0), (states_in, masks))
        return (outs_all, terms_all)
    outs_all, pullback, terms_all = jax.vjp(whole, states, params, has_aux=True)
    grad_states, grad_params = pullback(cotangent.astype(jnp.float32) * masks[:, :, None])
    totals = lax.optimization_barrier(jnp.sum(terms_all, axis=0))
    norms = jnp.sqrt(totals[:3 * LAYERS] / (totals[3 * LAYERS] * D))
    return (outs_all, grad_states, grad_params[0], grad_params[1], grad_params[2], grad_params[3], grad_params[4], grad_params[5], grad_params[6], grad_params[7], grad_params[8], grad_params[9], norms)
```

```python
import functools
import math

import jax
import jax.numpy as jnp
import numpy as np
from jax import lax
from jax.experimental import pallas as pl
from jax.experimental.pallas import tpu as pltpu
from jax.sharding import PartitionSpec as P

F32 = jnp.float32
BF16 = jnp.bfloat16

LAYERS = 2
ROWS = 256
WIDTH = 512
PIECES = 8
SLOTS = 4
HEAD_PAIR = 128
TILE = 64
CTX = 672
NEG = -1e30

FIRST = (0, 256, 384, 448, 480)
LAST = (240, 368, 432, 464, 480)
LEVEL_SIZE = (256, 128, 64, 32, 16)
CTX_PREV = (0, 288, 448, 544, 608)
CTX_OWN = (16, 304, 464, 560, None)
CTX_NEXT = (272, 432, 528, 592, 624)
CTX_Y = 640
CTX_DIAG = 656
TILES = (
    (0, 0, 96, 0),
    (64, 64, 96, 0),
    (128, 128, 96, 0),
    (192, 192, 96, 0),
    (256, 288, 96, 1),
    (320, 352, 96, 1),
    (384, 448, 96, 1),
    (448, 544, 128, 2),
)


def dot(left, right):
    return lax.dot_general(left, right, (((1,), (0,)), ((), ())), preferred_element_type=F32)


def dot_nt(left, right):
    return lax.dot_general(left, right, (((1,), (1,)), ((), ())), preferred_element_type=F32)


def dot_tn(left, right):
    return lax.dot_general(left, right, (((0,), (0,)), ((), ())), preferred_element_type=F32)


def coarse_tables():
    spread = np.zeros((ROWS, ROWS), np.float32)
    step = np.ones((ROWS,), np.float32)
    at = 0
    for level in range(1, 6):
        factor = 2**level
        for index in range(ROWS // factor):
            spread[index * factor : (index + 1) * factor, at] = 1.0
            step[at] = factor
            at += 1
    return spread, step


def mask_tables():
    query = np.arange(TILE)[:, None]
    key = np.arange(128)[None, :]
    near = (key // 16 - query // 16 >= 0) & (key // 16 - query // 16 <= 2)
    exact = near & (key < 96)
    far = np.abs((query + 16) // 8 - key // 8) >= 2
    coarse = near & far & (key < 96)
    top = np.zeros((TILE, 128), bool)
    top[:32, :64] = (near & far)[:32, :64]
    half_query = 2 + np.arange(16)[:, None] // 8
    half_prev = np.arange(16)[None, :] // 8
    top[32:48, 64:80] = np.abs(half_query - half_prev) >= 2
    top[32:48, 80:96] = np.abs(half_query - half_prev - 4) >= 2
    top[48:56, 96:104] = True
    top[48:56, 112:120] = True
    tables = []
    for table in (exact, coarse, top):
        bias = np.where(table, 0.0, NEG).astype(np.float32)
        tables.append(np.concatenate([bias, bias], axis=0))
    return np.stack(tables)


def context_tables():
    step = np.ones((CTX,), np.int32)
    start = np.zeros((CTX,), np.int32)
    kind = np.zeros((CTX,), np.int32)
    for level in range(5):
        size = LEVEL_SIZE[level]
        for offset in range(16):
            for base, first in ((CTX_PREV[level], -16), (CTX_NEXT[level], size)):
                step[base + offset] = 2**level
                start[base + offset] = first + offset
        if CTX_OWN[level] is not None:
            for offset in range(size):
                step[CTX_OWN[level] + offset] = 2**level
                start[CTX_OWN[level] + offset] = offset
    for offset in range(16):
        for base, which in ((CTX_Y, 1), (CTX_DIAG, 2)):
            step[base + offset] = 32
            start[base + offset] = offset
            kind[base + offset] = which if offset < 8 else 3
    return step, start, kind


def halo_tables():
    first = np.zeros((ROWS, 80), np.float32)
    last = np.zeros((ROWS, 80), np.float32)
    whole = np.zeros((ROWS, 16), np.float32)
    step = np.ones((192,), np.float32)
    for level in range(5):
        factor = 2**level
        size = LEVEL_SIZE[level]
        for offset in range(16):
            column = level * 16 + offset
            first[offset * factor : (offset + 1) * factor, column] = 1.0
            index = size - 16 + offset
            last[index * factor : (index + 1) * factor, column] = 1.0
            step[column] = factor
            step[80 + column] = factor
    for offset in range(8):
        whole[offset * 32 : (offset + 1) * 32, offset] = 1.0
    step[160:] = 32.0
    return first, last, whole, step


SPREAD, STEP = coarse_tables()
MASKS = mask_tables()


def normalize(values):
    center = values - jnp.mean(values, axis=-1, keepdims=True)
    spread = jnp.mean(center * center, axis=-1, keepdims=True)
    scale = lax.rsqrt(spread + 1e-05)
    return center * scale, scale


def normalize_back(values, gain, grad):
    hat, scale = normalize(values)
    inner = grad * gain
    mean = jnp.mean(inner, axis=-1, keepdims=True)
    along = jnp.mean(inner * hat, axis=-1, keepdims=True)
    result = scale * (inner - mean - hat * along)
    return result, jnp.sum(grad * hat, axis=0, keepdims=True), jnp.sum(grad, axis=0, keepdims=True)


def gelu_parts(values):
    size = jnp.abs(values) * (1.0 / math.sqrt(2.0))
    ratio = 1.0 / (1.0 + 0.3275911 * size)
    bell = jnp.exp(-size * size)
    poly = ratio * (
        0.254829592
        + ratio * (-0.284496736 + ratio * (1.421413741 + ratio * (-1.453152027 + ratio * 1.061405429)))
    )
    tail = 0.5 * poly * bell
    share = jnp.where(values >= 0.0, 1.0 - tail, tail)
    slope = share + values * bell * (1.0 / math.sqrt(2.0 * math.pi))
    return values * share, slope


def row_mask(info_ref, shape):
    return lax.broadcasted_iota(jnp.int32, shape, 0) < info_ref[0]


def project(normed, weights, info_ref, spread_t, step_inv, qkv_ref, core_ref, diag_ref, far_ref):
    even = info_ref[1] == 1
    keep = row_mask(info_ref, (ROWS, 3 * HEAD_PAIR))
    column = lax.broadcasted_iota(jnp.int32, (ROWS, 3 * HEAD_PAIR), 1)
    column_scale = jnp.where(column < HEAD_PAIR, 0.125, 1.0)
    step_wide = jnp.concatenate([step_inv, step_inv], axis=1)
    for slot in range(SLOTS):
        rounded = dot(normed, weights[slot][...]).astype(BF16).astype(F32)
        exact = (jnp.where(keep, rounded, 0.0) * column_scale).astype(BF16)
        qkv_ref[slot, :ROWS, :] = exact
        pooled = dot(spread_t, exact)
        qkv_ref[slot, ROWS:, : 2 * HEAD_PAIR] = (pooled[:, : 2 * HEAD_PAIR] * step_wide).astype(BF16)
        qkv_ref[slot, ROWS:, 2 * HEAD_PAIR :] = pooled[:, 2 * HEAD_PAIR :].astype(BF16)
        for level in range(5):
            first = qkv_ref[slot, FIRST[level] : FIRST[level] + 16, HEAD_PAIR:]
            last = qkv_ref[slot, LAST[level] : LAST[level] + 16, HEAD_PAIR:]
            core_ref[slot, level * 16 : level * 16 + 16, :] = jnp.where(even, last, first)
            diag_ref[slot, level * 16 : level * 16 + 16, :] = jnp.where(even, first, last)
        qkv_ref.flush_part(slot)
        top = qkv_ref[slot, 496:512, HEAD_PAIR:]
        diag_ref[slot, 80:96, :] = top
        far_ref[slot, :, :] = top


def first_kernel(
    info_ref, x_ref, gain_ref, offset_ref, w0, w1, w2, w3, spread_t_ref, step_ref,
    normed_ref, qkv_ref, core_ref, diag_ref, far_ref,
):
    hat, _ = normalize(x_ref[0].astype(F32))
    normed = (hat * gain_ref[0, 0:1, :] + offset_ref[0, 0:1, :]).astype(BF16)
    normed_ref[...] = normed
    project(
        normed, (w0, w1, w2, w3), info_ref, spread_t_ref[...], step_ref[...],
        qkv_ref, core_ref, diag_ref, far_ref,
    )


def head_stack(values):
    column = lax.broadcasted_iota(jnp.int32, values.shape, 1) % HEAD_PAIR
    zero = jnp.zeros_like(values)
    left = jnp.where(column < HEAD_PAIR // 2, values, zero)
    right = jnp.where(column < HEAD_PAIR // 2, zero, values)
    return jnp.concatenate([left, right], axis=0)


def head_join(stacked):
    column = lax.broadcasted_iota(jnp.int32, (TILE, stacked.shape[1]), 1) % HEAD_PAIR
    return jnp.where(column < HEAD_PAIR // 2, stacked[:TILE], stacked[TILE:])


def mix_kernel(
    layer, info_ref, qkv_ref, core_ref, diag_ref, far_ref, count_ref, bias_ref, spread_ref,
    stream_ref, gain_ref, offset_ref, w0, w1, w2, w3,
    ctx_ref, mixed_ref, inverse_ref, middle_ref, normed_ref, stat_ref,
    pair_ref,
):
    even = info_ref[1] == 1
    near = info_ref[2] == 1
    for slot in range(SLOTS):
        for level in range(5):
            rows = slice(level * 16, level * 16 + 16)
            core = core_ref[slot ^ 1, rows, :]
            diag = diag_ref[slot ^ 3, rows, :]
            diag = jnp.where(near, diag, jnp.zeros_like(diag))
            ctx_ref[slot, CTX_PREV[level] : CTX_PREV[level] + 16, :] = jnp.where(even, diag, core)
            ctx_ref[slot, CTX_NEXT[level] : CTX_NEXT[level] + 16, :] = jnp.where(even, core, diag)
            if CTX_OWN[level] is not None:
                own = slice(CTX_OWN[level], CTX_OWN[level] + LEVEL_SIZE[level])
                source = slice(FIRST[level], FIRST[level] + LEVEL_SIZE[level])
                ctx_ref[slot, own, :] = qkv_ref[slot, source, HEAD_PAIR:]
        ctx_ref[slot, CTX_Y : CTX_Y + 16, :] = far_ref[slot ^ 2, :, :]
        diag = diag_ref[slot ^ 3, 80:96, :]
        ctx_ref[slot, CTX_DIAG : CTX_DIAG + 16, :] = jnp.where(near, jnp.zeros_like(diag), diag)

    ctx_ref.flush()
    ready(qkv_ref, bias_ref, count_ref, spread_ref)

    @pl.loop(0, SLOTS)
    def _(slot):
        for query_row, context_row, keys, mask in TILES:
            queries = head_stack(qkv_ref[slot, query_row : query_row + TILE, :HEAD_PAIR])
            context = slice(context_row, context_row + keys)
            scores = dot_nt(queries, ctx_ref[slot, context, :HEAD_PAIR])
            weights = jnp.exp(scores + bias_ref[mask, :, :keys]).astype(BF16)
            values = jnp.concatenate(
                [ctx_ref[slot, context, HEAD_PAIR:], count_ref[context, :]], axis=1
            )
            pair_ref[query_row : query_row + TILE, :] = head_join(dot(weights, values))
        coarse = pair_ref[ROWS:, :]
        high = coarse.astype(BF16)
        low = (coarse - high.astype(F32)).astype(BF16)
        spread = spread_ref[...]
        total = pair_ref[:ROWS, :] + dot(spread, high) + dot(spread, low)
        inverse = 1.0 / total[:, HEAD_PAIR:]
        inverse_ref[slot, :, :] = inverse
        mixed_ref[slot, :, :] = (total[:, :HEAD_PAIR] * inverse).astype(BF16)
        inverse_ref.flush_part(slot)
        mixed_ref.flush_part(slot)

    attended = None
    for slot, weight in enumerate((w0, w1, w2, w3)):
        block = jnp.concatenate(
            [weight[j * 128 : (j + 1) * 128, :] for j in range(4)], axis=1
        )
        part = dot(mixed_ref[slot, :, :], block)
        attended = part if attended is None else attended + part
    keep = row_mask(info_ref, attended.shape)
    stat_ref[...] = jnp.sum(jnp.where(keep, attended * attended, 0.0), axis=0, keepdims=True)
    stream = stream_ref[0] if layer == 0 else stream_ref[...]
    middle = stream.astype(F32) + attended
    middle_ref[...] = middle
    hat, _ = normalize(middle)
    gain, offset = gain_ref[layer, 1:2, :], offset_ref[layer, 1:2, :]
    normed_ref[...] = (hat * gain + offset).astype(BF16)


def feed_kernel(
    info_ref, normed_ref, middle_ref, w0, w1, w2, w3, bias_out_ref,
    gain_ref, offset_ref, p0, p1, p2, p3, spread_t_ref, step_ref,
    act_ref, slope_ref, stat_ref, stream_ref, next_ref, qkv_ref, core_ref, diag_ref, far_ref,
):
    normed = normed_ref[...]
    total = None
    for slot, weight in enumerate((w0, w1, w2, w3)):
        hidden = dot(normed, weight[:512, :]) + weight[1024:1025, :].astype(F32)
        act, slope = gelu_parts(hidden)
        act = act.astype(BF16)
        act_ref[slot, :, :] = act
        slope_ref[slot, :, :] = slope.astype(BF16)
        act_ref.flush_part(slot)
        slope_ref.flush_part(slot)
        part = dot(act, weight[512:1024, :])
        total = part if total is None else total + part
    total = total + bias_out_ref[0:1, :]
    keep = row_mask(info_ref, total.shape)
    stream = middle_ref[...] + total
    stat_ref[0:1, :] = jnp.sum(jnp.where(keep, total * total, 0.0), axis=0, keepdims=True)
    stat_ref[1:2, :] = jnp.sum(jnp.where(keep, stream * stream, 0.0), axis=0, keepdims=True)
    stream_ref[...] = stream
    hat, _ = normalize(stream)
    following = (hat * gain_ref[1, 0:1, :] + offset_ref[1, 0:1, :]).astype(BF16)
    next_ref[...] = following
    project(
        following, (p0, p1, p2, p3), info_ref, spread_t_ref[...], step_ref[...],
        qkv_ref, core_ref, diag_ref, far_ref,
    )


def put_grads(keep_ref, send_ref, slot, matrix, value, at=0):
    target = keep_ref if slot % 2 == 0 else send_ref
    low = value.astype(BF16)
    for piece in range(PIECES):
        target[slot // 2, piece, matrix * 64 : matrix * 64 + 64, at : at + value.shape[1]] = low[
            piece * 64 : piece * 64 + 64
        ]


def put_output_grads(keep_ref, send_ref, output_ref, matrix):
    for slot in range(SLOTS):
        put_grads(keep_ref, send_ref, slot, matrix, output_ref[slot, :, :], 3 * HEAD_PAIR)


def turn_kernel(
    info_ref, normed_ref, middle_ref, w0, w1, w2, w3, bias_out_ref, cotangent_ref, gain_ref,
    stream_ref, stat_ref, keep_ref, send_ref, hidden_grad_ref, small_ref, grad_ref,
):
    normed = normed_ref[...]
    keep = row_mask(info_ref, normed.shape)
    grad = jnp.where(keep, cotangent_ref[0].astype(F32), 0.0)
    grad_low = grad.astype(BF16)
    total = None
    back = None
    for slot, weight in enumerate((w0, w1, w2, w3)):
        hidden = dot(normed, weight[:512, :]) + weight[1024:1025, :].astype(F32)
        act, slope = gelu_parts(hidden)
        act = act.astype(BF16)
        part = dot(act, weight[512:1024, :])
        total = part if total is None else total + part
        hidden_grad = (dot_nt(grad_low, weight[512:1024, :]) * slope).astype(BF16)
        part = dot_nt(hidden_grad, weight[:512, :])
        back = part if back is None else back + part
        put_grads(keep_ref, send_ref, slot, 0, dot_tn(normed, hidden_grad))
        put_grads(keep_ref, send_ref, slot, 1, dot_tn(act, grad_low))
        hidden_grad_ref[slot : slot + 1, :] = jnp.sum(hidden_grad.astype(F32), axis=0, keepdims=True)
    keep_ref.flush()
    send_ref.flush()
    total = total + bias_out_ref[1:2, :]
    stream = middle_ref[...] + total
    stat_ref[0:1, :] = jnp.sum(jnp.where(keep, total * total, 0.0), axis=0, keepdims=True)
    stat_ref[1:2, :] = jnp.sum(jnp.where(keep, stream * stream, 0.0), axis=0, keepdims=True)
    stream_ref[...] = stream
    through, gain_grad, offset_grad = normalize_back(middle_ref[...], gain_ref[1, 1:2, :], back)
    small_ref[0:1, :] = gain_grad
    small_ref[1:2, :] = offset_grad
    small_ref[2:3, :] = jnp.sum(grad_low.astype(F32), axis=0, keepdims=True)
    grad_ref[...] = grad + through


def mix_back_kernel(
    info_ref, grad_ref, w0, w1, w2, w3, mixed_ref, inverse_ref, qkv_ref, ctx_ref, count_ref,
    bias_ref, spread_ref, spread_t_ref, step_ref,
    output_ref, local_ref, core_ref, diag_ref, far_ref,
    low_ref, pair_ref, query_ref, context_ref,
):
    even = info_ref[1] == 1
    grad_low = grad_ref[...].astype(BF16)
    step_inv = step_ref[...]
    for slot, weight in enumerate((w0, w1, w2, w3)):
        block = jnp.concatenate(
            [weight[j * 128 : (j + 1) * 128, :] for j in range(4)], axis=1
        )
        mixed = mixed_ref[slot, :, :]
        rows_grad = dot_tn(mixed, grad_low)
        for j in range(4):
            output_ref[slot, j * 128 : (j + 1) * 128, :] = rows_grad[
                :, j * 128 : (j + 1) * 128
            ].astype(BF16)
        back = dot_nt(grad_low, block).astype(BF16).astype(F32)
        scaled = back * inverse_ref[slot, :, :]
        low_ref[slot, :, :HEAD_PAIR] = scaled.astype(BF16)
        low_ref[slot, :, HEAD_PAIR:] = (-scaled * mixed.astype(F32)).astype(BF16)

    output_ref.flush()
    ready(qkv_ref, ctx_ref, bias_ref, count_ref, spread_ref, spread_t_ref)

    @pl.loop(0, SLOTS)
    def _(slot):
        pair_ref[:ROWS, :] = low_ref[slot, :, :]
        pair_ref[ROWS:, :] = dot(spread_t_ref[...], low_ref[slot, :, :]).astype(BF16)
        context_ref[...] = jnp.zeros_like(context_ref)
        for query_row, context_row, keys, mask in TILES:
            queries = head_stack(qkv_ref[slot, query_row : query_row + TILE, :HEAD_PAIR])
            context = slice(context_row, context_row + keys)
            keyed = ctx_ref[slot, context, :HEAD_PAIR]
            scores = dot_nt(queries, keyed)
            weights = jnp.exp(scores + bias_ref[mask, :, :keys])
            values = jnp.concatenate(
                [ctx_ref[slot, context, HEAD_PAIR:], count_ref[context, :]], axis=1
            )
            upper = head_stack(pair_ref[query_row : query_row + TILE, :])
            grad_scores = (dot_nt(upper, values) * weights).astype(BF16)
            query_ref[query_row : query_row + TILE, :] = head_join(dot(grad_scores, keyed)) * 0.125
            context_ref[context, :HEAD_PAIR] += dot_tn(grad_scores, queries)
            context_ref[context, HEAD_PAIR:] += dot_tn(weights.astype(BF16), upper[:, :HEAD_PAIR])
        query_coarse = query_ref[ROWS:, :] * step_inv
        key_coarse = jnp.concatenate(
            [
                context_ref[CTX_OWN[level] : CTX_OWN[level] + LEVEL_SIZE[level], :HEAD_PAIR]
                for level in (1, 2, 3)
            ]
            + [jnp.zeros((32, HEAD_PAIR), F32)],
            axis=0,
        ) * step_inv
        value_coarse = jnp.concatenate(
            [
                context_ref[CTX_OWN[level] : CTX_OWN[level] + LEVEL_SIZE[level], HEAD_PAIR:]
                for level in (1, 2, 3)
            ]
            + [jnp.zeros((32, HEAD_PAIR), F32)],
            axis=0,
        )
        coarse = jnp.concatenate([query_coarse, key_coarse, value_coarse], axis=1).astype(BF16)
        down = dot(spread_ref[...], coarse)
        local_ref[slot, :, :HEAD_PAIR] = query_ref[:ROWS, :] + down[:, :HEAD_PAIR]
        local_ref[slot, :, HEAD_PAIR:] = context_ref[16 : 16 + ROWS, :] + down[:, HEAD_PAIR:]
        local_ref.flush_part(slot)
        for level in range(5):
            rows = slice(level * 16, level * 16 + 16)
            before = context_ref[CTX_PREV[level] : CTX_PREV[level] + 16, :]
            after = context_ref[CTX_NEXT[level] : CTX_NEXT[level] + 16, :]
            core_ref[slot, rows, :] = jnp.where(even, after, before).astype(BF16)
            diag_ref[slot, rows, :] = jnp.where(even, before, after).astype(BF16)
        diag_ref[slot, 80:96, :] = context_ref[CTX_DIAG : CTX_DIAG + 16, :].astype(BF16)
        far_ref[slot, :, :] = context_ref[CTX_Y : CTX_Y + 16, :].astype(BF16)
        for target in (core_ref, diag_ref, far_ref):
            target.flush_part(slot)


def project_back(
    info_ref, local_ref, core_ref, diag_ref, far_ref, halo_ref, halo_step_ref, normed, weights,
    keep_ref, send_ref,
):
    keep = row_mask(info_ref, (ROWS, 3 * HEAD_PAIR))
    halo = halo_ref[...]
    halo_step = halo_step_ref[...]
    back = None
    for slot in range(SLOTS):
        arrived = jnp.concatenate(
            [core_ref[slot ^ 1, :, :], diag_ref[slot ^ 3, :, :], far_ref[slot ^ 2, :, :]], axis=0
        ).astype(F32)
        arrived = jnp.concatenate(
            [arrived[:, :HEAD_PAIR] * halo_step, arrived[:, HEAD_PAIR:]], axis=1
        ).astype(BF16)
        added = dot(halo, arrived)
        local = local_ref[slot, :, :]
        whole = jnp.concatenate([local[:, :HEAD_PAIR], local[:, HEAD_PAIR:] + added], axis=1)
        low = jnp.where(keep, whole, 0.0).astype(BF16)
        put_grads(keep_ref, send_ref, slot, 0, dot_tn(normed, low))
        part = dot_nt(low, weights[slot][...])
        back = part if back is None else back + part
    return back


def between_kernel(
    info_ref, local_ref, core_ref, diag_ref, far_ref, halo_ref, halo_step_ref,
    normed_ref, p0, p1, p2, p3, grad_in_ref, stream_ref, gain_ref,
    act_ref, slope_ref, second_ref, middle_ref, w0, w1, w2, w3, output_ref,
    keep_ref, send_ref, feed_keep_ref, feed_send_ref, hidden_grad_ref, small_ref, grad_ref,
):
    back = project_back(
        info_ref, local_ref, core_ref, diag_ref, far_ref, halo_ref, halo_step_ref,
        normed_ref[...], (p0, p1, p2, p3), keep_ref, send_ref,
    )
    put_output_grads(keep_ref, send_ref, output_ref, 0)
    keep_ref.flush()
    send_ref.flush()
    through, gain_grad, offset_grad = normalize_back(stream_ref[...], gain_ref[1, 0:1, :], back)
    small_ref[0:1, :] = gain_grad
    small_ref[1:2, :] = offset_grad
    grad = grad_in_ref[...] + through
    grad_low = grad.astype(BF16)
    small_ref[4:5, :] = jnp.sum(grad_low.astype(F32), axis=0, keepdims=True)
    second = second_ref[...]
    back = None
    for slot, weight in enumerate((w0, w1, w2, w3)):
        hidden_grad = (
            dot_nt(grad_low, weight[512:1024, :]) * slope_ref[slot, :, :].astype(F32)
        ).astype(BF16)
        part = dot_nt(hidden_grad, weight[:512, :])
        back = part if back is None else back + part
        put_grads(feed_keep_ref, feed_send_ref, slot, 0, dot_tn(second, hidden_grad))
        put_grads(feed_keep_ref, feed_send_ref, slot, 1, dot_tn(act_ref[slot, :, :], grad_low))
        hidden_grad_ref[slot : slot + 1, :] = jnp.sum(hidden_grad.astype(F32), axis=0, keepdims=True)
    feed_keep_ref.flush()
    feed_send_ref.flush()
    through, gain_grad, offset_grad = normalize_back(middle_ref[...], gain_ref[0, 1:2, :], back)
    small_ref[2:3, :] = gain_grad
    small_ref[3:4, :] = offset_grad
    grad_ref[...] = grad + through


def last_kernel(
    info_ref, local_ref, core_ref, diag_ref, far_ref, halo_ref, halo_step_ref,
    normed_ref, p0, p1, p2, p3, grad_in_ref, stream_ref, gain_ref, output_ref,
    stat_a, stat_b, stat_c, stat_d, small_a, small_b, hidden_one, hidden_two,
    keep_ref, send_ref, grad_ref,
):
    back = project_back(
        info_ref, local_ref, core_ref, diag_ref, far_ref, halo_ref, halo_step_ref,
        normed_ref[...], (p0, p1, p2, p3), keep_ref, send_ref,
    )
    put_output_grads(keep_ref, send_ref, output_ref, 0)
    through, gain_grad, offset_grad = normalize_back(
        stream_ref[0].astype(F32), gain_ref[0, 0:1, :], back
    )
    grad_ref[...] = grad_in_ref[...] + through
    position = lax.broadcasted_iota(jnp.int32, (1, WIDTH), 1)
    valid = jnp.where(position < jnp.minimum(info_ref[0], ROWS), 1.0, 0.0)
    lines = [
        gain_grad, offset_grad,
        small_b[0:1, :], small_b[1:2, :], small_b[2:3, :], small_b[3:4, :], small_b[4:5, :],
        small_a[0:1, :], small_a[1:2, :], small_a[2:3, :],
        stat_a[...], stat_b[0:1, :], stat_b[1:2, :], stat_c[...], stat_d[0:1, :], stat_d[1:2, :],
        valid,
    ]
    zero = jnp.zeros((1, WIDTH), F32)
    for slot in range(SLOTS):
        target = keep_ref if slot % 2 == 0 else send_ref
        own = lines + [hidden_one[slot : slot + 1, :], hidden_two[slot : slot + 1, :]]
        own = own + [zero] * (8 * PIECES - len(own))
        for piece in range(PIECES):
            rows = jnp.concatenate(own[piece * 8 : piece * 8 + 8], axis=0)
            target[slot // 2, piece, 64:72, :] = rows.astype(BF16)


def core_sum_kernel(keep_hbm, arrived_hbm, far_ref, keep_ref, arrived_ref, sems):
    copies = [
        pltpu.make_async_copy(keep_hbm.at[1], keep_ref, sems.at[0]),
        pltpu.make_async_copy(arrived_hbm.at[1], arrived_ref, sems.at[1]),
    ]
    for copy in copies:
        copy.start()
    for copy in copies:
        copy.wait()
    far_ref[...] = (keep_ref[...].astype(F32) + arrived_ref[...].astype(F32)).astype(BF16)


def far_sum_kernel(
    index_ref, keep_hbm, arrived_hbm, back_hbm, stay_ref, go_ref, keep_ref, arrived_ref, back_ref, sems
):
    copies = [
        pltpu.make_async_copy(keep_hbm.at[0], keep_ref, sems.at[0]),
        pltpu.make_async_copy(arrived_hbm.at[0], arrived_ref, sems.at[1]),
        pltpu.make_async_copy(back_hbm, back_ref, sems.at[2]),
    ]
    for copy in copies:
        copy.start()
    for copy in copies:
        copy.wait()
    side = index_ref[0]
    for place in range(PIECES // 2):
        for target, which in ((stay_ref, side), (go_ref, 1 - side)):
            piece = 2 * place + which
            target[place] = (
                keep_ref[piece].astype(F32)
                + arrived_ref[piece].astype(F32)
                + back_ref[piece].astype(F32)
            ).astype(BF16)


def split_sum_kernel(bit, index_ref, stay_ref, arrived_ref, next_stay_ref, next_go_ref):
    side = index_ref[bit]
    for place in range(next_stay_ref.shape[0]):
        for target, which in ((next_stay_ref, side), (next_go_ref, 1 - side)):
            piece = 2 * place + which
            target[place] = (stay_ref[piece].astype(F32) + arrived_ref[piece].astype(F32)).astype(BF16)


def add_kernel(stay_ref, arrived_ref, sum_ref):
    sum_ref[...] = (stay_ref[...].astype(F32) + arrived_ref[...].astype(F32)).astype(BF16)


def join_kernel(bit, index_ref, own_ref, other_ref, block_ref):
    side = index_ref[bit]
    for place in range(own_ref.shape[0]):
        block_ref[2 * place + side] = own_ref[place]
        block_ref[2 * place + 1 - side] = other_ref[place]


def placed(info_ref, own, other):
    side = info_ref[3]
    for place in range(PIECES // 2):
        yield 2 * place + side, own, place
        yield 2 * place + 1 - side, other, place


def feed_result_kernel(info_ref, own_one, other_one, own_two, other_two, in_ref, out_ref):
    for layer, pair in ((1, (own_two, other_two)), (0, (own_one, other_one))):
        ready(*pair)
        for piece, source, place in placed(info_ref, *pair):
            rows = pl.ds(pl.multiple_of(piece * 64, 64), 64)
            in_ref[layer, rows, :] = source[place, :64, :].astype(F32)
            out_ref[layer, rows, :] = source[place, 64:, :].astype(F32)
        in_ref.flush_part(layer)
        out_ref.flush_part(layer)


def attn_result_kernel(
    info_ref, own_one, other_one, own_two, other_two,
    query_ref, key_ref, value_ref, output_ref, b_in_ref, gain_ref, offset_ref, b_out_ref, norm_ref,
    lines_ref,
):
    for layer, pair in ((1, (own_two, other_two)), (0, (own_one, other_one))):
        ready(*pair)
        for piece, source, place in placed(info_ref, *pair):
            rows = pl.ds(pl.multiple_of(piece * 64, 64), 64)
            part = source[place, :64, :].astype(F32)
            for i, target in enumerate((query_ref, key_ref, value_ref)):
                target[layer, rows, :] = part[:, i * HEAD_PAIR : (i + 1) * HEAD_PAIR]
            where = pl.ds(pl.multiple_of((piece % 2) * 64, 64), 64)
            columns = pl.ds(pl.multiple_of((piece // 2) * 128, 128), 128)
            output_ref[layer, where, columns] = part[:, 3 * HEAD_PAIR :]
            if layer == 0:
                rows = pl.ds(pl.multiple_of(piece * 8, 8), 8)
                lines_ref[rows, :] = source[place, 64:, :].astype(F32)
        for target in (query_ref, key_ref, value_ref, output_ref):
            target.flush_part(layer)
    for number, (target, place) in enumerate(
        (
            (gain_ref, (0, 0)), (offset_ref, (0, 0)), (gain_ref, (1, 0)), (offset_ref, (1, 0)),
            (gain_ref, (0, 1)), (offset_ref, (0, 1)), (b_out_ref, (0,)),
            (gain_ref, (1, 1)), (offset_ref, (1, 1)), (b_out_ref, (1,)),
        )
    ):
        line = lines_ref[number : number + 1, :]
        target[place[:-1] + (slice(place[-1], place[-1] + 1), slice(None))] = line
    b_in_ref[...] = lines_ref[17:19, :]
    squares = jnp.sum(lines_ref[10:18, :], axis=1, keepdims=True)
    count = jnp.sum(lines_ref[16:17, :], axis=1, keepdims=True)
    norm_ref[...] = jnp.broadcast_to(jnp.sqrt(squares / (count * WIDTH)), (8, 128))


ORDER = [None]


class Columns:
    def __init__(self, parts, start, stop):
        self.parts, self.start, self.stop = parts, start, stop


class Arriving:
    def __init__(self, ref, copies):
        self.ref, self.copies = ref, copies

    def wait(self):
        for copy in self.copies:
            copy.wait()
        self.copies = []

    def __getitem__(self, place):
        self.wait()
        return self.ref[place]


class Leaving:
    def __init__(self, ref, target, sem):
        self.ref, self.target, self.sem, self.started = ref, target, sem, False
        self.copy = pltpu.make_async_copy(ref, target, sem)

    def flush(self):
        if not self.started:
            self.copy.start()
        self.started = True

    def flush_part(self, place):
        pltpu.make_async_copy(self.ref.at[place], self.target.at[place], self.sem).start()
        self.started = True

    def __getitem__(self, place):
        return self.ref[place]

    def __setitem__(self, place, value):
        self.ref[place] = value


def ready(*arriving):
    for operand in arriving:
        operand.wait()


def staged(body, name, out, args, scratch=(), flops=0):
    args = (tie(args[0], ORDER[0]) if ORDER[0] is not None else args[0],) + tuple(args[1:])
    columns = [(arg.start, arg.stop) if isinstance(arg, Columns) else None for arg in args[1:]]
    groups = [arg.parts if isinstance(arg, Columns) else arg for arg in args[1:]]
    groups = [group if isinstance(group, tuple) else (group,) for group in groups]
    flat = [part for group in groups for part in group]
    held = []
    for group, pair in zip(groups, columns):
        dims = (group[0].shape[0] * len(group),) + group[0].shape[1:]
        if pair is not None:
            dims = (dims[0], pair[1] - pair[0])
        held.append(pltpu.VMEM(dims, group[0].dtype))

    def kernel(*refs):
        info_ref, refs = refs[0], list(refs[1:])
        sources = [refs.pop(0) for _ in flat]
        targets = [refs.pop(0) for _ in out]
        inner = [refs.pop(0) for _ in held]
        outer = [refs.pop(0) for _ in out]
        sem_in, sem_out = refs.pop(), None
        sem_out = refs.pop()
        arriving = []
        number = 0
        for group, ref, pair in zip(groups, inner, columns):
            copies = []
            for half, part in enumerate(group):
                rows = part.shape[0]
                target = ref
                if len(group) == 2:
                    side = info_ref[3] if half == 0 else 1 - info_ref[3]
                    target = ref.at[pl.ds(pl.multiple_of(side * rows, 16), rows)]
                source = sources[number]
                if pair is not None:
                    source = source.at[:, pair[0] : pair[1]]
                copies.append(pltpu.make_async_copy(source, target, sem_in.at[number]))
                copies[-1].start()
                number += 1
            arriving.append(Arriving(ref, copies))
        leaving = [
            Leaving(ref, target, sem_out.at[i])
            for i, (ref, target) in enumerate(zip(outer, targets))
        ]
        body(info_ref, *arriving, *leaving, *refs)
        for operand in arriving:
            operand.wait()
        for result in leaving:
            result.flush()
        for result in leaving:
            result.copy.wait()

    result = pl.pallas_call(
        kernel,
        out_shape=tuple(out),
        in_specs=[pl.BlockSpec(memory_space=pltpu.SMEM)]
        + [pl.BlockSpec(memory_space=pl.ANY)] * len(flat),
        out_specs=tuple(pl.BlockSpec(memory_space=pl.ANY) for _ in out),
        scratch_shapes=held
        + [pltpu.VMEM(o.shape, o.dtype) for o in out]
        + list(scratch)
        + [pltpu.SemaphoreType.DMA((len(out),)), pltpu.SemaphoreType.DMA((len(flat),))],
        cost_estimate=pl.CostEstimate(flops=1, bytes_accessed=1, transcendentals=0),
        name=name,
    )(args[0], *flat)
    ORDER[0] = result[-1]
    return result


def call(body, name, out, args, scalars=0, scratch=(), hbm=False):
    space = pl.ANY if hbm else pltpu.VMEM
    in_specs = [pl.BlockSpec(memory_space=pltpu.SMEM)] * scalars
    in_specs += [pl.BlockSpec(memory_space=space)] * (len(args) - scalars)
    args = (tie(args[0], ORDER[0]),) + tuple(args[1:])
    params = {} if hbm else dict(vmem_limit_bytes=4 << 20)
    result = pl.pallas_call(
        body,
        out_shape=tuple(out),
        in_specs=in_specs,
        out_specs=tuple(pl.BlockSpec(memory_space=pltpu.VMEM) for _ in out),
        scratch_shapes=list(scratch),
        compiler_params=pltpu.CompilerParams(**params),
        cost_estimate=pl.CostEstimate(flops=1, bytes_accessed=1, transcendentals=0),
        name=name,
    )(*args)
    ORDER[0] = result[-1]
    return result


def pack_first_kernel(wq, wk, wv, wo, own_ref, block, sems):
    pack_attn(0, wq, wk, wv, wo, block, sems)
    copy = pltpu.make_async_copy(block, own_ref, sems.at[0])
    copy.start()
    copy.wait()


def start_attn(layer, wq, wk, wv, wo, block, sems):
    copies = []
    for i, source in enumerate((wq, wk, wv)):
        target = block.at[:, i * HEAD_PAIR : (i + 1) * HEAD_PAIR]
        copies.append(pltpu.make_async_copy(source.at[layer], target, sems.at[i]))
    for j in range(4):
        target = block.at[j * 128 : (j + 1) * 128, 3 * HEAD_PAIR :]
        source = wo.at[layer, :, j * 128 : (j + 1) * 128]
        copies.append(pltpu.make_async_copy(source, target, sems.at[3 + j]))
    for copy in copies:
        copy.start()
    return copies


def pack_attn(layer, wq, wk, wv, wo, block, sems):
    for copy in start_attn(layer, wq, wk, wv, wo, block, sems):
        copy.wait()


def pack_rest_kernel(
    info_ref, wq, wk, wv, wo, w_in, b_in, w_out,
    attn_ref, feed_one, half_one, feed_two, half_two,
    attn, feeds, biases, sems, feed_sems, out_sems,
):
    side = info_ref[3]
    copies = start_attn(1, wq, wk, wv, wo, attn, sems)
    for layer in range(LAYERS):
        for i, source in enumerate((w_in, w_out)):
            copies.append(
                pltpu.make_async_copy(
                    source.at[layer], feeds.at[layer, i * 512 : i * 512 + 512],
                    feed_sems.at[layer * 2 + i],
                )
            )
            copies[-1].start()
    bias_copy = pltpu.make_async_copy(b_in, biases, feed_sems.at[4])
    bias_copy.start()
    bias_copy.wait()
    row = lax.broadcasted_iota(jnp.int32, (32, WIDTH), 0)
    for layer in range(LAYERS):
        line = jnp.broadcast_to(biases[layer : layer + 1, :].astype(F32), (32, WIDTH))
        feeds[layer, 1024:1056, :] = jnp.where(row == 0, line, 0.0).astype(BF16)
    for copy in copies:
        copy.wait()
    sent = []
    place = pl.ds(pl.multiple_of(side * 528, 16), 528)
    for source, whole, half in (
        (feeds.at[0], feed_one, half_one), (attn, attn_ref, None), (feeds.at[1], feed_two, half_two),
    ):
        pairs = [(source, whole)]
        if half is not None:
            pairs.append((source.at[place], half))
        for part, target in pairs:
            sent.append(pltpu.make_async_copy(part, target, out_sems.at[len(sent)]))
            sent[-1].start()
    for copy in sent:
        copy.wait()


def pack_first(weights):
    return pl.pallas_call(
        pack_first_kernel,
        out_shape=shape((512, 512), BF16),
        in_specs=[pl.BlockSpec(memory_space=pl.ANY)] * 4,
        out_specs=pl.BlockSpec(memory_space=pl.ANY),
        scratch_shapes=[pltpu.VMEM((512, 512), BF16), pltpu.SemaphoreType.DMA((7,))],
        name="pack_first",
    )(*weights)


def pack_rest(info, weights):
    out = [shape(dims, BF16) for dims in ((512, 512), (1056, 512), (528, 512))]
    return pl.pallas_call(
        pack_rest_kernel,
        out_shape=tuple(out + out[1:]),
        in_specs=[pl.BlockSpec(memory_space=pltpu.SMEM)] + [pl.BlockSpec(memory_space=pl.ANY)] * 7,
        out_specs=tuple([pl.BlockSpec(memory_space=pl.ANY)] * 5),
        scratch_shapes=[
            pltpu.VMEM((512, 512), BF16), pltpu.VMEM((2, 1056, 512), BF16), pltpu.VMEM((2, 512), BF16),
            pltpu.SemaphoreType.DMA((7,)), pltpu.SemaphoreType.DMA((5,)), pltpu.SemaphoreType.DMA((5,)),
        ],
        name="pack_rest",
    )(info, *weights)


def shape(dims, dtype):
    return jax.ShapeDtypeStruct(dims, dtype)


def swap(value, axis, bit):
    size = lax.axis_size(axis)
    return lax.ppermute(value, axis, [(i, i ^ bit) for i in range(size)])


def halo_swap(core, diag, far):
    return swap(core, "tensor", 1), swap(diag, "tensor", 3), swap(far, "tensor", 2)


def tie(value, *others):
    return lax.optimization_barrier((value, *others))[0]


def far_sum(index, keep, arrived, back):
    pieces, rows = keep.shape[1:3]
    half = [shape((pieces // 2, rows, WIDTH), BF16)] * 2
    return call(
        far_sum_kernel, "far_sum", half, (index, keep, arrived, back), 1,
        [pltpu.VMEM(keep.shape[1:], BF16)] * 3 + [pltpu.SemaphoreType.DMA((3,))], True,
    )


def core_sum(keep, arrived):
    return call(
        core_sum_kernel, "core_sum", [shape(keep.shape[1:], BF16)], (keep, arrived), 0,
        [pltpu.VMEM(keep.shape[1:], BF16)] * 2 + [pltpu.SemaphoreType.DMA((2,))], True,
    )[0]


class Chain:
    def __init__(self, index, stay, go):
        self.index, self.stay, self.at = index, stay, 0
        self.arriving = swap(go, "dp", 1)

    def step(self):
        rest = self.stay.shape[1:]
        pieces = self.stay.shape[0]
        if self.at == 0:
            half = shape((pieces // 2,) + rest, BF16)
            self.stay, go = call(
                functools.partial(split_sum_kernel, 1), "split_sum", [half] * 2,
                (self.index, self.stay, self.arriving), 1,
            )
            self.arriving = swap(go, "dp", 2)
        elif self.at < 3:
            self.stay = call(
                add_kernel, "add", [shape(self.stay.shape, BF16)], (self.stay, self.arriving)
            )[0]
            if self.at == 2:
                bit = PIECES
                while bit < lax.axis_size("dp"):
                    self.stay = self.stay + swap(self.stay, "dp", bit)
                    bit *= 2
            self.arriving = swap(self.stay, "dp", 4 if self.at == 1 else 2)
        else:
            self.stay = call(
                functools.partial(join_kernel, 1), "join", [shape((pieces * 2,) + rest, BF16)],
                (self.index, self.stay, self.arriving), 1,
            )[0]
            self.arriving = swap(self.stay, "dp", 1)
        self.at += 1

    def result(self):
        assert self.at == 4
        return self.stay, self.arriving


def on_device(
    inputs, lengths, cotangent, ln_gains, ln_biases,
    w_query, w_key, w_value, w_output, w_in, b_in, w_out, b_out,
):
    assert inputs.shape == (1, ROWS, WIDTH)
    assert lax.axis_size("tensor") == SLOTS and lax.axis_size("dp") % PIECES == 0
    rank = lax.axis_index("tensor")
    position = lax.axis_index("dp")
    side = position % 2
    index = jnp.stack([side, position // 2 % 2, position // 4 % 2]).astype(jnp.int32)
    near = (rank == 1) | (rank == 2)
    length = lengths[0]
    info = jnp.stack(
        [length - rank * ROWS, 1 - rank % 2, near.astype(jnp.int32), side]
    ).astype(jnp.int32)

    spread = jnp.asarray(SPREAD, BF16)
    spread_t = jnp.asarray(SPREAD.T.copy(), BF16)
    step_inv = jnp.asarray(np.broadcast_to(1.0 / STEP[:, None], (ROWS, HEAD_PAIR)).copy(), F32)
    bias = jnp.asarray(MASKS, F32)
    step, start, kind = (jnp.asarray(t) for t in context_tables())
    owner = jnp.where(kind == 1, rank ^ 2, jnp.where(kind == 2, rank ^ 3, rank))
    place = owner * ROWS + start * step
    count = jnp.clip(length - place, 0, step)
    usable = (place >= 0) & (kind != 3) & ~((kind == 2) & near)
    count = jnp.where(usable, count, 0).astype(BF16)
    count = jnp.broadcast_to(count[:, None], (CTX, HEAD_PAIR))
    first, last, whole, halo_step = halo_tables()
    none, few = np.zeros_like(first), np.zeros_like(whole)
    tables = [
        np.concatenate([last if even else first, (first if even else last) if close else none,
                        few if close else whole, whole], axis=1)
        for even in (0, 1) for close in (0, 1)
    ]
    halo = jnp.asarray(np.stack(tables), BF16)[(1 - rank % 2) * 2 + near.astype(jnp.int32)]
    halo_step = jnp.asarray(np.broadcast_to(1.0 / halo_step[:, None], (192, HEAD_PAIR)).copy(), F32)

    def qkv_part(slots):
        return [Columns(parts, 0, 384) for parts in slots]

    def output_part(slots):
        return [Columns(parts, 384, 512) for parts in slots]

    ORDER[0] = None
    attn_own = pack_first((w_query, w_key, w_value, w_output))
    attn_two, feed_one, feed_one_half, feed_two, feed_two_half = pack_rest(
        tie(info, attn_own), (w_query, w_key, w_value, w_output, w_in, b_in, w_out)
    )
    own_far = swap(attn_own, "tensor", 2)
    own_core = swap(attn_own, "tensor", 1)
    attn_weights = [((attn_own,), (own_core,), (own_far,), (swap(own_far, "tensor", 1),))]
    here_f1 = swap(feed_one_half, "tensor", 2)
    core_w = [swap(tie(own, own_core), "tensor", 1) for own in (feed_one, attn_two, feed_two)]

    qkv_shapes = [
        shape((SLOTS, 512, 384), BF16),
        shape((SLOTS, 80, 256), BF16),
        shape((SLOTS, 96, 256), BF16),
        shape((SLOTS, 16, 256), BF16),
    ]
    block_f32 = shape((ROWS, WIDTH), F32)
    block_low = shape((ROWS, WIDTH), BF16)

    def mix(layer, qkv, halos, stream):
        return staged(
            functools.partial(mix_kernel, layer), "mix",
            [
                shape((SLOTS, CTX, 256), BF16), shape((SLOTS, ROWS, 128), BF16),
                shape((SLOTS, ROWS, 128), F32), block_f32, block_low, shape((1, WIDTH), F32),
            ],
            (
                info, qkv, *halos, count, bias, spread, stream, ln_gains, ln_biases,
                *output_part(attn_weights[layer]),
            ),
            [pltpu.VMEM((512, 256), F32)],
        )

    def mix_back(layer, grad, saved, qkv):
        ctx, mixed, inverse = saved
        return staged(
            mix_back_kernel, "mix_back",
            [
                shape((SLOTS, 512, 128), BF16),
                shape((SLOTS, ROWS, 384), F32), shape((SLOTS, 80, 256), BF16),
                shape((SLOTS, 96, 256), BF16), shape((SLOTS, 16, 256), BF16),
            ],
            (
                info, grad, *output_part(attn_weights[layer]), mixed, inverse, qkv, ctx, count, bias, spread,
                spread_t, step_inv,
            ),
            [
                pltpu.VMEM((SLOTS, ROWS, 256), BF16), pltpu.VMEM((512, 256), BF16),
                pltpu.VMEM((512, 128), F32), pltpu.VMEM((CTX, 256), F32),
            ],
        )

    normed_one, qkv_one, *pay = staged(
        first_kernel, "first", [block_low] + qkv_shapes,
        (info, inputs, ln_gains, ln_biases, *qkv_part(attn_weights[0]), spread_t, step_inv),
    )
    halos = halo_swap(*pay)
    there_f1 = swap(tie(here_f1, halos[0]), "dp", 1)
    diag_f1 = swap(tie(here_f1, halos[0]), "tensor", 1)
    far_a2 = swap(tie(attn_two, here_f1, *halos), "tensor", 2)
    *saved_one, middle_one, second_one, stat_a = mix(0, qkv_one, halos, inputs)
    here_f2 = swap(tie(feed_two_half, here_f1, stat_a), "tensor", 2)
    feed_weights = [
        ((feed_one,), (core_w[0],), (here_f1, there_f1),
         (diag_f1, swap(tie(there_f1, stat_a), "tensor", 1)))
    ]
    attn_weights.append(
        ((attn_two,), (core_w[1],), (far_a2,), (swap(tie(far_a2, stat_a), "tensor", 1),))
    )
    hidden = shape((SLOTS, ROWS, 512), BF16)
    act, slope, stat_b, stream, normed_two, qkv_two, *pay = staged(
        feed_kernel, "feed",
        [hidden, hidden, shape((2, WIDTH), F32), block_f32, block_low] + qkv_shapes,
        (
            info, second_one, middle_one, *feed_weights[0], b_out, ln_gains, ln_biases,
            *qkv_part(attn_weights[1]), spread_t, step_inv,
        ),
    )
    there_f2 = swap(tie(here_f2, there_f1, stat_b), "dp", 1)
    diag_f2 = swap(tie(here_f2, there_f1, stat_b), "tensor", 1)
    halos = halo_swap(*pay)
    feed_weights.append(
        ((feed_two,), (core_w[2],), (here_f2, there_f2),
         (diag_f2, swap(tie(there_f2, halos[0]), "tensor", 1)))
    )
    *saved_two, middle_two, second_two, stat_c = mix(1, qkv_two, halos, stream)

    def grads(matrices, extra=0):
        return [shape((2, PIECES, 64 * matrices + extra, WIDTH), BF16)] * 2

    result, stat_d, keep_f2, send_f2, hidden_two, small_a, grad = staged(
        turn_kernel, "turn",
        [block_f32, shape((2, WIDTH), F32)] + grads(2)
        + [shape((SLOTS, WIDTH), F32), shape((3, WIDTH), F32), block_f32],
        (info, second_two, middle_two, *feed_weights[1], b_out, cotangent, ln_gains),
    )
    core_f2 = swap(send_f2, "tensor", 1)
    output_two, local, *pay = mix_back(1, grad, saved_two, qkv_two)
    halos = halo_swap(*pay)
    far_f2 = core_sum(keep_f2, core_f2)
    back_f2 = swap(tie(far_f2, *halos), "tensor", 2)
    keep_a2, send_a2, keep_f1, send_f1, hidden_one, small_b, grad = staged(
        between_kernel, "between",
        grads(1) + grads(2)
        + [shape((SLOTS, WIDTH), F32), shape((5, WIDTH), F32), block_f32],
        (
            info, local, *halos, halo, halo_step, normed_two, *qkv_part(attn_weights[1]), grad,
            stream, ln_gains, act, slope, second_one, middle_one, *feed_weights[0],
            output_two,
        ),
    )
    core_f1 = swap(send_f1, "tensor", 1)
    core_a2 = swap(send_a2, "tensor", 1)
    output_one, local, *pay = mix_back(0, grad, saved_one, qkv_one)
    pay = [tie(part, back_f2) for part in pay]
    halos = halo_swap(*pay)
    chain_f2 = Chain(index, *far_sum(index, keep_f2, core_f2, back_f2))
    far_f1 = core_sum(keep_f1, core_f1)
    back_f1 = swap(tie(far_f1, *halos), "tensor", 2)
    far_a2 = core_sum(keep_a2, core_a2)
    back_a2 = swap(tie(far_a2, *halos), "tensor", 2)
    keep_a1, send_a1, input_grad = staged(
        last_kernel, "last",
        grads(1, 8) + [block_f32],
        (
            info, local, *halos, halo, halo_step, normed_one, *qkv_part(attn_weights[0]), grad,
            inputs, ln_gains, output_one, stat_a, stat_b, stat_c, stat_d, small_a, small_b,
            hidden_one, hidden_two,
        ),
    )
    core_a1 = swap(send_a1, "tensor", 1)
    far_a1 = core_sum(keep_a1, core_a1)
    back_a1 = swap(far_a1, "tensor", 2)
    chain_f2.step()
    chain_f2.step()
    chain_f1 = Chain(index, *far_sum(index, keep_f1, core_f1, back_f1))
    chain_f2.step()
    chain_a2 = Chain(index, *far_sum(index, keep_a2, core_a2, back_a2))
    chain_f2.step()
    for chain in (chain_f1, chain_a2, chain_f1):
        chain.step()
    chain_a1 = Chain(index, *far_sum(index, keep_a1, core_a1, back_a1))
    chain_a2.step()
    chain_a1.arriving = tie(chain_a1.arriving, chain_f2.arriving)
    for chain in (chain_a1, chain_f1, chain_a2, chain_a1, chain_f1, chain_a2, chain_a1):
        chain.step()
    grad_in, grad_out = staged(
        feed_result_kernel, "feed_result", [shape((2, 512, 512), F32)] * 2,
        (info, *chain_f1.result(), *chain_f2.result()),
    )
    chain_a1.stay = tie(chain_a1.stay, chain_a2.arriving)
    chain_a1.step()
    grad_query, grad_key, grad_value, grad_output, grad_b_in, gains, offsets, grad_b_out, norms = staged(
        attn_result_kernel, "attn_result",
        [shape((2, 512, 128), F32)] * 3
        + [
            shape((2, 128, 512), F32), shape((2, 512), F32), shape((2, 2, 512), F32),
            shape((2, 2, 512), F32), shape((2, 512), F32), shape((8, 128), F32),
        ],
        (info, *chain_a1.result(), *chain_a2.result()),
        [pltpu.VMEM((8 * PIECES, WIDTH), F32)],
    )
    return (
        result[None], input_grad[None], gains, offsets,
        grad_query, grad_key, grad_value, grad_output, grad_in, grad_b_in, grad_out,
        grad_b_out, norms[:6, 0],
    )


def solution(mesh):
    return jax.shard_map(
        on_device,
        mesh=mesh,
        in_specs=(
            P("dp", "tensor", None),
            P("dp"),
            P("dp", "tensor", None),
            P(),
            P(),
            P(None, None, "tensor"),
            P(None, None, "tensor"),
            P(None, None, "tensor"),
            P(None, "tensor", None),
            P(None, None, "tensor"),
            P(None, "tensor"),
            P(None, "tensor", None),
            P(),
        ),
        out_specs=(
            P("dp", "tensor", None),
            P("dp", "tensor", None),
            P(),
            P(),
            P(None, None, "tensor"),
            P(None, None, "tensor"),
            P(None, None, "tensor"),
            P(None, "tensor", None),
            P(None, None, "tensor"),
            P(None, "tensor"),
            P(None, "tensor", None),
            P(),
            P(),
        ),
        check_vma=False,
    )
```

```python
import functools
import math

import jax
import jax.numpy as jnp
import numpy as np
from jax import lax
from jax.experimental import pallas as pl
from jax.experimental.pallas import tpu as pltpu
from jax.sharding import PartitionSpec as P

F32 = jnp.float32
BF16 = jnp.bfloat16

LAYERS = 2
ROWS = 256
WIDTH = 512
PIECES = 8
SLOTS = 4
HEAD_PAIR = 128
TILE = 64
CTX = 672
NEG = -1e30

FIRST = (0, 256, 384, 448, 480)
LAST = (240, 368, 432, 464, 480)
LEVEL_SIZE = (256, 128, 64, 32, 16)
CTX_PREV = (0, 288, 448, 544, 608)
CTX_OWN = (16, 304, 464, 560, None)
CTX_NEXT = (272, 432, 528, 592, 624)
CTX_Y = 640
CTX_DIAG = 656
TILES = (
    (0, 0, 96, 0),
    (64, 64, 96, 0),
    (128, 128, 96, 0),
    (192, 192, 96, 0),
    (256, 288, 96, 1),
    (320, 352, 96, 1),
    (384, 448, 96, 1),
    (448, 544, 128, 2),
)


def dot(left, right):
    return lax.dot_general(left, right, (((1,), (0,)), ((), ())), preferred_element_type=F32)


def dot_nt(left, right):
    return lax.dot_general(left, right, (((1,), (1,)), ((), ())), preferred_element_type=F32)


def dot_tn(left, right):
    return lax.dot_general(left, right, (((0,), (0,)), ((), ())), preferred_element_type=F32)


def iota(dims, axis):
    return lax.broadcasted_iota(jnp.int32, dims, axis)


def by_level(index, values, rest):
    result = jnp.full(index.shape, rest, jnp.int32)
    for edge, value in reversed(tuple(zip((128, 192, 224, 240, 248), values))):
        result = jnp.where(index < edge, value, result)
    return result


def spread_table(transposed=False):
    shape = (ROWS, ROWS)
    position, coarse = iota(shape, 0), iota(shape, 1)
    if transposed:
        position, coarse = coarse, position
    level = by_level(coarse, (1, 2, 3, 4, 5), 0)
    base = by_level(coarse, (0, 128, 192, 224, 240), -ROWS)
    match = jnp.right_shift(position, level) == coarse - base
    return jnp.where(match, 1.0, 0.0).astype(BF16)


def step_inverse():
    index = iota((ROWS, HEAD_PAIR), 0)
    return 1.0 / by_level(index, (2, 4, 8, 16, 32), 1).astype(F32)


def fill_bias(bias_ref):
    query = iota((2 * TILE, 128), 0) % TILE
    key = iota((2 * TILE, 128), 1)
    near = (key // 16 >= query // 16) & (key // 16 <= query // 16 + 2) & (key < 96)
    far = jnp.abs((query + 16) // 8 - key // 8) >= 2
    bias_ref[0] = jnp.where(near, 0.0, NEG)
    bias_ref[1] = jnp.where(near & far, 0.0, NEG)
    half = (query % 16) // 8 + 2
    prev = (key >= 64) & (key < 80) & (jnp.abs(half - (key - 64) // 8) >= 2)
    after = (key >= 80) & (key < 96) & (jnp.abs(half - (key - 80) // 8 - 4) >= 2)
    top = ((key >= 96) & (key < 104)) | ((key >= 112) & (key < 120))
    third = (query < 32) & (key < 64) & near & far
    fourth = (query >= 32) & (query < 48) & (prev | after)
    fifth = (query >= 48) & (query < 56) & top
    bias_ref[2] = jnp.where(third | fourth | fifth, 0.0, NEG)


def fill_count(info_ref, count_ref):
    rest, close, rank = info_ref[0], info_ref[2], info_ref[4]

    def put(row, first, size, level, owner=0, usable=1):
        place = (iota((size, HEAD_PAIR), 0) + first) * 2**level + owner * ROWS
        inside = (place + rank * ROWS >= 0) & (usable == 1)
        held = jnp.where(inside, jnp.clip(rest - place, 0, 2**level), 0)
        count_ref[row : row + size, :] = held.astype(F32).astype(BF16)

    for level in range(5):
        put(CTX_PREV[level], -16, 16, level)
        put(CTX_NEXT[level], LEVEL_SIZE[level], 16, level)
        if CTX_OWN[level] is not None:
            put(CTX_OWN[level], 0, LEVEL_SIZE[level], level)
    for row, bits, usable in ((CTX_Y, 2, 1), (CTX_DIAG, 3, 1 - close)):
        place = iota((16, HEAD_PAIR), 0) * 32 + ((rank ^ bits) - rank) * ROWS
        inside = (iota((16, HEAD_PAIR), 0) < 8) & (usable == 1)
        held = jnp.where(inside, jnp.clip(rest - place, 0, 32), 0)
        count_ref[row : row + 16, :] = held.astype(F32).astype(BF16)


def halo_table(info_ref):
    even, close = info_ref[1] == 1, info_ref[2] == 1
    position, column = iota((ROWS, 192), 0), iota((ROWS, 192), 1)
    row = jnp.where(column < 80, column, column - 80)
    level, offset = row // 16, row % 16
    first = offset
    last = jnp.right_shift(ROWS, level) - 16 + offset
    core = jnp.where(even, last, first)
    diag = jnp.where(close, jnp.where(even, first, last), -1)
    top = jnp.where(offset < 8, offset, -1)
    diag_top = jnp.where(close, -1, top)
    index = jnp.where(
        column < 80, core, jnp.where(column < 160, diag, jnp.where(column < 176, diag_top, top))
    )
    level = jnp.where(column < 160, level, 5)
    return jnp.where(jnp.right_shift(position, level) == index, 1.0, 0.0).astype(BF16)


def halo_step():
    row = iota((192, HEAD_PAIR), 0)
    level = jnp.where(row < 160, jnp.where(row < 80, row, row - 80) // 16, 5)
    return 1.0 / jnp.left_shift(1, level).astype(F32)


def normalize(values):
    center = values - jnp.mean(values, axis=-1, keepdims=True)
    spread = jnp.mean(center * center, axis=-1, keepdims=True)
    scale = lax.rsqrt(spread + 1e-05)
    return center * scale, scale


def normalize_back(values, gain, grad):
    hat, scale = normalize(values)
    inner = grad * gain
    mean = jnp.mean(inner, axis=-1, keepdims=True)
    along = jnp.mean(inner * hat, axis=-1, keepdims=True)
    result = scale * (inner - mean - hat * along)
    return result, jnp.sum(grad * hat, axis=0, keepdims=True), jnp.sum(grad, axis=0, keepdims=True)


def gelu_parts(values):
    size = jnp.abs(values) * (1.0 / math.sqrt(2.0))
    ratio = 1.0 / (1.0 + 0.3275911 * size)
    bell = jnp.exp(-size * size)
    poly = ratio * (
        0.254829592
        + ratio * (-0.284496736 + ratio * (1.421413741 + ratio * (-1.453152027 + ratio * 1.061405429)))
    )
    tail = 0.5 * poly * bell
    share = jnp.where(values >= 0.0, 1.0 - tail, tail)
    slope = share + values * bell * (1.0 / math.sqrt(2.0 * math.pi))
    return values * share, slope


def row_mask(info_ref, shape):
    return lax.broadcasted_iota(jnp.int32, shape, 0) < info_ref[0]


def project(normed, weights, info_ref, spread_t, step_inv, qkv_ref, core_ref, diag_ref, far_ref):
    even = info_ref[1] == 1
    keep = row_mask(info_ref, (ROWS, 3 * HEAD_PAIR))
    column = lax.broadcasted_iota(jnp.int32, (ROWS, 3 * HEAD_PAIR), 1)
    column_scale = jnp.where(column < HEAD_PAIR, 0.125, 1.0)
    step_wide = jnp.concatenate([step_inv, step_inv], axis=1)
    for slot in range(SLOTS):
        rounded = dot(normed, weights[slot][...]).astype(BF16).astype(F32)
        exact = (jnp.where(keep, rounded, 0.0) * column_scale).astype(BF16)
        qkv_ref[slot, :ROWS, :] = exact
        pooled = dot(spread_t, exact)
        qkv_ref[slot, ROWS:, : 2 * HEAD_PAIR] = (pooled[:, : 2 * HEAD_PAIR] * step_wide).astype(BF16)
        qkv_ref[slot, ROWS:, 2 * HEAD_PAIR :] = pooled[:, 2 * HEAD_PAIR :].astype(BF16)
        for level in range(5):
            first = qkv_ref[slot, FIRST[level] : FIRST[level] + 16, HEAD_PAIR:]
            last = qkv_ref[slot, LAST[level] : LAST[level] + 16, HEAD_PAIR:]
            core_ref[slot, level * 16 : level * 16 + 16, :] = jnp.where(even, last, first)
            diag_ref[slot, level * 16 : level * 16 + 16, :] = jnp.where(even, first, last)
        qkv_ref.flush_part(slot)
        top = qkv_ref[slot, 496:512, HEAD_PAIR:]
        diag_ref[slot, 80:96, :] = top
        far_ref[slot, :, :] = top


def first_kernel(
    info_ref, x_ref, gain_ref, offset_ref, w0, w1, w2, w3,
    normed_ref, qkv_ref, core_ref, diag_ref, far_ref,
):
    hat, _ = normalize(x_ref[0].astype(F32))
    normed = (hat * gain_ref[0, 0:1, :] + offset_ref[0, 0:1, :]).astype(BF16)
    normed_ref[...] = normed
    project(
        normed, (w0, w1, w2, w3), info_ref, spread_table(True), step_inverse(),
        qkv_ref, core_ref, diag_ref, far_ref,
    )


def head_stack(values):
    column = lax.broadcasted_iota(jnp.int32, values.shape, 1) % HEAD_PAIR
    zero = jnp.zeros_like(values)
    left = jnp.where(column < HEAD_PAIR // 2, values, zero)
    right = jnp.where(column < HEAD_PAIR // 2, zero, values)
    return jnp.concatenate([left, right], axis=0)


def head_join(stacked):
    column = lax.broadcasted_iota(jnp.int32, (TILE, stacked.shape[1]), 1) % HEAD_PAIR
    return jnp.where(column < HEAD_PAIR // 2, stacked[:TILE], stacked[TILE:])


def mix_kernel(
    layer, info_ref, qkv_ref, core_ref, diag_ref, far_ref, stream_ref, gain_ref, offset_ref, w0, w1, w2, w3,
    ctx_ref, mixed_ref, inverse_ref, middle_ref, normed_ref, stat_ref,
    pair_ref, bias_ref, count_ref, spread_ref,
):
    even = info_ref[1] == 1
    near = info_ref[2] == 1
    fill_bias(bias_ref)
    fill_count(info_ref, count_ref)
    spread_ref[...] = spread_table()
    for slot in range(SLOTS):
        for level in range(5):
            rows = slice(level * 16, level * 16 + 16)
            core = core_ref[slot ^ 1, rows, :]
            diag = diag_ref[slot ^ 3, rows, :]
            diag = jnp.where(near, diag, jnp.zeros_like(diag))
            ctx_ref[slot, CTX_PREV[level] : CTX_PREV[level] + 16, :] = jnp.where(even, diag, core)
            ctx_ref[slot, CTX_NEXT[level] : CTX_NEXT[level] + 16, :] = jnp.where(even, core, diag)
            if CTX_OWN[level] is not None:
                own = slice(CTX_OWN[level], CTX_OWN[level] + LEVEL_SIZE[level])
                source = slice(FIRST[level], FIRST[level] + LEVEL_SIZE[level])
                ctx_ref[slot, own, :] = qkv_ref[slot, source, HEAD_PAIR:]
        ctx_ref[slot, CTX_Y : CTX_Y + 16, :] = far_ref[slot ^ 2, :, :]
        diag = diag_ref[slot ^ 3, 80:96, :]
        ctx_ref[slot, CTX_DIAG : CTX_DIAG + 16, :] = jnp.where(near, jnp.zeros_like(diag), diag)

    ctx_ref.flush()
    ready(qkv_ref)

    @pl.loop(0, SLOTS)
    def _(slot):
        for query_row, context_row, keys, mask in TILES:
            queries = head_stack(qkv_ref[slot, query_row : query_row + TILE, :HEAD_PAIR])
            context = slice(context_row, context_row + keys)
            scores = dot_nt(queries, ctx_ref[slot, context, :HEAD_PAIR])
            weights = jnp.exp(scores + bias_ref[mask, :, :keys]).astype(BF16)
            values = jnp.concatenate(
                [ctx_ref[slot, context, HEAD_PAIR:], count_ref[context, :]], axis=1
            )
            pair_ref[slot, query_row : query_row + TILE, :] = head_join(dot(weights, values))

    spread = spread_ref[...]
    for slot in range(SLOTS):
        coarse = pair_ref[slot, ROWS:, :]
        high = coarse.astype(BF16)
        low = (coarse - high.astype(F32)).astype(BF16)
        total = pair_ref[slot, :ROWS, :] + dot(spread, high) + dot(spread, low)
        inverse = 1.0 / total[:, HEAD_PAIR:]
        inverse_ref[slot, :, :] = inverse
        mixed_ref[slot, :, :] = (total[:, :HEAD_PAIR] * inverse).astype(BF16)
        inverse_ref.flush_part(slot)
        mixed_ref.flush_part(slot)

    attended = None
    for slot, weight in enumerate((w0, w1, w2, w3)):
        block = jnp.concatenate(
            [weight[j * 128 : (j + 1) * 128, :] for j in range(4)], axis=1
        )
        part = dot(mixed_ref[slot, :, :], block)
        attended = part if attended is None else attended + part
    keep = row_mask(info_ref, attended.shape)
    stat_ref[...] = jnp.sum(jnp.where(keep, attended * attended, 0.0), axis=0, keepdims=True)
    stream = stream_ref[0] if layer == 0 else stream_ref[...]
    middle = stream.astype(F32) + attended
    middle_ref[...] = middle
    hat, _ = normalize(middle)
    gain, offset = gain_ref[layer, 1:2, :], offset_ref[layer, 1:2, :]
    normed_ref[...] = (hat * gain + offset).astype(BF16)


def feed_kernel(
    info_ref, normed_ref, middle_ref, w0, w1, w2, w3, bias_out_ref,
    gain_ref, offset_ref, p0, p1, p2, p3,
    act_ref, slope_ref, stat_ref, stream_ref, next_ref, qkv_ref, core_ref, diag_ref, far_ref,
):
    normed = normed_ref[...]
    total = None
    for slot, weight in enumerate((w0, w1, w2, w3)):
        hidden = dot(normed, weight[:512, :]) + weight[1024:1025, :].astype(F32)
        act, slope = gelu_parts(hidden)
        act = act.astype(BF16)
        act_ref[slot, :, :] = act
        slope_ref[slot, :, :] = slope.astype(BF16)
        act_ref.flush_part(slot)
        slope_ref.flush_part(slot)
        part = dot(act, weight[512:1024, :])
        total = part if total is None else total + part
    total = total + bias_out_ref[0:1, :]
    keep = row_mask(info_ref, total.shape)
    stream = middle_ref[...] + total
    stat_ref[0:1, :] = jnp.sum(jnp.where(keep, total * total, 0.0), axis=0, keepdims=True)
    stat_ref[1:2, :] = jnp.sum(jnp.where(keep, stream * stream, 0.0), axis=0, keepdims=True)
    stream_ref[...] = stream
    hat, _ = normalize(stream)
    following = (hat * gain_ref[1, 0:1, :] + offset_ref[1, 0:1, :]).astype(BF16)
    next_ref[...] = following
    project(
        following, (p0, p1, p2, p3), info_ref, spread_table(True), step_inverse(),
        qkv_ref, core_ref, diag_ref, far_ref,
    )


def put_grads(target, matrix, value, at=0):
    low = value.astype(BF16)
    for piece in range(PIECES):
        target[piece, matrix * 64 : matrix * 64 + 64, at : at + value.shape[1]] = low[
            piece * 64 : piece * 64 + 64
        ]


def turn_kernel(
    info_ref, normed_ref, middle_ref, w0, w1, w2, w3, bias_out_ref, cotangent_ref, gain_ref,
    stream_ref, stat_ref, g0, g1, g2, g3, hidden_grad_ref, small_ref, grad_ref,
):
    normed = normed_ref[...]
    keep = row_mask(info_ref, normed.shape)
    grad = jnp.where(keep, cotangent_ref[0].astype(F32), 0.0)
    grad_low = grad.astype(BF16)
    total = None
    back = None
    for slot, weight in enumerate((w0, w1, w2, w3)):
        hidden = dot(normed, weight[:512, :]) + weight[1024:1025, :].astype(F32)
        act, slope = gelu_parts(hidden)
        act = act.astype(BF16)
        part = dot(act, weight[512:1024, :])
        total = part if total is None else total + part
        hidden_grad = (dot_nt(grad_low, weight[512:1024, :]) * slope).astype(BF16)
        part = dot_nt(hidden_grad, weight[:512, :])
        back = part if back is None else back + part
        target = (g0, g1, g2, g3)[slot]
        put_grads(target, 0, dot_tn(normed, hidden_grad))
        put_grads(target, 1, dot_tn(act, grad_low))
        target.flush()
        hidden_grad_ref[slot : slot + 1, :] = jnp.sum(hidden_grad.astype(F32), axis=0, keepdims=True)
    total = total + bias_out_ref[1:2, :]
    stream = middle_ref[...] + total
    stat_ref[0:1, :] = jnp.sum(jnp.where(keep, total * total, 0.0), axis=0, keepdims=True)
    stat_ref[1:2, :] = jnp.sum(jnp.where(keep, stream * stream, 0.0), axis=0, keepdims=True)
    stream_ref[...] = stream
    through, gain_grad, offset_grad = normalize_back(middle_ref[...], gain_ref[1, 1:2, :], back)
    small_ref[0:1, :] = gain_grad
    small_ref[1:2, :] = offset_grad
    small_ref[2:3, :] = jnp.sum(grad_low.astype(F32), axis=0, keepdims=True)
    grad_ref[...] = grad + through


def mix_back_kernel(
    info_ref, grad_ref, w0, w1, w2, w3, mixed_ref, inverse_ref, qkv_ref, ctx_ref,
    output_ref, local_ref, core_ref, diag_ref, far_ref,
    pair_ref, query_ref, context_ref, bias_ref, count_ref, spread_ref, spread_t_ref, step_ref,
):
    even = info_ref[1] == 1
    fill_bias(bias_ref)
    fill_count(info_ref, count_ref)
    spread_ref[...] = spread_table()
    spread_t_ref[...] = spread_table(True)
    step_ref[...] = step_inverse()
    grad_low = grad_ref[...].astype(BF16)
    for slot, weight in enumerate((w0, w1, w2, w3)):
        block = jnp.concatenate(
            [weight[j * 128 : (j + 1) * 128, :] for j in range(4)], axis=1
        )
        mixed = mixed_ref[slot, :, :]
        rows_grad = dot_tn(mixed, grad_low)
        for j in range(4):
            output_ref[slot, j * 128 : (j + 1) * 128, :] = rows_grad[
                :, j * 128 : (j + 1) * 128
            ].astype(BF16)
        back = dot_nt(grad_low, block).astype(BF16).astype(F32)
        scaled = back * inverse_ref[slot, :, :]
        low = jnp.concatenate([scaled, -scaled * mixed.astype(F32)], axis=1).astype(BF16)
        pair_ref[slot, :ROWS, :] = low
        pair_ref[slot, ROWS:, :] = dot(spread_t_ref[...], low).astype(BF16)

    output_ref.flush()
    ready(qkv_ref, ctx_ref)

    @pl.loop(0, SLOTS)
    def _(slot):
        held = None
        for query_row, context_row, keys, mask in TILES:
            queries = head_stack(qkv_ref[slot, query_row : query_row + TILE, :HEAD_PAIR])
            context = slice(context_row, context_row + keys)
            keyed = ctx_ref[slot, context, :HEAD_PAIR]
            scores = dot_nt(queries, keyed)
            weights = jnp.exp(scores + bias_ref[mask, :, :keys])
            values = jnp.concatenate(
                [ctx_ref[slot, context, HEAD_PAIR:], count_ref[context, :]], axis=1
            )
            upper = head_stack(pair_ref[slot, query_row : query_row + TILE, :])
            grad_scores = (dot_nt(upper, values) * weights).astype(BF16)
            query_ref[slot, query_row : query_row + TILE, :] = head_join(dot(grad_scores, keyed)) * 0.125
            key_part = dot_tn(grad_scores, queries)
            value_part = dot_tn(weights.astype(BF16), upper[:, :HEAD_PAIR])
            part = jnp.concatenate([key_part, value_part], axis=1)
            if context_row % TILE == 0 and context_row in (64, 128, 192) or context_row == 352:
                part = jnp.concatenate([part[:32] + held, part[32:]], axis=0)
            if context_row in (0, 64, 128, 288):
                held = part[TILE:]
                part = part[:TILE]
            context_ref[slot, context_row : context_row + part.shape[0], :] = part

    for slot in range(SLOTS):
        step_inv = step_ref[...]
        own = jnp.concatenate(
            [
                context_ref[slot, CTX_OWN[level] : CTX_OWN[level] + LEVEL_SIZE[level], :]
                for level in (1, 2, 3)
            ]
            + [jnp.zeros((32, 2 * HEAD_PAIR), F32)],
            axis=0,
        )
        coarse = jnp.concatenate(
            [query_ref[slot, ROWS:, :] * step_inv, own[:, :HEAD_PAIR] * step_inv, own[:, HEAD_PAIR:]],
            axis=1,
        ).astype(BF16)
        down = dot(spread_ref[...], coarse)
        local_ref[slot, :, :HEAD_PAIR] = query_ref[slot, :ROWS, :] + down[:, :HEAD_PAIR]
        local_ref[slot, :, HEAD_PAIR:] = context_ref[slot, 16 : 16 + ROWS, :] + down[:, HEAD_PAIR:]
        local_ref.flush_part(slot)
        for level in range(5):
            rows = slice(level * 16, level * 16 + 16)
            before = context_ref[slot, CTX_PREV[level] : CTX_PREV[level] + 16, :]
            after = context_ref[slot, CTX_NEXT[level] : CTX_NEXT[level] + 16, :]
            core_ref[slot, rows, :] = jnp.where(even, after, before).astype(BF16)
            diag_ref[slot, rows, :] = jnp.where(even, before, after).astype(BF16)
        diag_ref[slot, 80:96, :] = context_ref[slot, CTX_DIAG : CTX_DIAG + 16, :].astype(BF16)
        far_ref[slot, :, :] = context_ref[slot, CTX_Y : CTX_Y + 16, :].astype(BF16)
        for target in (core_ref, diag_ref, far_ref):
            target.flush_part(slot)


def project_back(
    info_ref, local_ref, core_ref, diag_ref, far_ref, normed, weights, targets, output_ref,
):
    keep = row_mask(info_ref, (ROWS, 3 * HEAD_PAIR))
    halo = halo_table(info_ref)
    scale = halo_step()
    back = None
    for slot in range(SLOTS):
        arrived = jnp.concatenate(
            [core_ref[slot ^ 1, :, :], diag_ref[slot ^ 3, :, :], far_ref[slot ^ 2, :, :]], axis=0
        ).astype(F32)
        arrived = jnp.concatenate(
            [arrived[:, :HEAD_PAIR] * scale, arrived[:, HEAD_PAIR:]], axis=1
        ).astype(BF16)
        added = dot(halo, arrived)
        local = local_ref[slot, :, :]
        whole = jnp.concatenate([local[:, :HEAD_PAIR], local[:, HEAD_PAIR:] + added], axis=1)
        low = jnp.where(keep, whole, 0.0).astype(BF16)
        put_grads(targets[slot], 0, dot_tn(normed, low))
        put_grads(targets[slot], 0, output_ref[slot, :, :], 3 * HEAD_PAIR)
        part = dot_nt(low, weights[slot][...])
        back = part if back is None else back + part
    return back


def between_kernel(
    info_ref, local_ref, core_ref, diag_ref, far_ref,
    normed_ref, p0, p1, p2, p3, grad_in_ref, stream_ref, gain_ref,
    act_ref, slope_ref, second_ref, middle_ref, w0, w1, w2, w3, output_ref,
    a0, a1, a2, a3, g0, g1, g2, g3, hidden_grad_ref, small_ref, grad_ref,
):
    back = project_back(
        info_ref, local_ref, core_ref, diag_ref, far_ref,
        normed_ref[...], (p0, p1, p2, p3), (a0, a1, a2, a3), output_ref,
    )
    for target in (a0, a1, a2, a3):
        target.flush()
    through, gain_grad, offset_grad = normalize_back(stream_ref[...], gain_ref[1, 0:1, :], back)
    small_ref[0:1, :] = gain_grad
    small_ref[1:2, :] = offset_grad
    grad = grad_in_ref[...] + through
    grad_low = grad.astype(BF16)
    small_ref[4:5, :] = jnp.sum(grad_low.astype(F32), axis=0, keepdims=True)
    second = second_ref[...]
    back = None
    for slot, weight in enumerate((w0, w1, w2, w3)):
        hidden_grad = (
            dot_nt(grad_low, weight[512:1024, :]) * slope_ref[slot, :, :].astype(F32)
        ).astype(BF16)
        part = dot_nt(hidden_grad, weight[:512, :])
        back = part if back is None else back + part
        target = (g0, g1, g2, g3)[slot]
        put_grads(target, 0, dot_tn(second, hidden_grad))
        put_grads(target, 1, dot_tn(act_ref[slot, :, :], grad_low))
        target.flush()
        hidden_grad_ref[slot : slot + 1, :] = jnp.sum(hidden_grad.astype(F32), axis=0, keepdims=True)
    through, gain_grad, offset_grad = normalize_back(middle_ref[...], gain_ref[0, 1:2, :], back)
    small_ref[2:3, :] = gain_grad
    small_ref[3:4, :] = offset_grad
    grad_ref[...] = grad + through


def last_kernel(
    info_ref, local_ref, core_ref, diag_ref, far_ref,
    normed_ref, p0, p1, p2, p3, grad_in_ref, stream_ref, gain_ref, output_ref,
    stat_a, stat_b, stat_c, stat_d, small_a, small_b, hidden_one, hidden_two,
    a0, a1, a2, a3, grad_ref,
):
    targets = (a0, a1, a2, a3)
    back = project_back(
        info_ref, local_ref, core_ref, diag_ref, far_ref,
        normed_ref[...], (p0, p1, p2, p3), targets, output_ref,
    )
    through, gain_grad, offset_grad = normalize_back(
        stream_ref[0].astype(F32), gain_ref[0, 0:1, :], back
    )
    grad_ref[...] = grad_in_ref[...] + through
    position = lax.broadcasted_iota(jnp.int32, (1, WIDTH), 1)
    valid = jnp.where(position < jnp.minimum(info_ref[0], ROWS), 1.0, 0.0)
    lines = [
        gain_grad, offset_grad,
        small_b[0:1, :], small_b[1:2, :], small_b[2:3, :], small_b[3:4, :], small_b[4:5, :],
        small_a[0:1, :], small_a[1:2, :], small_a[2:3, :],
        stat_a[...], stat_b[0:1, :], stat_b[1:2, :], stat_c[...], stat_d[0:1, :], stat_d[1:2, :],
        valid,
    ]
    zero = jnp.zeros((1, WIDTH), F32)
    for slot in range(SLOTS):
        target = targets[slot]
        own = lines + [hidden_one[slot : slot + 1, :], hidden_two[slot : slot + 1, :]]
        own = own + [zero] * (8 * PIECES - len(own))
        for piece in range(PIECES):
            rows = jnp.concatenate(own[piece * 8 : piece * 8 + 8], axis=0)
            target[piece, 64:72, :] = rows.astype(BF16)


def far_sum_kernel(index_ref, keep_ref, arrived_ref, back_ref, stay_ref, go_ref):
    side = index_ref[0]
    for place in range(PIECES // 2):
        for target, which in ((stay_ref, side), (go_ref, 1 - side)):
            piece = 2 * place + which
            target[place] = (
                keep_ref[piece].astype(F32)
                + arrived_ref[piece].astype(F32)
                + back_ref[piece].astype(F32)
            ).astype(BF16)


def split_sum_kernel(bit, index_ref, stay_ref, arrived_ref, next_stay_ref, next_go_ref):
    side = index_ref[bit]
    for place in range(next_stay_ref.shape[0]):
        for target, which in ((next_stay_ref, side), (next_go_ref, 1 - side)):
            piece = 2 * place + which
            target[place] = (stay_ref[piece].astype(F32) + arrived_ref[piece].astype(F32)).astype(BF16)


def add_kernel(stay_ref, arrived_ref, sum_ref):
    sum_ref[...] = (stay_ref[...].astype(F32) + arrived_ref[...].astype(F32)).astype(BF16)


def join_kernel(bit, index_ref, own_ref, other_ref, block_ref):
    side = index_ref[bit]
    for place in range(own_ref.shape[0]):
        block_ref[2 * place + side] = own_ref[place]
        block_ref[2 * place + 1 - side] = other_ref[place]


def placed(info_ref, own, other):
    side = info_ref[3]
    for place in range(PIECES // 2):
        yield 2 * place + side, own, place
        yield 2 * place + 1 - side, other, place


def feed_result_kernel(info_ref, own_one, other_one, own_two, other_two, in_ref, out_ref):
    for layer, pair in ((1, (own_two, other_two)), (0, (own_one, other_one))):
        ready(*pair)
        for piece, source, place in placed(info_ref, *pair):
            rows = pl.ds(pl.multiple_of(piece * 64, 64), 64)
            in_ref[layer, rows, :] = source[place, :64, :].astype(F32)
            out_ref[layer, rows, :] = source[place, 64:, :].astype(F32)
        in_ref.flush_part(layer)
        out_ref.flush_part(layer)


def attn_result_kernel(
    info_ref, own_one, other_one, own_two, other_two,
    query_ref, key_ref, value_ref, output_ref, b_in_ref, gain_ref, offset_ref, b_out_ref, norm_ref,
    lines_ref,
):
    for layer, pair in ((1, (own_two, other_two)), (0, (own_one, other_one))):
        ready(*pair)
        for piece, source, place in placed(info_ref, *pair):
            rows = pl.ds(pl.multiple_of(piece * 64, 64), 64)
            part = source[place, :64, :].astype(F32)
            for i, target in enumerate((query_ref, key_ref, value_ref)):
                target[layer, rows, :] = part[:, i * HEAD_PAIR : (i + 1) * HEAD_PAIR]
            where = pl.ds(pl.multiple_of((piece % 2) * 64, 64), 64)
            columns = pl.ds(pl.multiple_of((piece // 2) * 128, 128), 128)
            output_ref[layer, where, columns] = part[:, 3 * HEAD_PAIR :]
            if layer == 0:
                rows = pl.ds(pl.multiple_of(piece * 8, 8), 8)
                lines_ref[rows, :] = source[place, 64:, :].astype(F32)
        for target in (query_ref, key_ref, value_ref, output_ref):
            target.flush_part(layer)
    for number, (target, place) in enumerate(
        (
            (gain_ref, (0, 0)), (offset_ref, (0, 0)), (gain_ref, (1, 0)), (offset_ref, (1, 0)),
            (gain_ref, (0, 1)), (offset_ref, (0, 1)), (b_out_ref, (0,)),
            (gain_ref, (1, 1)), (offset_ref, (1, 1)), (b_out_ref, (1,)),
        )
    ):
        line = lines_ref[number : number + 1, :]
        target[place[:-1] + (slice(place[-1], place[-1] + 1), slice(None))] = line
    b_in_ref[...] = lines_ref[17:19, :]
    squares = jnp.sum(lines_ref[10:18, :], axis=1, keepdims=True)
    count = jnp.sum(lines_ref[16:17, :], axis=1, keepdims=True)
    roots = jnp.sqrt(squares / (count * WIDTH))
    lane = iota((1, 128), 1)
    row = jnp.zeros((1, 128), F32)
    for i in range(3 * LAYERS):
        row = jnp.where(lane == i, roots[i : i + 1, :], row)
    norm_ref[...] = row[:, : 3 * LAYERS]


ORDER = [None]


class Columns:
    def __init__(self, parts, start, stop):
        self.parts, self.start, self.stop = parts, start, stop


class Arriving:
    def __init__(self, ref, copies):
        self.ref, self.copies = ref, copies

    def wait(self):
        for copy in self.copies:
            copy.wait()
        self.copies = []

    def __getitem__(self, place):
        self.wait()
        return self.ref[place]


class Leaving:
    def __init__(self, ref, target, sem):
        self.ref, self.target, self.sem, self.started = ref, target, sem, False
        self.copy = pltpu.make_async_copy(ref, target, sem)

    def flush(self):
        if not self.started:
            self.copy.start()
        self.started = True

    def flush_part(self, place):
        pltpu.make_async_copy(self.ref.at[place], self.target.at[place], self.sem).start()
        self.started = True

    def __getitem__(self, place):
        return self.ref[place]

    def __setitem__(self, place, value):
        self.ref[place] = value


def ready(*arriving):
    for operand in arriving:
        operand.wait()


def staged(body, name, out, args, scratch=(), flops=0):
    args = (tie(args[0], ORDER[0]) if ORDER[0] is not None else args[0],) + tuple(args[1:])
    columns = [(arg.start, arg.stop) if isinstance(arg, Columns) else None for arg in args[1:]]
    groups = [arg.parts if isinstance(arg, Columns) else arg for arg in args[1:]]
    groups = [group if isinstance(group, tuple) else (group,) for group in groups]
    flat = [part for group in groups for part in group]
    held = []
    for group, pair in zip(groups, columns):
        dims = (group[0].shape[0] * len(group),) + group[0].shape[1:]
        if pair is not None:
            dims = (dims[0], pair[1] - pair[0])
        held.append(pltpu.VMEM(dims, group[0].dtype))

    def kernel(*refs):
        info_ref, refs = refs[0], list(refs[1:])
        sources = [refs.pop(0) for _ in flat]
        targets = [refs.pop(0) for _ in out]
        inner = [refs.pop(0) for _ in held]
        outer = [refs.pop(0) for _ in out]
        sem_in, sem_out = refs.pop(), None
        sem_out = refs.pop()
        arriving = []
        number = 0
        for group, ref, pair in zip(groups, inner, columns):
            copies = []
            for half, part in enumerate(group):
                rows = part.shape[0]
                target = ref
                if len(group) == 2:
                    side = info_ref[3] if half == 0 else 1 - info_ref[3]
                    target = ref.at[pl.ds(pl.multiple_of(side * rows, 16), rows)]
                source = sources[number]
                if pair is not None:
                    source = source.at[:, pair[0] : pair[1]]
                copies.append(pltpu.make_async_copy(source, target, sem_in.at[number]))
                copies[-1].start()
                number += 1
            arriving.append(Arriving(ref, copies))
        leaving = [
            Leaving(ref, target, sem_out.at[i])
            for i, (ref, target) in enumerate(zip(outer, targets))
        ]
        body(info_ref, *arriving, *leaving, *refs)
        for operand in arriving:
            operand.wait()
        for result in leaving:
            result.flush()
        for result in leaving:
            result.copy.wait()

    result = pl.pallas_call(
        kernel,
        out_shape=tuple(out),
        in_specs=[pl.BlockSpec(memory_space=pltpu.SMEM)]
        + [pl.BlockSpec(memory_space=pl.ANY)] * len(flat),
        out_specs=tuple(pl.BlockSpec(memory_space=pl.ANY) for _ in out),
        scratch_shapes=held
        + [pltpu.VMEM(o.shape, o.dtype) for o in out]
        + list(scratch)
        + [pltpu.SemaphoreType.DMA((len(out),)), pltpu.SemaphoreType.DMA((len(flat),))],
        cost_estimate=pl.CostEstimate(flops=1, bytes_accessed=1, transcendentals=0),
        name=name,
    )(args[0], *flat)
    ORDER[0] = result[-1]
    return result


def call(body, name, out, args, scalars=0):
    in_specs = [pl.BlockSpec(memory_space=pltpu.SMEM)] * scalars
    in_specs += [pl.BlockSpec(memory_space=pltpu.VMEM)] * (len(args) - scalars)
    args = (tie(args[0], ORDER[0]),) + tuple(args[1:])
    result = pl.pallas_call(
        body,
        out_shape=tuple(out),
        in_specs=in_specs,
        out_specs=tuple(pl.BlockSpec(memory_space=pltpu.VMEM) for _ in out),
        compiler_params=pltpu.CompilerParams(vmem_limit_bytes=4 << 20),
        cost_estimate=pl.CostEstimate(flops=1, bytes_accessed=1, transcendentals=0),
        name=name,
    )(*args)
    ORDER[0] = result[-1]
    return result


def start_attn(layer, wq, wk, wv, wo, block, sems):
    copies = []
    for i, source in enumerate((wq, wk, wv)):
        target = block.at[:, i * HEAD_PAIR : (i + 1) * HEAD_PAIR]
        copies.append(pltpu.make_async_copy(source.at[layer], target, sems.at[i]))
    for j in range(4):
        target = block.at[j * 128 : (j + 1) * 128, 3 * HEAD_PAIR :]
        source = wo.at[layer, :, j * 128 : (j + 1) * 128]
        copies.append(pltpu.make_async_copy(source, target, sems.at[3 + j]))
    for copy in copies:
        copy.start()
    return copies


def pack_kernel(
    info_ref, wq, wk, wv, wo, w_in, b_in, w_out,
    attn_one, attn_two, feed_one, half_one, feed_two, half_two,
    attn, feeds, biases, sems, feed_sems, out_sems,
):
    side = info_ref[3]
    pieces = [start_attn(layer, wq, wk, wv, wo, attn.at[layer], sems.at[layer]) for layer in range(LAYERS)]
    for layer in range(LAYERS):
        for i, source in enumerate((w_in, w_out)):
            copy = pltpu.make_async_copy(
                source.at[layer], feeds.at[layer, i * 512 : i * 512 + 512], feed_sems.at[layer * 2 + i]
            )
            copy.start()
            pieces.append([copy])
    bias_copy = pltpu.make_async_copy(b_in, biases, feed_sems.at[4])
    bias_copy.start()
    bias_copy.wait()
    row = iota((32, WIDTH), 0)
    for layer in range(LAYERS):
        line = jnp.broadcast_to(biases[layer : layer + 1, :].astype(F32), (32, WIDTH))
        feeds[layer, 1024:1056, :] = jnp.where(row == 0, line, 0.0).astype(BF16)
    place = pl.ds(pl.multiple_of(side * 528, 16), 528)
    sent = []
    for needed, parts in (
        (pieces[:1], [(attn.at[0], attn_one)]),
        (pieces[2:4], [(feeds.at[0, place], half_one), (feeds.at[0], feed_one)]),
        (pieces[1:2], [(attn.at[1], attn_two)]),
        (pieces[4:], [(feeds.at[1, place], half_two), (feeds.at[1], feed_two)]),
    ):
        for copies in needed:
            for copy in copies:
                copy.wait()
        for source, target in parts:
            sent.append(pltpu.make_async_copy(source, target, out_sems.at[len(sent)]))
            sent[-1].start()
    for copy in sent:
        copy.wait()


def pack(info, weights):
    out = [(512, 512), (512, 512), (1056, 512), (528, 512), (1056, 512), (528, 512)]
    return pl.pallas_call(
        pack_kernel,
        out_shape=tuple(shape(dims, BF16) for dims in out),
        in_specs=[pl.BlockSpec(memory_space=pltpu.SMEM)] + [pl.BlockSpec(memory_space=pl.ANY)] * 7,
        out_specs=tuple([pl.BlockSpec(memory_space=pl.ANY)] * 6),
        scratch_shapes=[
            pltpu.VMEM((2, 512, 512), BF16), pltpu.VMEM((2, 1056, 512), BF16), pltpu.VMEM((2, 512), BF16),
            pltpu.SemaphoreType.DMA((2, 7)), pltpu.SemaphoreType.DMA((5,)), pltpu.SemaphoreType.DMA((6,)),
        ],
        name="pack",
    )(info, *weights)


def shape(dims, dtype):
    return jax.ShapeDtypeStruct(dims, dtype)


def swap(value, axis, bit):
    size = lax.axis_size(axis)
    return lax.ppermute(value, axis, [(i, i ^ bit) for i in range(size)])


def halo_swap(core, diag, far):
    return swap(core, "tensor", 1), swap(diag, "tensor", 3), swap(far, "tensor", 2)


def tie(value, *others):
    return lax.optimization_barrier((value, *others))[0]


def far_sum(index, slots, arrived, back):
    pieces, rows = back.shape[:2]
    half = [shape((pieces // 2, rows, WIDTH), BF16)] * 2
    return call(far_sum_kernel, "far_sum", half, (index, slots[0], arrived[0], back), 1)


def core_swap(slots):
    return swap(slots[1], "tensor", 1), swap(slots[3], "tensor", 1)


def core_sum(slots, arrived):
    return call(add_kernel, "core_sum", [shape(slots[2].shape, BF16)], (slots[2], arrived[1]))[0]


class Chain:
    def __init__(self, index, stay, go):
        self.index, self.stay, self.at = index, stay, 0
        self.arriving = swap(go, "dp", 1)

    def step(self):
        rest = self.stay.shape[1:]
        pieces = self.stay.shape[0]
        if self.at == 0:
            half = shape((pieces // 2,) + rest, BF16)
            self.stay, go = call(
                functools.partial(split_sum_kernel, 1), "split_sum", [half] * 2,
                (self.index, self.stay, self.arriving), 1,
            )
            self.arriving = swap(go, "dp", 2)
        elif self.at < 3:
            self.stay = call(
                add_kernel, "add", [shape(self.stay.shape, BF16)], (self.stay, self.arriving)
            )[0]
            if self.at == 2:
                bit = PIECES
                while bit < lax.axis_size("dp"):
                    self.stay = self.stay + swap(self.stay, "dp", bit)
                    bit *= 2
            self.arriving = swap(self.stay, "dp", 4 if self.at == 1 else 2)
        else:
            self.stay = call(
                functools.partial(join_kernel, 1), "join", [shape((pieces * 2,) + rest, BF16)],
                (self.index, self.stay, self.arriving), 1,
            )[0]
            self.arriving = swap(self.stay, "dp", 1)
        self.at += 1

    def result(self):
        assert self.at == 4
        return self.stay, self.arriving


def on_device(
    inputs, lengths, cotangent, ln_gains, ln_biases,
    w_query, w_key, w_value, w_output, w_in, b_in, w_out, b_out,
):
    assert inputs.shape == (1, ROWS, WIDTH)
    assert lax.axis_size("tensor") == SLOTS and lax.axis_size("dp") % PIECES == 0
    rank = lax.axis_index("tensor")
    position = lax.axis_index("dp")
    side = position % 2
    index = jnp.stack([side, position // 2 % 2, position // 4 % 2]).astype(jnp.int32)
    near = (rank == 1) | (rank == 2)
    length = lengths[0]
    info = jnp.stack(
        [length - rank * ROWS, 1 - rank % 2, near.astype(jnp.int32), side, rank]
    ).astype(jnp.int32)

    def qkv_part(slots):
        return [Columns(parts, 0, 384) for parts in slots]

    def output_part(slots):
        return [Columns(parts, 384, 512) for parts in slots]

    ORDER[0] = None
    attn_own, attn_two, feed_one, feed_one_half, feed_two, feed_two_half = pack(
        info, (w_query, w_key, w_value, w_output, w_in, b_in, w_out)
    )
    own_far = swap(attn_own, "tensor", 2)
    own_core = swap(attn_own, "tensor", 1)
    attn_weights = [((attn_own,), (own_core,), (own_far,), (swap(own_far, "tensor", 1),))]
    here_f1 = swap(feed_one_half, "tensor", 2)
    core_w = [swap(tie(own, own_core), "tensor", 1) for own in (feed_one, attn_two, feed_two)]

    qkv_shapes = [
        shape((SLOTS, 512, 384), BF16),
        shape((SLOTS, 80, 256), BF16),
        shape((SLOTS, 96, 256), BF16),
        shape((SLOTS, 16, 256), BF16),
    ]
    block_f32 = shape((ROWS, WIDTH), F32)
    block_low = shape((ROWS, WIDTH), BF16)

    tables = [
        pltpu.VMEM((3, 128, 128), F32), pltpu.VMEM((CTX, 128), BF16), pltpu.VMEM((ROWS, ROWS), BF16)
    ]

    def mix(layer, qkv, halos, stream):
        return staged(
            functools.partial(mix_kernel, layer), "mix",
            [
                shape((SLOTS, CTX, 256), BF16), shape((SLOTS, ROWS, 128), BF16),
                shape((SLOTS, ROWS, 128), F32), block_f32, block_low, shape((1, WIDTH), F32),
            ],
            (
                info, qkv, *halos, stream, ln_gains, ln_biases,
                *output_part(attn_weights[layer]),
            ),
            [pltpu.VMEM((SLOTS, 512, 256), F32)] + tables,
        )

    def mix_back(layer, grad, saved, qkv):
        ctx, mixed, inverse = saved
        return staged(
            mix_back_kernel, "mix_back",
            [
                shape((SLOTS, 512, 128), BF16),
                shape((SLOTS, ROWS, 384), F32), shape((SLOTS, 80, 256), BF16),
                shape((SLOTS, 96, 256), BF16), shape((SLOTS, 16, 256), BF16),
            ],
            (
                info, grad, *output_part(attn_weights[layer]), mixed, inverse, qkv, ctx,
            ),
            [
                pltpu.VMEM((SLOTS, 512, 256), BF16), pltpu.VMEM((SLOTS, 512, 128), F32),
                pltpu.VMEM((SLOTS, CTX, 256), F32),
            ]
            + tables
            + [pltpu.VMEM((ROWS, ROWS), BF16), pltpu.VMEM((ROWS, 128), F32)],
        )

    normed_one, qkv_one, *pay = staged(
        first_kernel, "first", [block_low] + qkv_shapes,
        (info, inputs, ln_gains, ln_biases, *qkv_part(attn_weights[0])),
    )
    halos = halo_swap(*pay)
    there_f1 = swap(tie(here_f1, halos[0]), "dp", 1)
    diag_f1 = swap(tie(here_f1, halos[0]), "tensor", 1)
    far_a2 = swap(tie(attn_two, here_f1, *halos), "tensor", 2)
    *saved_one, middle_one, second_one, stat_a = mix(0, qkv_one, halos, inputs)
    here_f2 = swap(tie(feed_two_half, here_f1, stat_a), "tensor", 2)
    feed_weights = [
        ((feed_one,), (core_w[0],), (here_f1, there_f1),
         (diag_f1, swap(tie(there_f1, stat_a), "tensor", 1)))
    ]
    attn_weights.append(
        ((attn_two,), (core_w[1],), (far_a2,), (swap(tie(far_a2, stat_a), "tensor", 1),))
    )
    hidden = shape((SLOTS, ROWS, 512), BF16)
    act, slope, stat_b, stream, normed_two, qkv_two, *pay = staged(
        feed_kernel, "feed",
        [hidden, hidden, shape((2, WIDTH), F32), block_f32, block_low] + qkv_shapes,
        (
            info, second_one, middle_one, *feed_weights[0], b_out, ln_gains, ln_biases,
            *qkv_part(attn_weights[1]),
        ),
    )
    there_f2 = swap(tie(here_f2, there_f1, stat_b), "dp", 1)
    diag_f2 = swap(tie(here_f2, there_f1, stat_b), "tensor", 1)
    halos = halo_swap(*pay)
    *saved_two, middle_two, second_two, stat_c = mix(1, qkv_two, halos, stream)

    feed_weights.append(
        ((feed_two,), (core_w[2],), (here_f2, there_f2),
         (diag_f2, swap(tie(there_f2, stat_c), "tensor", 1)))
    )

    def grads(matrices, extra=0):
        return [shape((PIECES, 64 * matrices + extra, WIDTH), BF16)] * SLOTS

    result, stat_d, *f2, hidden_two, small_a, grad = staged(
        turn_kernel, "turn",
        [block_f32, shape((2, WIDTH), F32)] + grads(2)
        + [shape((SLOTS, WIDTH), F32), shape((3, WIDTH), F32), block_f32],
        (info, second_two, middle_two, *feed_weights[1], b_out, cotangent, ln_gains),
    )
    core_f2 = core_swap(f2)
    output_two, local, *pay = mix_back(1, grad, saved_two, qkv_two)
    halos = halo_swap(*pay)
    back_f2 = swap(tie(core_sum(f2, core_f2), *halos), "tensor", 2)
    *both, hidden_one, small_b, grad = staged(
        between_kernel, "between",
        grads(1) + grads(2)
        + [shape((SLOTS, WIDTH), F32), shape((5, WIDTH), F32), block_f32],
        (
            info, local, *halos, normed_two, *qkv_part(attn_weights[1]), grad,
            stream, ln_gains, act, slope, second_one, middle_one, *feed_weights[0],
            output_two,
        ),
    )
    a2, f1 = both[:SLOTS], both[SLOTS:]
    core_f1 = core_swap(f1)
    core_a2 = core_swap(a2)
    output_one, local, *pay = mix_back(0, grad, saved_one, qkv_one)
    pay = [tie(part, back_f2) for part in pay]
    halos = halo_swap(*pay)
    chain_f2 = Chain(index, *far_sum(index, f2, core_f2, back_f2))
    back_f1 = swap(tie(core_sum(f1, core_f1), *halos), "tensor", 2)
    *a1, input_grad = staged(
        last_kernel, "last",
        grads(1, 8) + [block_f32],
        (
            info, local, *halos, normed_one, *qkv_part(attn_weights[0]), grad,
            inputs, ln_gains, output_one, stat_a, stat_b, stat_c, stat_d, small_a, small_b,
            hidden_one, hidden_two,
        ),
    )
    core_a1 = core_swap(a1)
    back_a2 = swap(core_sum(a2, core_a2), "tensor", 2)
    chain_f2.step()
    chain_f2.step()
    chain_f1 = Chain(index, *far_sum(index, f1, core_f1, back_f1))
    back_a1 = swap(core_sum(a1, core_a1), "tensor", 2)
    chain_a2 = Chain(index, *far_sum(index, a2, core_a2, back_a2))
    chain_f2.step()
    chain_f1.step()
    chain_a2.step()
    chain_a1 = Chain(index, *far_sum(index, a1, core_a1, back_a1))
    chain_f2.step()
    chain_f1.step()
    chain_a2.step()
    chain_a1.step()
    chain_f1.step()
    chain_a2.arriving = tie(chain_a2.arriving, chain_f2.arriving)
    chain_a2.step()
    chain_a1.step()
    chain_f1.step()
    chain_a2.step()
    chain_a1.step()
    chain_a1.step()
    grad_in, grad_out = staged(
        feed_result_kernel, "feed_result", [shape((2, 512, 512), F32)] * 2,
        (info, *chain_f1.result(), *chain_f2.result()),
    )
    grad_query, grad_key, grad_value, grad_output, grad_b_in, gains, offsets, grad_b_out, norms = staged(
        attn_result_kernel, "attn_result",
        [shape((2, 512, 128), F32)] * 3
        + [
            shape((2, 128, 512), F32), shape((2, 512), F32), shape((2, 2, 512), F32),
            shape((2, 2, 512), F32), shape((2, 512), F32), shape((1, 3 * LAYERS), F32),
        ],
        (info, *chain_a1.result(), *chain_a2.result()),
        [pltpu.VMEM((8 * PIECES, WIDTH), F32)],
    )
    return (
        result[None], input_grad[None], gains, offsets,
        grad_query, grad_key, grad_value, grad_output, grad_in, grad_b_in, grad_out,
        grad_b_out, norms.reshape(3 * LAYERS),
    )


def solution(mesh):
    return jax.shard_map(
        on_device,
        mesh=mesh,
        in_specs=(
            P("dp", "tensor", None),
            P("dp"),
            P("dp", "tensor", None),
            P(),
            P(),
            P(None, None, "tensor"),
            P(None, None, "tensor"),
            P(None, None, "tensor"),
            P(None, "tensor", None),
            P(None, None, "tensor"),
            P(None, "tensor"),
            P(None, "tensor", None),
            P(),
        ),
        out_specs=(
            P("dp", "tensor", None),
            P("dp", "tensor", None),
            P(),
            P(),
            P(None, None, "tensor"),
            P(None, None, "tensor"),
            P(None, None, "tensor"),
            P(None, "tensor", None),
            P(None, None, "tensor"),
            P(None, "tensor"),
            P(None, "tensor", None),
            P(),
            P(),
        ),
        check_vma=False,
    )
```

```python
import functools
import math

import jax
import jax.numpy as jnp
import numpy as np
from jax import lax
from jax.experimental import pallas as pl
from jax.experimental.pallas import tpu as pltpu
from jax.sharding import PartitionSpec as P

F32 = jnp.float32
BF16 = jnp.bfloat16

LAYERS = 2
ROWS = 256
WIDTH = 512
PIECES = 8
SLOTS = 4
HEAD_PAIR = 128
TILE = 64
CTX = 672
NEG = -1e30

FIRST = (0, 256, 384, 448, 480)
LAST = (240, 368, 432, 464, 480)
LEVEL_SIZE = (256, 128, 64, 32, 16)
CTX_PREV = (0, 288, 448, 544, 608)
CTX_OWN = (16, 304, 464, 560, None)
CTX_NEXT = (272, 432, 528, 592, 624)
CTX_Y = 640
CTX_DIAG = 656
TILES = (
    (0, 0, 96, 0),
    (64, 64, 96, 0),
    (128, 128, 96, 0),
    (192, 192, 96, 0),
    (256, 288, 96, 1),
    (320, 352, 96, 1),
    (384, 448, 96, 1),
    (448, 544, 128, 2),
)


def dot(left, right):
    return lax.dot_general(left, right, (((1,), (0,)), ((), ())), preferred_element_type=F32)


def dot_nt(left, right):
    return lax.dot_general(left, right, (((1,), (1,)), ((), ())), preferred_element_type=F32)


def dot_tn(left, right):
    return lax.dot_general(left, right, (((0,), (0,)), ((), ())), preferred_element_type=F32)


def iota(dims, axis):
    return lax.broadcasted_iota(jnp.int32, dims, axis)


def by_level(index, values, rest):
    result = jnp.full(index.shape, rest, jnp.int32)
    for edge, value in reversed(tuple(zip((128, 192, 224, 240, 248), values))):
        result = jnp.where(index < edge, value, result)
    return result


def spread_table(transposed=False):
    shape = (ROWS, ROWS)
    position, coarse = iota(shape, 0), iota(shape, 1)
    if transposed:
        position, coarse = coarse, position
    level = by_level(coarse, (1, 2, 3, 4, 5), 0)
    base = by_level(coarse, (0, 128, 192, 224, 240), -ROWS)
    match = jnp.right_shift(position, level) == coarse - base
    return jnp.where(match, 1.0, 0.0).astype(BF16)


def step_inverse():
    index = iota((ROWS, HEAD_PAIR), 0)
    return 1.0 / by_level(index, (2, 4, 8, 16, 32), 1).astype(F32)


def fill_bias(bias_ref):
    query = iota((2 * TILE, 128), 0) & (TILE - 1)
    key = iota((2 * TILE, 128), 1)
    block = (key >> 4) - (query >> 4)
    near = (block >= 0) & (block <= 2) & (key < 96)
    far = jnp.abs(((query + 16) >> 3) - (key >> 3)) >= 2
    coarse = near & far
    bias_ref[0] = jnp.where(near, 0.0, NEG)
    bias_ref[1] = jnp.where(coarse, 0.0, NEG)
    half = ((query & 15) >> 3) + 2
    other = jnp.where(key < 80, (key >> 3) - 8, (key >> 3) - 6)
    fourth = (query >= 32) & (query < 48) & (key >= 64) & (key < 96) & (jnp.abs(half - other) >= 2)
    third = (query < 32) & (key < 64) & coarse
    fifth = (query >= 48) & (query < 56) & (key >= 96) & ((key & 15) < 8)
    bias_ref[2] = jnp.where(third | fourth | fifth, 0.0, NEG)


def fill_count(info_ref, count_ref):
    rest, close, rank = info_ref[0], info_ref[2], info_ref[4]

    def put(row, first, size, level, owner=0, usable=1):
        place = (iota((size, HEAD_PAIR), 0) + first) * 2**level + owner * ROWS
        inside = (place + rank * ROWS >= 0) & (usable == 1)
        held = jnp.where(inside, jnp.clip(rest - place, 0, 2**level), 0)
        count_ref[row : row + size, :] = held.astype(F32).astype(BF16)

    for level in range(5):
        put(CTX_PREV[level], -16, 16, level)
        put(CTX_NEXT[level], LEVEL_SIZE[level], 16, level)
        if CTX_OWN[level] is not None:
            put(CTX_OWN[level], 0, LEVEL_SIZE[level], level)
    for row, bits, usable in ((CTX_Y, 2, 1), (CTX_DIAG, 3, 1 - close)):
        place = iota((16, HEAD_PAIR), 0) * 32 + ((rank ^ bits) - rank) * ROWS
        inside = (iota((16, HEAD_PAIR), 0) < 8) & (usable == 1)
        held = jnp.where(inside, jnp.clip(rest - place, 0, 32), 0)
        count_ref[row : row + 16, :] = held.astype(F32).astype(BF16)


def halo_table(info_ref):
    even, close = info_ref[1] == 1, info_ref[2] == 1
    position, column = iota((ROWS, 192), 0), iota((ROWS, 192), 1)
    row = jnp.where(column < 80, column, column - 80)
    level, offset = row >> 4, row & 15
    first = offset
    last = jnp.right_shift(ROWS, level) - 16 + offset
    core = jnp.where(even, last, first)
    diag = jnp.where(close, jnp.where(even, first, last), -1)
    top = jnp.where(offset < 8, offset, -1)
    diag_top = jnp.where(close, -1, top)
    index = jnp.where(
        column < 80, core, jnp.where(column < 160, diag, jnp.where(column < 176, diag_top, top))
    )
    level = jnp.where(column < 160, level, 5)
    return jnp.where(jnp.right_shift(position, level) == index, 1.0, 0.0).astype(BF16)


def halo_step():
    row = iota((192, HEAD_PAIR), 0)
    level = jnp.where(row < 160, jnp.where(row < 80, row, row - 80) >> 4, 5)
    return 1.0 / jnp.left_shift(1, level).astype(F32)


def normalize(values):
    center = values - jnp.mean(values, axis=-1, keepdims=True)
    spread = jnp.mean(center * center, axis=-1, keepdims=True)
    scale = lax.rsqrt(spread + 1e-05)
    return center * scale, scale


def by_rows(body, sums=0):
    totals = tuple(jnp.zeros((8, WIDTH), F32) for _ in range(sums))
    for start in range(0, ROWS, 32):
        totals = body(pl.ds(start, 32), totals)
    return [jnp.sum(t, axis=0, keepdims=True) for t in totals]


def fold(total, values):
    return total + jnp.sum(values.reshape(4, 8, WIDTH), axis=0)


def valid_rows(info_ref, rows):
    return iota((32, WIDTH), 0) + rows.start < info_ref[0]


def normalize_back(values, gain, grad, totals):
    hat, scale = normalize(values)
    inner = grad * gain
    mean = jnp.mean(inner, axis=-1, keepdims=True)
    along = jnp.mean(inner * hat, axis=-1, keepdims=True)
    result = scale * (inner - mean - hat * along)
    return result, (fold(totals[0], grad * hat), fold(totals[1], grad))


def gelu_parts(values):
    size = jnp.abs(values) * (1.0 / math.sqrt(2.0))
    ratio = 1.0 / (1.0 + 0.3275911 * size)
    bell = jnp.exp(-size * size)
    poly = ratio * (
        0.254829592
        + ratio * (-0.284496736 + ratio * (1.421413741 + ratio * (-1.453152027 + ratio * 1.061405429)))
    )
    tail = 0.5 * poly * bell
    share = jnp.where(values >= 0.0, 1.0 - tail, tail)
    slope = share + values * bell * (1.0 / math.sqrt(2.0 * math.pi))
    return values * share, slope


def row_mask(info_ref, shape):
    return lax.broadcasted_iota(jnp.int32, shape, 0) < info_ref[0]


def project(
    normed, weights, info_ref, spread_t, step_inv, qkv_ref, core_ref, diag_ref, far_ref, slots=SLOTS
):
    even = info_ref[1] == 1
    keep = row_mask(info_ref, (ROWS, 3 * HEAD_PAIR))
    column = lax.broadcasted_iota(jnp.int32, (ROWS, 3 * HEAD_PAIR), 1)
    column_scale = jnp.where(column < HEAD_PAIR, 0.125, 1.0)
    step_wide = jnp.concatenate([step_inv, step_inv], axis=1)
    for slot in range(slots):
        rounded = dot(normed, weights[:, slot * 384 : (slot + 1) * 384]).astype(BF16).astype(F32)
        exact = (jnp.where(keep, rounded, 0.0) * column_scale).astype(BF16)
        qkv_ref[slot, :ROWS, :] = exact
        pooled = dot(spread_t, exact)
        qkv_ref[slot, ROWS:, : 2 * HEAD_PAIR] = (pooled[:, : 2 * HEAD_PAIR] * step_wide).astype(BF16)
        qkv_ref[slot, ROWS:, 2 * HEAD_PAIR :] = pooled[:, 2 * HEAD_PAIR :].astype(BF16)
        for level in range(5):
            first = qkv_ref[slot, FIRST[level] : FIRST[level] + 16, HEAD_PAIR:]
            last = qkv_ref[slot, LAST[level] : LAST[level] + 16, HEAD_PAIR:]
            core_ref[slot, level * 16 : level * 16 + 16, :] = jnp.where(even, last, first)
            diag_ref[slot, level * 16 : level * 16 + 16, :] = jnp.where(even, first, last)
        qkv_ref.flush_part(slot)
        top = qkv_ref[slot, 496:512, HEAD_PAIR:]
        diag_ref[slot, 80:96, :] = top
        far_ref[slot, :, :] = top


def first_near_kernel(
    info_ref, x_ref, gain_ref, offset_ref, weights,
    normed_ref, stream_ref, qkv_ref, core_ref, diag_ref, far_ref,
):
    ready(x_ref, gain_ref, offset_ref)

    def start(rows, totals):
        stream = x_ref[0, rows, :].astype(F32)
        stream_ref[rows, :] = stream
        hat, _ = normalize(stream)
        normed_ref[rows, :] = (hat * gain_ref[0, 0:1, :] + offset_ref[0, 0:1, :]).astype(BF16)
        return totals

    by_rows(start)
    normed_ref.flush()
    stream_ref.flush()
    project(
        normed_ref[...], weights, info_ref, spread_table(True), step_inverse(),
        qkv_ref, core_ref, diag_ref, far_ref, 2,
    )


def first_kernel(
    info_ref, normed_ref, weights, near_core, near_diag, near_far,
    qkv_ref, core_ref, diag_ref, far_ref, part_core, part_diag, part_far,
):
    spread_t, step_inv = spread_table(True), step_inverse()
    parts = (part_core, part_diag, part_far)
    project(normed_ref[...], weights, info_ref, spread_t, step_inv, qkv_ref, *parts, 2)
    for near, part, target in zip(
        (near_core, near_diag, near_far), parts, (core_ref, diag_ref, far_ref)
    ):
        target[0:2] = near[...]
        target[2:4] = part[...]
        target.flush()


def head_stack(values):
    column = iota(values.shape, 1) & (HEAD_PAIR - 1)
    zero = jnp.zeros_like(values)
    left = jnp.where(column < HEAD_PAIR // 2, values, zero)
    right = jnp.where(column < HEAD_PAIR // 2, zero, values)
    return jnp.concatenate([left, right], axis=0)


def head_join(stacked):
    column = iota((TILE, stacked.shape[1]), 1) & (HEAD_PAIR - 1)
    return jnp.where(column < HEAD_PAIR // 2, stacked[:TILE], stacked[TILE:])


def mix_kernel(
    layer, info_ref, qkv_ref, core_ref, diag_ref, far_ref, stream_ref, gain_ref, offset_ref, weights_ref,
    ctx_ref, mixed_ref, inverse_ref, middle_ref, normed_ref, stat_ref,
    pair_ref, sum_ref, bias_ref, count_ref, spread_ref,
):
    even = info_ref[1] == 1
    near = info_ref[2] == 1
    fill_bias(bias_ref)
    fill_count(info_ref, count_ref)
    spread_ref[...] = spread_table()
    for slot in range(SLOTS):
        for level in range(5):
            rows = slice(level * 16, level * 16 + 16)
            core = core_ref[slot ^ 1, rows, :]
            diag = diag_ref[slot ^ 3, rows, :]
            diag = jnp.where(near, diag, jnp.zeros_like(diag))
            ctx_ref[slot, CTX_PREV[level] : CTX_PREV[level] + 16, :] = jnp.where(even, diag, core)
            ctx_ref[slot, CTX_NEXT[level] : CTX_NEXT[level] + 16, :] = jnp.where(even, core, diag)
            if CTX_OWN[level] is not None:
                own = slice(CTX_OWN[level], CTX_OWN[level] + LEVEL_SIZE[level])
                source = slice(FIRST[level], FIRST[level] + LEVEL_SIZE[level])
                ctx_ref[slot, own, :] = qkv_ref[slot, source, HEAD_PAIR:]
        ctx_ref[slot, CTX_Y : CTX_Y + 16, :] = far_ref[slot ^ 2, :, :]
        diag = diag_ref[slot ^ 3, 80:96, :]
        ctx_ref[slot, CTX_DIAG : CTX_DIAG + 16, :] = jnp.where(near, jnp.zeros_like(diag), diag)

    ctx_ref.flush()
    ready(qkv_ref)
    begin(weights_ref, stream_ref, gain_ref, offset_ref)

    @pl.loop(0, SLOTS)
    def _(slot):
        for query_row, context_row, keys, mask in TILES:
            queries = head_stack(qkv_ref[slot, query_row : query_row + TILE, :HEAD_PAIR])
            context = slice(context_row, context_row + keys)
            scores = dot_nt(queries, ctx_ref[slot, context, :HEAD_PAIR])
            weights = jnp.exp(scores + bias_ref[mask, :, :keys]).astype(BF16)
            values = jnp.concatenate(
                [ctx_ref[slot, context, HEAD_PAIR:], count_ref[context, :]], axis=1
            )
            pair_ref[slot, query_row : query_row + TILE, :] = head_join(dot(weights, values))

    spread = spread_ref[...]
    for slot in range(SLOTS):
        coarse = pair_ref[slot, ROWS:, :]
        high = coarse.astype(BF16)
        low = (coarse - high.astype(F32)).astype(BF16)
        total = pair_ref[slot, :ROWS, :] + dot(spread, high) + dot(spread, low)
        inverse = 1.0 / total[:, HEAD_PAIR:]
        columns = slice(slot * HEAD_PAIR, (slot + 1) * HEAD_PAIR)
        inverse_ref[:, columns] = inverse
        mixed_ref[:, columns] = (total[:, :HEAD_PAIR] * inverse).astype(BF16)
    inverse_ref.flush()
    mixed_ref.flush()
    sum_ref[...] = dot(mixed_ref[...], weights_ref[...])
    ready(stream_ref, gain_ref, offset_ref)

    def finish(rows, totals):
        attended = sum_ref[rows, :]
        squares = jnp.where(valid_rows(info_ref, rows), attended * attended, 0.0)
        middle = stream_ref[rows, :] + attended
        middle_ref[rows, :] = middle
        hat, _ = normalize(middle)
        gain, offset = gain_ref[layer, 1:2, :], offset_ref[layer, 1:2, :]
        normed_ref[rows, :] = (hat * gain + offset).astype(BF16)
        return (fold(totals[0], squares),)

    (stat_ref[...],) = by_rows(finish, 1)


def halves(half):
    start = pl.multiple_of(half * 256, 256)
    return pl.ds(start, 256), pl.ds(512 + start, 256)


def feed_slots(normed, weights, following, act_ref, slope_ref, total_ref, fresh):
    for slot, weight in enumerate(weights):
        ready(weight)
        begin(*following[slot])
        hidden = dot(normed, weight[:512, :]) + weight[1024:1025, :].astype(F32)
        act, slope = gelu_parts(hidden)
        act = act.astype(BF16)
        act_ref[slot, :, :] = act
        slope_ref[slot, :, :] = slope.astype(BF16)
        act_ref.flush_part(slot)
        slope_ref.flush_part(slot)
        part = dot(act, weight[512:1024, :])
        if slot == 0 and fresh:
            total_ref[...] = part
        else:
            total_ref[...] += part


def feed_near_kernel(info_ref, normed_ref, w0, w1, act_ref, slope_ref, total_ref):
    feed_slots(normed_ref[...], (w0, w1), ((), ()), act_ref, slope_ref, total_ref, True)


def feed_kernel(
    info_ref, normed_ref, middle_ref, w0, w1, near_ref, bias_out_ref,
    gain_ref, offset_ref, projections,
    act_ref, slope_ref, stat_ref, stream_ref, next_ref, qkv_ref, core_ref, diag_ref, far_ref,
    total_ref,
):
    following = ((near_ref, middle_ref, bias_out_ref, gain_ref, offset_ref), (projections,))
    feed_slots(normed_ref[...], (w0, w1), following, act_ref, slope_ref, total_ref, True)
    ready(near_ref)
    ready(middle_ref, bias_out_ref, gain_ref, offset_ref)

    def finish(rows, totals):
        total_ref[rows, :] += near_ref[rows, :]
        stream, totals = add_branch(info_ref, rows, totals, total_ref, bias_out_ref[0:1, :], middle_ref)
        stream_ref[rows, :] = stream
        hat, _ = normalize(stream)
        next_ref[rows, :] = (hat * gain_ref[1, 0:1, :] + offset_ref[1, 0:1, :]).astype(BF16)
        return totals

    stat_ref[0:1, :], stat_ref[1:2, :] = by_rows(finish, 2)
    stream_ref.flush()
    next_ref.flush()
    project(
        next_ref[...], projections, info_ref, spread_table(True), step_inverse(),
        qkv_ref, core_ref, diag_ref, far_ref,
    )


def add_branch(info_ref, rows, totals, branch_ref, bias, middle_ref):
    branch = branch_ref[rows, :] + bias
    stream = middle_ref[rows, :] + branch
    valid = valid_rows(info_ref, rows)
    return stream, (
        fold(totals[0], jnp.where(valid, branch * branch, 0.0)),
        fold(totals[1], jnp.where(valid, stream * stream, 0.0)),
    )


def put_grads(target, matrix, value, at=0):
    low = value.astype(BF16)
    for piece in range(PIECES):
        target[piece, matrix * 64 : matrix * 64 + 64, at : at + value.shape[1]] = low[
            piece * 64 : piece * 64 + 64
        ]


def put_half(in_target, out_target, start, half, in_grad, out_grad):
    columns, _ = halves(half)
    low = in_grad.astype(BF16)
    for piece in range(PIECES):
        in_target[piece, :64, columns] = low[piece * 64 : piece * 64 + 64]
    low = out_grad.astype(BF16)
    for piece in range(PIECES // 2):
        place = half * (PIECES // 2) + piece
        out_target[place, start : start + 64, :] = low[piece * 64 : piece * 64 + 64]


def turn_kernel(
    info_ref, normed_ref, middle_ref, w0, w1, w2, w3, bias_out_ref, cotangent_ref, gain_ref,
    stream_ref, stat_ref, g0, g1, g2, g3, hidden_grad_ref, small_ref, grad_ref,
    total_ref, back_ref, low_ref, after,
):
    normed = normed_ref[...]
    following = ((w2,), (w3,), (middle_ref, bias_out_ref, gain_ref), after)

    def begin_grad(rows, totals):
        grad = jnp.where(valid_rows(info_ref, rows), cotangent_ref[0, rows, :].astype(F32), 0.0)
        low_ref[rows, :] = grad.astype(BF16)
        return (fold(totals[0], grad),)

    ready(cotangent_ref)
    (small_ref[2:3, :],) = by_rows(begin_grad, 1)
    grad_low = low_ref[...]
    total_ref[...] = jnp.zeros_like(total_ref)
    back_ref[...] = jnp.zeros_like(back_ref)
    for slot, weight in enumerate((w0, w1, w2, w3)):
        ready(weight)
        begin(*following[slot])
        target = (g0, g1, g2, g3)[slot]

        @pl.loop(0, 2)
        def _(half):
            columns, rows = halves(half)
            hidden = dot(normed, weight[:512, columns]) + weight[1024:1025, columns].astype(F32)
            act, slope = gelu_parts(hidden)
            act = act.astype(BF16)
            total_ref[...] += dot(act, weight[rows, :])
            hidden_grad = (dot_nt(grad_low, weight[rows, :]) * slope).astype(BF16)
            back_ref[...] += dot_nt(hidden_grad, weight[:512, columns])
            put_half(target, target, 64, half, dot_tn(normed, hidden_grad), dot_tn(act, grad_low))
            hidden_grad_ref[slot : slot + 1, columns] = jnp.sum(
                hidden_grad.astype(F32), axis=0, keepdims=True
            )

        target.flush()
    ready(middle_ref, bias_out_ref, gain_ref)

    def finish(rows, totals):
        stream, first = add_branch(
            info_ref, rows, totals[:2], total_ref, bias_out_ref[1:2, :], middle_ref
        )
        stream_ref[rows, :] = stream
        through, second = normalize_back(
            middle_ref[rows, :], gain_ref[1, 1:2, :], back_ref[rows, :], totals[2:]
        )
        grad = jnp.where(valid_rows(info_ref, rows), cotangent_ref[0, rows, :].astype(F32), 0.0) + through
        grad_ref[rows, :] = grad
        return first + second

    stat_ref[0:1, :], stat_ref[1:2, :], small_ref[0:1, :], small_ref[1:2, :] = by_rows(finish, 4)


def mix_back_kernel(
    info_ref, grad_ref, weights_ref, mixed_ref, inverse_ref, qkv_ref, ctx_ref,
    output_ref, local_ref, core_ref, diag_ref, far_ref,
    sum_ref, pair_ref, query_ref, context_ref, bias_ref, count_ref, spread_ref, spread_t_ref, step_ref,
):
    even = info_ref[1] == 1
    grad_low = grad_ref[...].astype(BF16)
    sum_ref[...] = dot_nt(grad_low, weights_ref[...])
    rows_grad = dot_tn(mixed_ref[...], grad_low).astype(BF16)
    for slot in range(SLOTS):
        for j in range(4):
            output_ref[slot, j * 128 : (j + 1) * 128, :] = rows_grad[
                slot * 128 : (slot + 1) * 128, j * 128 : (j + 1) * 128
            ]
    ready(mixed_ref, inverse_ref)

    def scale(rows, totals):
        scaled = sum_ref[rows, :].astype(BF16).astype(F32) * inverse_ref[rows, :]
        along = -scaled * mixed_ref[rows, :].astype(F32)
        for slot in range(SLOTS):
            columns = slice(slot * HEAD_PAIR, (slot + 1) * HEAD_PAIR)
            pair_ref[slot, rows, :HEAD_PAIR] = scaled[:, columns].astype(BF16)
            pair_ref[slot, rows, HEAD_PAIR:] = along[:, columns].astype(BF16)
        return totals

    by_rows(scale)
    for slot in range(SLOTS):
        pair_ref[slot, ROWS:, :] = dot(spread_t_ref[...], pair_ref[slot, :ROWS, :]).astype(BF16)

    output_ref.flush()
    ready(qkv_ref, ctx_ref)

    @pl.loop(0, SLOTS)
    def _(slot):
        held = None
        for query_row, context_row, keys, mask in TILES:
            queries = head_stack(qkv_ref[slot, query_row : query_row + TILE, :HEAD_PAIR])
            context = slice(context_row, context_row + keys)
            keyed = ctx_ref[slot, context, :HEAD_PAIR]
            scores = dot_nt(queries, keyed)
            weights = jnp.exp(scores + bias_ref[mask, :, :keys])
            values = jnp.concatenate(
                [ctx_ref[slot, context, HEAD_PAIR:], count_ref[context, :]], axis=1
            )
            upper = head_stack(pair_ref[slot, query_row : query_row + TILE, :])
            grad_scores = (dot_nt(upper, values) * weights).astype(BF16)
            query_ref[slot, query_row : query_row + TILE, :] = head_join(dot(grad_scores, keyed)) * 0.125
            key_part = dot_tn(grad_scores, queries)
            value_part = dot_tn(weights.astype(BF16), upper[:, :HEAD_PAIR])
            part = jnp.concatenate([key_part, value_part], axis=1)
            if context_row % TILE == 0 and context_row in (64, 128, 192) or context_row == 352:
                part = jnp.concatenate([part[:32] + held, part[32:]], axis=0)
            if context_row in (0, 64, 128, 288):
                held = part[TILE:]
                part = part[:TILE]
            context_ref[slot, context_row : context_row + part.shape[0], :] = part

    for slot in range(SLOTS):
        step_inv = step_ref[...]
        own = jnp.concatenate(
            [
                context_ref[slot, CTX_OWN[level] : CTX_OWN[level] + LEVEL_SIZE[level], :]
                for level in (1, 2, 3)
            ]
            + [jnp.zeros((32, 2 * HEAD_PAIR), F32)],
            axis=0,
        )
        coarse = jnp.concatenate(
            [query_ref[slot, ROWS:, :] * step_inv, own[:, :HEAD_PAIR] * step_inv, own[:, HEAD_PAIR:]],
            axis=1,
        ).astype(BF16)
        down = dot(spread_ref[...], coarse)
        local = query_ref[slot, :ROWS, :] + down[:, :HEAD_PAIR]
        local_ref[slot, :, :HEAD_PAIR] = local.astype(BF16)
        local = context_ref[slot, 16 : 16 + ROWS, :] + down[:, HEAD_PAIR:]
        local_ref[slot, :, HEAD_PAIR:] = local.astype(BF16)
        local_ref.flush_part(slot)
        for level in range(5):
            rows = slice(level * 16, level * 16 + 16)
            before = context_ref[slot, CTX_PREV[level] : CTX_PREV[level] + 16, :]
            after = context_ref[slot, CTX_NEXT[level] : CTX_NEXT[level] + 16, :]
            core_ref[slot, rows, :] = jnp.where(even, after, before).astype(BF16)
            diag_ref[slot, rows, :] = jnp.where(even, before, after).astype(BF16)
        diag_ref[slot, 80:96, :] = context_ref[slot, CTX_DIAG : CTX_DIAG + 16, :].astype(BF16)
        far_ref[slot, :, :] = context_ref[slot, CTX_Y : CTX_Y + 16, :].astype(BF16)
        for target in (core_ref, diag_ref, far_ref):
            target.flush_part(slot)


def back_tables(info_ref, bias_ref, count_ref, spread_ref, spread_t_ref, step_ref):
    fill_bias(bias_ref)
    fill_count(info_ref, count_ref)
    spread_ref[...] = spread_table()
    spread_t_ref[...] = spread_table(True)
    step_ref[...] = step_inverse()


def chained(body, inputs, outputs, scratch):
    def kernel(info_ref, *refs):
        refs = list(refs)
        parts = [[refs.pop(0) for _ in range(n)] for n in (inputs, 5, outputs, 5, scratch)]
        ins, back_ins, outs, back_outs, held = parts
        back_tables(info_ref, *refs[4:])
        body(info_ref, *ins, *outs, *held, tuple(back_ins))
        for result in outs:
            result.flush()
        mix_back_kernel(info_ref, outs[-1], *back_ins, *back_outs, *refs)

    return kernel


def project_back(
    info_ref, local_ref, core_ref, diag_ref, far_ref, normed, weights, targets, output_ref,
    low_ref, back_ref,
):
    keep = row_mask(info_ref, (ROWS, 3 * HEAD_PAIR))
    halo = halo_table(info_ref)
    scale = halo_step()
    for slot in range(SLOTS):
        arrived = jnp.concatenate(
            [core_ref[slot ^ 1, :, :], diag_ref[slot ^ 3, :, :], far_ref[slot ^ 2, :, :]], axis=0
        ).astype(F32)
        arrived = jnp.concatenate(
            [arrived[:, :HEAD_PAIR] * scale, arrived[:, HEAD_PAIR:]], axis=1
        ).astype(BF16)
        added = dot(halo, arrived)
        local = local_ref[slot, :, :].astype(F32)
        whole = jnp.concatenate([local[:, :HEAD_PAIR], local[:, HEAD_PAIR:] + added], axis=1)
        low_ref[:, slot * 384 : (slot + 1) * 384] = jnp.where(keep, whole, 0.0).astype(BF16)
    back_ref[...] = dot_nt(low_ref[...], weights[...])
    for slot in range(SLOTS):
        put_grads(targets[slot], 0, dot_tn(normed, low_ref[:, slot * 384 : (slot + 1) * 384]))
        put_grads(targets[slot], 0, output_ref[slot, :, :], 3 * HEAD_PAIR)


def between_kernel(
    info_ref, local_ref, core_ref, diag_ref, far_ref,
    normed_ref, projections, grad_in_ref, stream_ref, gain_ref,
    act_ref, slope_ref, second_ref, middle_ref, w0, w1, w2, w3, output_ref,
    a0, a1, a2, a3, g0, g1, g2, g3, o0, o1, o2, o3, hidden_grad_ref, small_ref, grad_ref,
    back_ref, mid_ref, low_ref, joint_ref, after,
):
    ready(local_ref, core_ref, diag_ref, far_ref, normed_ref, projections)
    begin(output_ref, grad_in_ref, stream_ref, gain_ref, w0, slope_ref, second_ref, act_ref)
    following = ((w2, middle_ref), (w3,), (), after)
    project_back(
        info_ref, local_ref, core_ref, diag_ref, far_ref,
        normed_ref[...], projections, (a0, a1, a2, a3), output_ref, joint_ref, back_ref,
    )
    for target in (a0, a1, a2, a3):
        target.flush()
    ready(grad_in_ref, stream_ref, gain_ref)

    def middle(rows, totals):
        through, first = normalize_back(
            stream_ref[rows, :], gain_ref[1, 0:1, :], back_ref[rows, :], totals[:2]
        )
        grad = grad_in_ref[rows, :] + through
        mid_ref[rows, :] = grad
        low = grad.astype(BF16)
        low_ref[rows, :] = low
        return first + (fold(totals[2], low.astype(F32)),)

    small_ref[0:1, :], small_ref[1:2, :], small_ref[4:5, :] = by_rows(middle, 3)
    grad_low = low_ref[...]
    second = second_ref[...]
    back_ref[...] = jnp.zeros_like(back_ref)
    ready(act_ref, slope_ref)
    begin(w1)
    for slot, weight in enumerate((w0, w1, w2, w3)):
        ready(weight)
        begin(*following[slot])
        in_target, out_target = (g0, g1, g2, g3)[slot], (o0, o1, o2, o3)[slot]

        @pl.loop(0, 2)
        def _(half):
            columns, rows = halves(half)
            slope = slope_ref[slot, :, columns].astype(F32)
            hidden_grad = (dot_nt(grad_low, weight[rows, :]) * slope).astype(BF16)
            back_ref[...] += dot_nt(hidden_grad, weight[:512, columns])
            put_half(
                in_target, out_target, 0, half, dot_tn(second, hidden_grad), dot_tn(act_ref[slot, :, columns], grad_low)
            )
            hidden_grad_ref[slot : slot + 1, columns] = jnp.sum(
                hidden_grad.astype(F32), axis=0, keepdims=True
            )

        in_target.flush()
        out_target.flush()
    ready(middle_ref)

    def finish(rows, totals):
        through, totals = normalize_back(
            middle_ref[rows, :], gain_ref[0, 1:2, :], back_ref[rows, :], totals
        )
        grad_ref[rows, :] = mid_ref[rows, :] + through
        return totals

    small_ref[2:3, :], small_ref[3:4, :] = by_rows(finish, 2)


def last_kernel(
    info_ref, local_ref, core_ref, diag_ref, far_ref,
    normed_ref, projections, grad_in_ref, stream_ref, gain_ref, output_ref,
    stat_a, stat_b, stat_c, stat_d, small_a, small_b, hidden_one, hidden_two,
    a0, a1, a2, a3, grad_ref,
    joint_ref, back_ref,
):
    targets = (a0, a1, a2, a3)
    ready(local_ref, core_ref, diag_ref, far_ref, normed_ref, projections)
    begin(
        output_ref, grad_in_ref, stream_ref, gain_ref, stat_a, stat_b, stat_c, stat_d, small_a, small_b,
        hidden_one, hidden_two,
    )
    project_back(
        info_ref, local_ref, core_ref, diag_ref, far_ref,
        normed_ref[...], projections, targets, output_ref, joint_ref, back_ref,
    )
    ready(grad_in_ref, stream_ref, gain_ref)

    def finish(rows, totals):
        through, totals = normalize_back(
            stream_ref[0, rows, :].astype(F32), gain_ref[0, 0:1, :], back_ref[rows, :], totals
        )
        grad_ref[rows, :] = grad_in_ref[rows, :] + through
        return totals

    gain_grad, offset_grad = by_rows(finish, 2)
    grad_ref.flush()
    position = lax.broadcasted_iota(jnp.int32, (1, WIDTH), 1)
    valid = jnp.where(position < jnp.minimum(info_ref[0], ROWS), 1.0, 0.0)
    lines = [
        gain_grad, offset_grad,
        small_b[0:1, :], small_b[1:2, :], small_b[2:3, :], small_b[3:4, :], small_b[4:5, :],
        small_a[0:1, :], small_a[1:2, :], small_a[2:3, :],
        stat_a[...], stat_b[0:1, :], stat_b[1:2, :], stat_c[...], stat_d[0:1, :], stat_d[1:2, :],
        valid,
    ]
    zero = jnp.zeros((1, WIDTH), F32)
    for slot in range(SLOTS):
        target = targets[slot]
        own = lines + [hidden_one[slot : slot + 1, :], hidden_two[slot : slot + 1, :]]
        own = own + [zero] * (8 * PIECES - len(own))
        for piece in range(PIECES):
            rows = jnp.concatenate(own[piece * 8 : piece * 8 + 8], axis=0)
            target[piece, 64:72, :] = rows.astype(BF16)


def far_sum_kernel(index_ref, keep_ref, arrived_ref, back_ref, stay_ref, go_ref):
    side = index_ref[0]
    for place in range(PIECES // 2):
        for target, which in ((stay_ref, side), (go_ref, 1 - side)):
            piece = 2 * place + which
            target[place] = (
                keep_ref[piece].astype(F32)
                + arrived_ref[piece].astype(F32)
                + back_ref[piece].astype(F32)
            ).astype(BF16)


def split_sum_kernel(bit, index_ref, stay_ref, arrived_ref, next_stay_ref, next_go_ref):
    side = index_ref[bit]
    for place in range(next_stay_ref.shape[0]):
        for target, which in ((next_stay_ref, side), (next_go_ref, 1 - side)):
            piece = 2 * place + which
            target[place] = (stay_ref[piece].astype(F32) + arrived_ref[piece].astype(F32)).astype(BF16)


def add_kernel(stay_ref, arrived_ref, sum_ref):
    sum_ref[...] = (stay_ref[...].astype(F32) + arrived_ref[...].astype(F32)).astype(BF16)


def join_kernel(bit, index_ref, own_ref, other_ref, block_ref):
    side = index_ref[bit]
    for place in range(own_ref.shape[0]):
        block_ref[2 * place + side] = own_ref[place]
        block_ref[2 * place + 1 - side] = other_ref[place]


def placed(info_ref, own, other):
    side = info_ref[3]
    for place in range(PIECES // 2):
        yield 2 * place + side, own, place
        yield 2 * place + 1 - side, other, place


def feed_result_kernel(
    info_ref, own_two, other_two, own_in, other_in, own_out, other_out, in_ref, out_ref
):
    ready(own_two, other_two, own_in, other_in, own_out, other_out)
    for layer, target, pair, start in (
        (1, in_ref, (own_two, other_two), 0), (1, out_ref, (own_two, other_two), 64),
        (0, in_ref, (own_in, other_in), 0), (0, out_ref, (own_out, other_out), 0),
    ):
        for piece, source, place in placed(info_ref, *pair):
            rows = pl.ds(pl.multiple_of(piece * 64, 64), 64)
            target[layer, rows, :] = source[place, start : start + 64, :].astype(F32)
        target.flush_part(layer)


def attn_result_kernel(
    info_ref, own_one, other_one, own_two, other_two,
    query_ref, key_ref, value_ref, output_ref, b_in_ref, gain_ref, offset_ref, b_out_ref, norm_ref,
    lines_ref,
):
    for layer, pair in ((1, (own_two, other_two)), (0, (own_one, other_one))):
        ready(*pair)
        for piece, source, place in placed(info_ref, *pair):
            rows = pl.ds(pl.multiple_of(piece * 64, 64), 64)
            part = source[place, :64, :].astype(F32)
            for i, target in enumerate((query_ref, key_ref, value_ref)):
                target[layer, rows, :] = part[:, i * HEAD_PAIR : (i + 1) * HEAD_PAIR]
            where = pl.ds(pl.multiple_of((piece % 2) * 64, 64), 64)
            columns = pl.ds(pl.multiple_of((piece // 2) * 128, 128), 128)
            output_ref[layer, where, columns] = part[:, 3 * HEAD_PAIR :]
            if layer == 0:
                rows = pl.ds(pl.multiple_of(piece * 8, 8), 8)
                lines_ref[rows, :] = source[place, 64:, :].astype(F32)
        for target in (query_ref, key_ref, value_ref, output_ref):
            target.flush_part(layer)
    for number, (target, place) in enumerate(
        (
            (gain_ref, (0, 0)), (offset_ref, (0, 0)), (gain_ref, (1, 0)), (offset_ref, (1, 0)),
            (gain_ref, (0, 1)), (offset_ref, (0, 1)), (b_out_ref, (0,)),
            (gain_ref, (1, 1)), (offset_ref, (1, 1)), (b_out_ref, (1,)),
        )
    ):
        line = lines_ref[number : number + 1, :]
        target[place[:-1] + (slice(place[-1], place[-1] + 1), slice(None))] = line
    b_in_ref[...] = lines_ref[17:19, :]
    squares = jnp.sum(lines_ref[10:18, :], axis=1, keepdims=True)
    count = jnp.sum(lines_ref[16:17, :], axis=1, keepdims=True)
    roots = jnp.sqrt(squares / (count * WIDTH))
    lane = iota((1, 128), 1)
    row = jnp.zeros((1, 128), F32)
    for i in range(3 * LAYERS):
        row = jnp.where(lane == i, roots[i : i + 1, :], row)
    norm_ref[...] = row[:, : 3 * LAYERS]


AFTER = []
ORDER = [None]


def in_order(value):
    before = [other for other in (ORDER[0], *AFTER) if other is not None]
    AFTER.clear()
    return tie(value, *before) if before else value


class Plan:
    def __init__(self, parts, dims, moves):
        self.parts, self.dims, self.moves = list(parts), dims, moves


def everything(value):
    return Plan([value], value.shape, [(0, None, None)])


def feed_plan(parts):
    if len(parts) == 1:
        return everything(parts[0])
    rows, width = parts[0].shape

    def half(number):
        def place(info_ref):
            side = info_ref[3] if number == 0 else 1 - info_ref[3]
            return pl.ds(pl.multiple_of(side * rows, 16), rows), slice(None)

        return place

    return Plan(parts, (2 * rows, width), [(i, None, half(i)) for i in range(2)])


def qkv_plan(slots):
    parts, moves = [], []
    for slot, group in enumerate(slots):
        rows = 512 // len(group)
        for i, part in enumerate(group):
            place = (slice(i * rows, (i + 1) * rows), slice(slot * 384, (slot + 1) * 384))
            moves.append((len(parts), (slice(None), slice(0, 384)), place))
            parts.append(part)
    return Plan(parts, (512, 384 * len(slots)), moves)


def output_plan(slots):
    parts, moves = [], []
    for slot, group in enumerate(slots):
        for j in range(4):
            rows = 4 // len(group)
            start = j % rows * 128
            source = (slice(start, start + 128), slice(384, 512))
            number = len(parts) + j // rows
            place = (slice(slot * 128, (slot + 1) * 128), slice(j * 128, (j + 1) * 128))
            moves.append((number, source, place))
        parts += group
    return Plan(parts, (512, 512), moves)


class Late:
    def __init__(self, arg):
        self.arg = arg


class Arriving:
    def __init__(self, ref, make, late):
        self.ref, self.make, self.copies = ref, make, None
        if not late:
            self.start()

    def start(self):
        if self.copies is None:
            self.copies = self.make()
            for copy in self.copies:
                copy.start()

    def wait(self):
        self.start()
        for copy in self.copies:
            copy.wait()
        self.copies = []

    def __getitem__(self, place):
        self.wait()
        return self.ref[place]


def begin(*arriving):
    for operand in arriving:
        operand.start()


class Leaving:
    def __init__(self, ref, target, sem):
        self.ref, self.target, self.sem, self.started = ref, target, sem, False
        self.copy = pltpu.make_async_copy(ref, target, sem)

    def flush(self):
        if not self.started:
            self.copy.start()
        self.started = True

    def flush_part(self, place):
        pltpu.make_async_copy(self.ref.at[place], self.target.at[place], self.sem).start()
        self.started = True

    def __getitem__(self, place):
        return self.ref[place]

    def __setitem__(self, place, value):
        self.ref[place] = value


def ready(*arriving):
    for operand in arriving:
        operand.wait()


def staged(body, name, out, args, scratch=(), flops=0):
    args = (in_order(args[0]),) + tuple(args[1:])
    late = [isinstance(arg, Late) for arg in args[1:]]
    plans = [arg.arg if isinstance(arg, Late) else arg for arg in args[1:]]
    plans = [plan if isinstance(plan, Plan) else everything(plan) for plan in plans]
    flat = [part for plan in plans for part in plan.parts]
    count = sum(len(plan.moves) for plan in plans)
    held = [pltpu.VMEM(plan.dims, plan.parts[0].dtype) for plan in plans]

    def kernel(*refs):
        info_ref, refs = refs[0], list(refs[1:])
        sources = [refs.pop(0) for _ in flat]
        targets = [refs.pop(0) for _ in out]
        inner = [refs.pop(0) for _ in held]
        outer = [refs.pop(0) for _ in out]
        sem_in = refs.pop()
        sem_out = refs.pop()
        arriving = []
        start, number = 0, 0
        for plan, ref, later in zip(plans, inner, late):

            def make(plan=plan, ref=ref, start=start, number=number):
                copies = []
                for i, (part, source_place, place) in enumerate(plan.moves):
                    source, target = sources[start + part], ref
                    if source_place is not None:
                        source = source.at[source_place]
                    if place is not None:
                        target = target.at[place(info_ref) if callable(place) else place]
                    copies.append(pltpu.make_async_copy(source, target, sem_in.at[number + i]))
                return copies

            arriving.append(Arriving(ref, make, later))
            start += len(plan.parts)
            number += len(plan.moves)
        leaving = [
            Leaving(ref, target, sem_out.at[i])
            for i, (ref, target) in enumerate(zip(outer, targets))
        ]
        body(info_ref, *arriving, *leaving, *refs)
        for operand in arriving:
            operand.wait()
        for result in leaving:
            result.flush()
        for result in leaving:
            result.copy.wait()

    result = pl.pallas_call(
        kernel,
        out_shape=tuple(out),
        in_specs=[pl.BlockSpec(memory_space=pltpu.SMEM)]
        + [pl.BlockSpec(memory_space=pl.ANY)] * len(flat),
        out_specs=tuple(pl.BlockSpec(memory_space=pl.ANY) for _ in out),
        scratch_shapes=held
        + [pltpu.VMEM(o.shape, o.dtype) for o in out]
        + list(scratch)
        + [pltpu.SemaphoreType.DMA((len(out),)), pltpu.SemaphoreType.DMA((count,))],
        cost_estimate=pl.CostEstimate(flops=1, bytes_accessed=1, transcendentals=0),
        name=name,
    )(args[0], *flat)
    ORDER[0] = result[-1]
    return result


def call(body, name, out, args, scalars=0):
    in_specs = [pl.BlockSpec(memory_space=pltpu.SMEM)] * scalars
    in_specs += [pl.BlockSpec(memory_space=pltpu.VMEM)] * (len(args) - scalars)
    args = (in_order(args[0]),) + tuple(args[1:])
    result = pl.pallas_call(
        body,
        out_shape=tuple(out),
        in_specs=in_specs,
        out_specs=tuple(pl.BlockSpec(memory_space=pltpu.VMEM) for _ in out),
        compiler_params=pltpu.CompilerParams(vmem_limit_bytes=4 << 20),
        cost_estimate=pl.CostEstimate(flops=1, bytes_accessed=1, transcendentals=0),
        name=name,
    )(*args)
    ORDER[0] = result[-1]
    return result


def start_attn(layer, wq, wk, wv, wo, block, sems):
    copies = []
    for i, source in enumerate((wq, wk, wv)):
        target = block.at[:, i * HEAD_PAIR : (i + 1) * HEAD_PAIR]
        copies.append(pltpu.make_async_copy(source.at[layer], target, sems.at[i]))
    for j in range(4):
        target = block.at[j * 128 : (j + 1) * 128, 3 * HEAD_PAIR :]
        source = wo.at[layer, :, j * 128 : (j + 1) * 128]
        copies.append(pltpu.make_async_copy(source, target, sems.at[3 + j]))
    for copy in copies:
        copy.start()
    return copies


def pack_first_kernel(wq, wk, wv, wo, own_ref, block, sems):
    for copy in start_attn(0, wq, wk, wv, wo, block, sems):
        copy.wait()
    copy = pltpu.make_async_copy(block, own_ref, sems.at[0])
    copy.start()
    copy.wait()


def pack_rest_kernel(
    info_ref, wq, wk, wv, wo, w_in, b_in, w_out,
    attn_two, feed_one, half_one, feed_two, half_two,
    attn, feeds, biases, sems, feed_sems, out_sems,
):
    side = info_ref[3]
    attn_copies = start_attn(1, wq, wk, wv, wo, attn, sems)
    feed_copies = []
    for layer in range(LAYERS):
        for i, source in enumerate((w_in, w_out)):
            copy = pltpu.make_async_copy(
                source.at[layer], feeds.at[layer, i * 512 : i * 512 + 512], feed_sems.at[layer * 2 + i]
            )
            copy.start()
            feed_copies.append(copy)
    bias_copy = pltpu.make_async_copy(b_in, biases, feed_sems.at[4])
    bias_copy.start()
    bias_copy.wait()
    row = iota((32, WIDTH), 0)
    for layer in range(LAYERS):
        line = jnp.broadcast_to(biases[layer : layer + 1, :].astype(F32), (32, WIDTH))
        feeds[layer, 1024:1056, :] = jnp.where(row == 0, line, 0.0).astype(BF16)
    place = pl.ds(pl.multiple_of(side * 528, 16), 528)
    sent = []
    for copies, parts in (
        (feed_copies[:2], [(feeds.at[0, place], half_one), (feeds.at[0], feed_one)]),
        (attn_copies, [(attn, attn_two)]),
        (feed_copies[2:], [(feeds.at[1, place], half_two), (feeds.at[1], feed_two)]),
    ):
        for copy in copies:
            copy.wait()
        for source, target in parts:
            sent.append(pltpu.make_async_copy(source, target, out_sems.at[len(sent)]))
            sent[-1].start()
    for copy in sent:
        copy.wait()


def pack_first(weights):
    return pl.pallas_call(
        pack_first_kernel,
        out_shape=shape((512, 512), BF16),
        in_specs=[pl.BlockSpec(memory_space=pl.ANY)] * 4,
        out_specs=pl.BlockSpec(memory_space=pl.ANY),
        scratch_shapes=[pltpu.VMEM((512, 512), BF16), pltpu.SemaphoreType.DMA((7,))],
        name="pack_first",
    )(*weights)


def pack_rest(info, weights):
    out = [(512, 512), (1056, 512), (528, 512), (1056, 512), (528, 512)]
    return pl.pallas_call(
        pack_rest_kernel,
        out_shape=tuple(shape(dims, BF16) for dims in out),
        in_specs=[pl.BlockSpec(memory_space=pltpu.SMEM)] + [pl.BlockSpec(memory_space=pl.ANY)] * 7,
        out_specs=tuple([pl.BlockSpec(memory_space=pl.ANY)] * 5),
        scratch_shapes=[
            pltpu.VMEM((512, 512), BF16),
            pltpu.VMEM((2, 1056, 512), BF16), pltpu.VMEM((2, 512), BF16),
            pltpu.SemaphoreType.DMA((7,)), pltpu.SemaphoreType.DMA((5,)), pltpu.SemaphoreType.DMA((5,)),
        ],
        name="pack_rest",
    )(info, *weights)


def shape(dims, dtype):
    return jax.ShapeDtypeStruct(dims, dtype)


def swap(value, axis, bit):
    size = lax.axis_size(axis)
    return lax.ppermute(value, axis, [(i, i ^ bit) for i in range(size)])


def halo_swap(core, diag, far):
    return swap(core, "tensor", 1), swap(diag, "tensor", 3), swap(far, "tensor", 2)


def tie(value, *others):
    return lax.optimization_barrier((value, *others))[0]


def far_sum(index, slots, arrived, back):
    pieces, rows = back.shape[:2]
    half = [shape((pieces // 2, rows, WIDTH), BF16)] * 2
    return call(far_sum_kernel, "far_sum", half, (index, slots[0], arrived[0], back), 1)


def core_swap(slots):
    far = swap(slots[3], "tensor", 1)
    return swap(slots[1], "tensor", 1), far


def core_sum(slots, arrived):
    return call(add_kernel, "core_sum", [shape(slots[2].shape, BF16)], (slots[2], arrived[1]))[0]


class Chain:
    def __init__(self, index, stay, go):
        self.index, self.stay, self.at = index, stay, 0
        self.arriving = swap(go, "dp", 1)

    def step(self):
        rest = self.stay.shape[1:]
        pieces = self.stay.shape[0]
        if self.at == 0:
            half = shape((pieces // 2,) + rest, BF16)
            self.stay, go = call(
                functools.partial(split_sum_kernel, 1), "split_sum", [half] * 2,
                (self.index, self.stay, self.arriving), 1,
            )
            self.arriving = swap(go, "dp", 2)
        elif self.at < 3:
            self.stay = call(
                add_kernel, "add", [shape(self.stay.shape, BF16)], (self.stay, self.arriving)
            )[0]
            if self.at == 2:
                bit = PIECES
                while bit < lax.axis_size("dp"):
                    self.stay = self.stay + swap(self.stay, "dp", bit)
                    bit *= 2
            self.arriving = swap(self.stay, "dp", 4 if self.at == 1 else 2)
        else:
            self.stay = call(
                functools.partial(join_kernel, 1), "join", [shape((pieces * 2,) + rest, BF16)],
                (self.index, self.stay, self.arriving), 1,
            )[0]
            self.arriving = swap(self.stay, "dp", 1)
        self.at += 1

    def result(self):
        assert self.at == 4
        return self.stay, self.arriving


class Flow:
    def __init__(self, index, slots, arrived, back=None, halos=()):
        self.index, self.slots, self.arrived, self.halos = index, slots, arrived, halos
        self.back, self.chain, self.at = back, None, 0 if back is None else 1

    def step(self):
        if self.at == 0:
            far = core_sum(self.slots, self.arrived)
            self.back = swap(tie(far, *self.halos) if self.halos else far, "tensor", 2)
        elif self.at == 1:
            self.chain = Chain(self.index, *far_sum(self.index, self.slots, self.arrived, self.back))
        elif self.at < 6:
            self.chain.step()
        else:
            AFTER.append(self.chain.arriving)
        self.at += 1


def on_device(
    inputs, lengths, cotangent, ln_gains, ln_biases,
    w_query, w_key, w_value, w_output, w_in, b_in, w_out, b_out,
):
    assert inputs.shape == (1, ROWS, WIDTH)
    assert lax.axis_size("tensor") == SLOTS and lax.axis_size("dp") % PIECES == 0
    rank = lax.axis_index("tensor")
    position = lax.axis_index("dp")
    side = position % 2
    index = jnp.stack([side, position // 2 % 2, position // 4 % 2]).astype(jnp.int32)
    near = (rank == 1) | (rank == 2)
    length = lengths[0]
    info = jnp.stack(
        [length - rank * ROWS, 1 - rank % 2, near.astype(jnp.int32), side, rank]
    ).astype(jnp.int32)

    def later(*values):
        return [Late(value) for value in values]

    ORDER[0] = None
    AFTER.clear()
    attn_own = pack_first((w_query, w_key, w_value, w_output))
    attn_two, feed_one, feed_one_half, feed_two, feed_two_half = pack_rest(
        tie(info, attn_own), (w_query, w_key, w_value, w_output, w_in, b_in, w_out)
    )
    own_far = swap(attn_own, "tensor", 2)
    own_core = swap(attn_own, "tensor", 1)
    slots = ((attn_own,), (own_core,))
    here_f1 = swap(feed_one_half, "tensor", 2)
    core_w = [swap(tie(own, own_core), "tensor", 1) for own in (feed_one, attn_two, feed_two)]

    qkv_shapes = [
        shape((SLOTS, 512, 384), BF16),
        shape((SLOTS, 80, 256), BF16),
        shape((SLOTS, 96, 256), BF16),
        shape((SLOTS, 16, 256), BF16),
    ]
    block_f32 = shape((ROWS, WIDTH), F32)
    block_low = shape((ROWS, WIDTH), BF16)

    sums = pltpu.VMEM((ROWS, WIDTH), F32)
    tables = [
        pltpu.VMEM((3, 128, 128), F32), pltpu.VMEM((CTX, 128), BF16), pltpu.VMEM((ROWS, ROWS), BF16)
    ]

    def mix(layer, qkv, halos, stream):
        return staged(
            functools.partial(mix_kernel, layer), "mix",
            [
                shape((SLOTS, CTX, 256), BF16), block_low, block_f32, block_f32, block_low, shape((1, WIDTH), F32),
            ],
            (
                info, qkv, *halos,
                *later(stream, ln_gains, ln_biases, output_weights[layer]),
            ),
            [pltpu.VMEM((SLOTS, 512, 256), F32), sums] + tables,
        )

    def with_mix_back(layer, body, name, out, args, held, saved, qkv):
        ctx, mixed, inverse = saved
        result = staged(
            chained(body, len(args), len(out), len(held)), name,
            list(out)
            + [
                shape((SLOTS, 512, 128), BF16),
                shape((SLOTS, ROWS, 384), BF16), shape((SLOTS, 80, 256), BF16),
                shape((SLOTS, 96, 256), BF16), shape((SLOTS, 16, 256), BF16),
            ],
            (info, *args, *later(output_weights[layer], mixed, inverse, qkv, ctx)),
            list(held)
            + [
                sums, pltpu.VMEM((SLOTS, 512, 256), BF16), pltpu.VMEM((SLOTS, 512, 128), F32),
                pltpu.VMEM((SLOTS, CTX, 256), F32),
            ]
            + tables
            + [pltpu.VMEM((ROWS, ROWS), BF16), pltpu.VMEM((ROWS, 128), F32)],
        )
        return result[: len(out)], result[len(out) :]

    near_shapes = [shape((2,) + dims.shape[1:], BF16) for dims in qkv_shapes]
    normed_one, stream_one, qkv_near, *pay_near = staged(
        first_near_kernel, "first_near", [block_low, block_f32] + near_shapes,
        (tie(info, feed_one_half), inputs, ln_gains, ln_biases, qkv_plan(slots[:2])),
    )
    own_diag = tuple(
        swap(part, "tensor", 1)
        for part in (tie(own_far, normed_one)[i * 256 : i * 256 + 256] for i in range(2))
    )
    slots += ((own_far,), own_diag)
    qkv_weights, output_weights = [qkv_plan(slots)], [output_plan(slots)]
    qkv_far, *pay = staged(
        first_kernel, "first", near_shapes[:1] + qkv_shapes[1:],
        (info, normed_one, qkv_plan(slots[2:]), *pay_near),
        [pltpu.VMEM(dims.shape, BF16) for dims in near_shapes[1:]],
    )
    qkv_one = Plan(
        (qkv_near, qkv_far), (SLOTS, 512, 384),
        [(0, None, (slice(0, 2),)), (1, None, (slice(2, 4),))],
    )
    halos = halo_swap(*pay)
    there_f1 = swap(tie(here_f1, halos[0]), "dp", 1)
    diag_f1 = swap(tie(here_f1, halos[0]), "tensor", 1)
    far_a2 = swap(tie(attn_two, here_f1, *halos), "tensor", 2)
    *saved_one, middle_one, second_one, stat_a = mix(0, qkv_one, halos, stream_one)
    here_f2 = swap(tie(feed_two_half, here_f1, stat_a), "tensor", 2)
    feed_weights = [[
        feed_plan(parts)
        for parts in (
            (feed_one,), (core_w[0],), (here_f1, there_f1),
            (diag_f1, swap(tie(there_f1, stat_a), "tensor", 1)),
        )
    ]]
    hidden = shape((SLOTS // 2, ROWS, 512), BF16)
    act_near, slope_near, total_near = staged(
        feed_near_kernel, "feed_near", [hidden, hidden, block_f32],
        (info, second_one, *feed_weights[0][:2]),
    )
    slots = (
        (attn_two,), (core_w[1],), (far_a2,), (swap(tie(far_a2, total_near), "tensor", 1),)
    )
    qkv_weights.append(qkv_plan(slots))
    output_weights.append(output_plan(slots))
    act_far, slope_far, stat_b, stream, normed_two, qkv_two, *pay = staged(
        feed_kernel, "feed",
        [hidden, hidden, shape((2, WIDTH), F32), block_f32, block_low] + qkv_shapes,
        (
            info, second_one, Late(middle_one), *feed_weights[0][2:],
            *later(total_near, b_out, ln_gains, ln_biases, qkv_weights[1]),
        ),
        [sums],
    )
    act, slope = (
        Plan(
            pair, (SLOTS, ROWS, 512),
            [(0, None, (slice(0, 2),)), (1, None, (slice(2, 4),))],
        )
        for pair in ((act_near, act_far), (slope_near, slope_far))
    )
    there_f2 = swap(tie(here_f2, there_f1, stat_b), "dp", 1)
    diag_f2 = swap(tie(here_f2, there_f1, stat_b), "tensor", 1)
    halos = halo_swap(*pay)
    *saved_two, middle_two, second_two, stat_c = mix(1, qkv_two, halos, stream)

    feed_weights.append([
        feed_plan(parts)
        for parts in (
            (feed_two,), (core_w[2],), (here_f2, there_f2),
            (diag_f2, swap(tie(there_f2, stat_c), "tensor", 1)),
        )
    ])

    def grads(matrices, extra=0):
        return [shape((PIECES, 64 * matrices + extra, WIDTH), BF16)] * SLOTS

    (result, stat_d, *f2, hidden_two, small_a, grad), (output_two, local, *pay) = with_mix_back(
        1, turn_kernel, "turn",
        [block_f32, shape((2, WIDTH), F32)] + grads(2)
        + [shape((SLOTS, WIDTH), F32), shape((3, WIDTH), F32), block_f32],
        (
            second_two, Late(middle_two), *feed_weights[1][:2], *later(*feed_weights[1][2:]),
            Late(b_out), cotangent, Late(ln_gains),
        ),
        [sums] * 2 + [pltpu.VMEM((ROWS, WIDTH), BF16)], saved_two, qkv_two,
    )
    halos = halo_swap(*pay)
    core_f2 = core_swap(f2)
    back_f2 = swap(tie(core_sum(f2, core_f2), *halos), "tensor", 2)
    (*both, hidden_one, small_b, grad), (output_one, local, *pay) = with_mix_back(
        0, between_kernel, "between",
        grads(1) * 3 + [shape((SLOTS, WIDTH), F32), shape((5, WIDTH), F32), block_f32],
        (
            local, *halos, normed_two, qkv_weights[1],
            *later(
                grad, stream, ln_gains, act, slope, second_one, middle_one, *feed_weights[0], output_two
            ),
        ),
        [sums] * 2 + [pltpu.VMEM((ROWS, WIDTH), BF16), pltpu.VMEM((ROWS, 384 * SLOTS), BF16)],
        saved_one, qkv_one,
    )
    a2, f1, g1 = both[:SLOTS], both[SLOTS : 2 * SLOTS], both[2 * SLOTS :]
    pay = [tie(part, back_f2) for part in pay]
    halos = halo_swap(*pay)
    core_f1 = core_swap(f1)
    core_a2 = core_swap(a2)
    core_g1 = core_swap(g1)
    f2 = Flow(index, f2, core_f2, back_f2)
    f1 = Flow(index, f1, core_f1, halos=halos)
    a2 = Flow(index, a2, core_a2, halos=halos)
    g1 = Flow(index, g1, core_g1, halos=halos)
    for flow in (f2, g1,):
        flow.step()
    *a1, input_grad = staged(
        last_kernel, "last",
        grads(1, 8) + [block_f32],
        (
            info, local, *halos, normed_one, qkv_weights[0],
            *later(
                grad, inputs, ln_gains, output_one, stat_a, stat_b, stat_c, stat_d, small_a, small_b,
                hidden_one, hidden_two,
            ),
        ),
        [pltpu.VMEM((ROWS, 384 * SLOTS), BF16), sums],
    )
    a1 = Flow(index, a1, core_swap(a1))
    for flow in (
        f1, f2, g1, a1, f2, g1, f1, a2, a1, f1, g1, f2,
        f1, a2, a1, f2, f1, a2, a1, g1, f1, a2, a1, g1,
        f2, f1, a2, a1, g1,
    ):
        flow.step()
    a2.step()
    grad_in, grad_out = staged(
        feed_result_kernel, "feed_result", [shape((2, 512, 512), F32)] * 2,
        (info, *f2.chain.result(), *f1.chain.result(), *g1.chain.result()),
    )
    a1.step()
    a2.step()
    (
        grad_query, grad_key, grad_value, grad_output, grad_b_in, gains, offsets, grad_b_out, norms
    ) = staged(
        attn_result_kernel, "attn_result",
        [shape((2, 512, 128), F32)] * 3
        + [
            shape((2, 128, 512), F32), shape((2, 512), F32), shape((2, 2, 512), F32),
            shape((2, 2, 512), F32), shape((2, 512), F32), shape((1, 3 * LAYERS), F32),
        ],
        (info, *a1.chain.result(), *a2.chain.result()),
        [pltpu.VMEM((8 * PIECES, WIDTH), F32)],
    )
    return (
        result[None], input_grad[None], gains, offsets,
        grad_query, grad_key, grad_value, grad_output, grad_in, grad_b_in, grad_out,
        grad_b_out, norms.reshape(3 * LAYERS),
    )


def solution(mesh):
    return jax.shard_map(
        on_device,
        mesh=mesh,
        in_specs=(
            P("dp", "tensor", None),
            P("dp"),
            P("dp", "tensor", None),
            P(),
            P(),
            P(None, None, "tensor"),
            P(None, None, "tensor"),
            P(None, None, "tensor"),
            P(None, "tensor", None),
            P(None, None, "tensor"),
            P(None, "tensor"),
            P(None, "tensor", None),
            P(),
        ),
        out_specs=(
            P("dp", "tensor", None),
            P("dp", "tensor", None),
            P(),
            P(),
            P(None, None, "tensor"),
            P(None, None, "tensor"),
            P(None, None, "tensor"),
            P(None, "tensor", None),
            P(None, None, "tensor"),
            P(None, "tensor"),
            P(None, "tensor", None),
            P(),
            P(),
        ),
        check_vma=False,
    )
```

```python
import functools
import math

import jax
import jax.numpy as jnp
import numpy as np
from jax import lax
from jax.experimental import pallas as pl
from jax.experimental.pallas import tpu as pltpu
from jax.sharding import PartitionSpec as P

F32 = jnp.float32
BF16 = jnp.bfloat16

LAYERS = 2
ROWS = 256
WIDTH = 512
PIECES = 8
SLOTS = 4
HEAD_PAIR = 128
TILE = 64
CTX = 672
NEG = -1e30

FIRST = (0, 256, 384, 448, 480)
LAST = (240, 368, 432, 464, 480)
LEVEL_SIZE = (256, 128, 64, 32, 16)
CTX_PREV = (0, 288, 448, 544, 608)
CTX_OWN = (16, 304, 464, 560, None)
CTX_NEXT = (272, 432, 528, 592, 624)
CTX_Y = 640
CTX_DIAG = 656
TILES = (
    (0, 0, 96, 0),
    (64, 64, 96, 0),
    (128, 128, 96, 0),
    (192, 192, 96, 0),
    (256, 288, 96, 1),
    (320, 352, 96, 1),
    (384, 448, 96, 1),
    (448, 544, 128, 2),
)


def dot(left, right):
    return lax.dot_general(left, right, (((1,), (0,)), ((), ())), preferred_element_type=F32)


def dot_nt(left, right):
    return lax.dot_general(left, right, (((1,), (1,)), ((), ())), preferred_element_type=F32)


def dot_tn(left, right):
    return lax.dot_general(left, right, (((0,), (0,)), ((), ())), preferred_element_type=F32)


def iota(dims, axis):
    return lax.broadcasted_iota(jnp.int32, dims, axis)


def by_level(index, values, rest):
    result = jnp.full(index.shape, rest, jnp.int32)
    for edge, value in reversed(tuple(zip((128, 192, 224, 240, 248), values))):
        result = jnp.where(index < edge, value, result)
    return result


def spread_table(transposed=False):
    shape = (ROWS, ROWS)
    position, coarse = iota(shape, 0), iota(shape, 1)
    if transposed:
        position, coarse = coarse, position
    level = by_level(coarse, (1, 2, 3, 4, 5), 0)
    base = by_level(coarse, (0, 128, 192, 224, 240), -ROWS)
    match = jnp.right_shift(position, level) == coarse - base
    return jnp.where(match, 1.0, 0.0).astype(BF16)


def step_inverse():
    index = iota((ROWS, HEAD_PAIR), 0)
    return 1.0 / by_level(index, (2, 4, 8, 16, 32), 1).astype(F32)


def fill_bias(bias_ref):
    query = iota((2 * TILE, 128), 0) & (TILE - 1)
    key = iota((2 * TILE, 128), 1)
    block = (key >> 4) - (query >> 4)
    near = (block >= 0) & (block <= 2) & (key < 96)
    far = jnp.abs(((query + 16) >> 3) - (key >> 3)) >= 2
    coarse = near & far
    bias_ref[0] = jnp.where(near, 0.0, NEG)
    bias_ref[1] = jnp.where(coarse, 0.0, NEG)
    half = ((query & 15) >> 3) + 2
    other = jnp.where(key < 80, (key >> 3) - 8, (key >> 3) - 6)
    fourth = (query >= 32) & (query < 48) & (key >= 64) & (key < 96) & (jnp.abs(half - other) >= 2)
    third = (query < 32) & (key < 64) & coarse
    fifth = (query >= 48) & (query < 56) & (key >= 96) & ((key & 15) < 8)
    bias_ref[2] = jnp.where(third | fourth | fifth, 0.0, NEG)


def fill_count(info_ref, count_ref):
    rest, close, rank = info_ref[0], info_ref[2], info_ref[4]

    def put(row, first, size, level, owner=0, usable=1):
        place = (iota((size, HEAD_PAIR), 0) + first) * 2**level + owner * ROWS
        inside = (place + rank * ROWS >= 0) & (usable == 1)
        held = jnp.where(inside, jnp.clip(rest - place, 0, 2**level), 0)
        count_ref[row : row + size, :] = held.astype(F32).astype(BF16)

    for level in range(5):
        put(CTX_PREV[level], -16, 16, level)
        put(CTX_NEXT[level], LEVEL_SIZE[level], 16, level)
        if CTX_OWN[level] is not None:
            put(CTX_OWN[level], 0, LEVEL_SIZE[level], level)
    for row, bits, usable in ((CTX_Y, 2, 1), (CTX_DIAG, 3, 1 - close)):
        place = iota((16, HEAD_PAIR), 0) * 32 + ((rank ^ bits) - rank) * ROWS
        inside = (iota((16, HEAD_PAIR), 0) < 8) & (usable == 1)
        held = jnp.where(inside, jnp.clip(rest - place, 0, 32), 0)
        count_ref[row : row + 16, :] = held.astype(F32).astype(BF16)


def halo_table(info_ref):
    even, close = info_ref[1] == 1, info_ref[2] == 1
    position, column = iota((ROWS, 192), 0), iota((ROWS, 192), 1)
    row = jnp.where(column < 80, column, column - 80)
    level, offset = row >> 4, row & 15
    first = offset
    last = jnp.right_shift(ROWS, level) - 16 + offset
    core = jnp.where(even, last, first)
    diag = jnp.where(close, jnp.where(even, first, last), -1)
    top = jnp.where(offset < 8, offset, -1)
    diag_top = jnp.where(close, -1, top)
    index = jnp.where(
        column < 80, core, jnp.where(column < 160, diag, jnp.where(column < 176, diag_top, top))
    )
    level = jnp.where(column < 160, level, 5)
    return jnp.where(jnp.right_shift(position, level) == index, 1.0, 0.0).astype(BF16)


def halo_step():
    row = iota((192, HEAD_PAIR), 0)
    level = jnp.where(row < 160, jnp.where(row < 80, row, row - 80) >> 4, 5)
    return 1.0 / jnp.left_shift(1, level).astype(F32)


def normalize(values):
    center = values - jnp.mean(values, axis=-1, keepdims=True)
    spread = jnp.mean(center * center, axis=-1, keepdims=True)
    scale = lax.rsqrt(spread + 1e-05)
    return center * scale, scale


def by_rows(body, sums=0):
    totals = tuple(jnp.zeros((8, WIDTH), F32) for _ in range(sums))
    for start in range(0, ROWS, 32):
        totals = body(pl.ds(start, 32), totals)
    return [jnp.sum(t, axis=0, keepdims=True) for t in totals]


def fold(total, values):
    return total + jnp.sum(values.reshape(4, 8, WIDTH), axis=0)


def valid_rows(info_ref, rows):
    return iota((32, WIDTH), 0) + rows.start < info_ref[0]


def normalize_back(values, gain, grad, totals):
    hat, scale = normalize(values)
    inner = grad * gain
    mean = jnp.mean(inner, axis=-1, keepdims=True)
    along = jnp.mean(inner * hat, axis=-1, keepdims=True)
    result = scale * (inner - mean - hat * along)
    return result, (fold(totals[0], grad * hat), fold(totals[1], grad))


def gelu_parts(values):
    size = jnp.abs(values) * (1.0 / math.sqrt(2.0))
    ratio = 1.0 / (1.0 + 0.3275911 * size)
    bell = jnp.exp(-size * size)
    poly = ratio * (
        0.254829592
        + ratio * (-0.284496736 + ratio * (1.421413741 + ratio * (-1.453152027 + ratio * 1.061405429)))
    )
    tail = 0.5 * poly * bell
    share = jnp.where(values >= 0.0, 1.0 - tail, tail)
    slope = share + values * bell * (1.0 / math.sqrt(2.0 * math.pi))
    return values * share, slope


def row_mask(info_ref, shape):
    return lax.broadcasted_iota(jnp.int32, shape, 0) < info_ref[0]


def project(
    normed, weights, info_ref, spread_t, step_inv, qkv_ref, core_ref, diag_ref, far_ref, slots=SLOTS
):
    even = info_ref[1] == 1
    keep = row_mask(info_ref, (ROWS, 3 * HEAD_PAIR))
    column = lax.broadcasted_iota(jnp.int32, (ROWS, 3 * HEAD_PAIR), 1)
    column_scale = jnp.where(column < HEAD_PAIR, 0.125, 1.0)
    step_wide = jnp.concatenate([step_inv, step_inv], axis=1)
    for slot in range(slots):
        rounded = dot(normed, weights[:, slot * 384 : (slot + 1) * 384]).astype(BF16).astype(F32)
        exact = (jnp.where(keep, rounded, 0.0) * column_scale).astype(BF16)
        qkv_ref[slot, :ROWS, :] = exact
        pooled = dot(spread_t, exact)
        qkv_ref[slot, ROWS:, : 2 * HEAD_PAIR] = (pooled[:, : 2 * HEAD_PAIR] * step_wide).astype(BF16)
        qkv_ref[slot, ROWS:, 2 * HEAD_PAIR :] = pooled[:, 2 * HEAD_PAIR :].astype(BF16)
        for level in range(5):
            first = qkv_ref[slot, FIRST[level] : FIRST[level] + 16, HEAD_PAIR:]
            last = qkv_ref[slot, LAST[level] : LAST[level] + 16, HEAD_PAIR:]
            core_ref[slot, level * 16 : level * 16 + 16, :] = jnp.where(even, last, first)
            diag_ref[slot, level * 16 : level * 16 + 16, :] = jnp.where(even, first, last)
        qkv_ref.flush_part(slot)
        top = qkv_ref[slot, 496:512, HEAD_PAIR:]
        diag_ref[slot, 80:96, :] = top
        far_ref[slot, :, :] = top


def first_near_kernel(
    info_ref, x_ref, gain_ref, offset_ref, weights,
    normed_ref, stream_ref, qkv_ref, core_ref, diag_ref, far_ref,
):
    ready(x_ref, gain_ref, offset_ref)

    def start(rows, totals):
        stream = x_ref[0, rows, :].astype(F32)
        stream_ref[rows, :] = stream
        hat, _ = normalize(stream)
        normed_ref[rows, :] = (hat * gain_ref[0, 0:1, :] + offset_ref[0, 0:1, :]).astype(BF16)
        return totals

    by_rows(start)
    normed_ref.flush()
    stream_ref.flush()
    project(
        normed_ref[...], weights, info_ref, spread_table(True), step_inverse(),
        qkv_ref, core_ref, diag_ref, far_ref, 2,
    )


def first_kernel(
    info_ref, normed_ref, weights, near_core, near_diag, near_far,
    qkv_ref, core_ref, diag_ref, far_ref, part_core, part_diag, part_far,
):
    spread_t, step_inv = spread_table(True), step_inverse()
    parts = (part_core, part_diag, part_far)
    project(normed_ref[...], weights, info_ref, spread_t, step_inv, qkv_ref, *parts, 2)
    for near, part, target in zip(
        (near_core, near_diag, near_far), parts, (core_ref, diag_ref, far_ref)
    ):
        target[0:2] = near[...]
        target[2:4] = part[...]
        target.flush()


def head_stack(values):
    column = iota(values.shape, 1) & (HEAD_PAIR - 1)
    zero = jnp.zeros_like(values)
    left = jnp.where(column < HEAD_PAIR // 2, values, zero)
    right = jnp.where(column < HEAD_PAIR // 2, zero, values)
    return jnp.concatenate([left, right], axis=0)


def head_join(stacked):
    column = iota((TILE, stacked.shape[1]), 1) & (HEAD_PAIR - 1)
    return jnp.where(column < HEAD_PAIR // 2, stacked[:TILE], stacked[TILE:])


def mix_kernel(
    layer, info_ref, qkv_ref, core_ref, diag_ref, far_ref, stream_ref, gain_ref, offset_ref, weights_ref,
    ctx_ref, mixed_ref, inverse_ref, middle_ref, normed_ref, stat_ref,
    pair_ref, sum_ref, bias_ref, count_ref, spread_ref,
):
    even = info_ref[1] == 1
    near = info_ref[2] == 1
    fill_bias(bias_ref)
    fill_count(info_ref, count_ref)
    spread_ref[...] = spread_table()
    for slot in range(SLOTS):
        for level in range(5):
            rows = slice(level * 16, level * 16 + 16)
            core = core_ref[slot ^ 1, rows, :]
            diag = diag_ref[slot ^ 3, rows, :]
            diag = jnp.where(near, diag, jnp.zeros_like(diag))
            ctx_ref[slot, CTX_PREV[level] : CTX_PREV[level] + 16, :] = jnp.where(even, diag, core)
            ctx_ref[slot, CTX_NEXT[level] : CTX_NEXT[level] + 16, :] = jnp.where(even, core, diag)
            if CTX_OWN[level] is not None:
                own = slice(CTX_OWN[level], CTX_OWN[level] + LEVEL_SIZE[level])
                source = slice(FIRST[level], FIRST[level] + LEVEL_SIZE[level])
                ctx_ref[slot, own, :] = qkv_ref[slot, source, HEAD_PAIR:]
        ctx_ref[slot, CTX_Y : CTX_Y + 16, :] = far_ref[slot ^ 2, :, :]
        diag = diag_ref[slot ^ 3, 80:96, :]
        ctx_ref[slot, CTX_DIAG : CTX_DIAG + 16, :] = jnp.where(near, jnp.zeros_like(diag), diag)

    ctx_ref.flush()
    ready(qkv_ref)
    begin(weights_ref, stream_ref, gain_ref, offset_ref)

    @pl.loop(0, SLOTS)
    def _(slot):
        for query_row, context_row, keys, mask in TILES:
            queries = head_stack(qkv_ref[slot, query_row : query_row + TILE, :HEAD_PAIR])
            context = slice(context_row, context_row + keys)
            scores = dot_nt(queries, ctx_ref[slot, context, :HEAD_PAIR])
            weights = jnp.exp(scores + bias_ref[mask, :, :keys]).astype(BF16)
            values = jnp.concatenate(
                [ctx_ref[slot, context, HEAD_PAIR:], count_ref[context, :]], axis=1
            )
            pair_ref[slot, query_row : query_row + TILE, :] = head_join(dot(weights, values))

    spread = spread_ref[...]
    for slot in range(SLOTS):
        coarse = pair_ref[slot, ROWS:, :]
        high = coarse.astype(BF16)
        low = (coarse - high.astype(F32)).astype(BF16)
        total = pair_ref[slot, :ROWS, :] + dot(spread, high) + dot(spread, low)
        inverse = 1.0 / total[:, HEAD_PAIR:]
        columns = slice(slot * HEAD_PAIR, (slot + 1) * HEAD_PAIR)
        inverse_ref[:, columns] = inverse
        mixed_ref[:, columns] = (total[:, :HEAD_PAIR] * inverse).astype(BF16)
    inverse_ref.flush()
    mixed_ref.flush()
    sum_ref[...] = dot(mixed_ref[...], weights_ref[...])
    ready(stream_ref, gain_ref, offset_ref)

    def finish(rows, totals):
        attended = sum_ref[rows, :]
        squares = jnp.where(valid_rows(info_ref, rows), attended * attended, 0.0)
        middle = stream_ref[rows, :] + attended
        middle_ref[rows, :] = middle
        hat, _ = normalize(middle)
        gain, offset = gain_ref[layer, 1:2, :], offset_ref[layer, 1:2, :]
        normed_ref[rows, :] = (hat * gain + offset).astype(BF16)
        return (fold(totals[0], squares),)

    (stat_ref[...],) = by_rows(finish, 1)


def halves(half):
    start = pl.multiple_of(half * 256, 256)
    return pl.ds(start, 256), pl.ds(512 + start, 256)


def feed_slots(normed, weights, following, act_ref, slope_ref, total_ref, fresh):
    for slot, weight in enumerate(weights):
        ready(weight)
        begin(*following[slot])
        hidden = dot(normed, weight[:512, :]) + weight[1024:1025, :].astype(F32)
        act, slope = gelu_parts(hidden)
        act = act.astype(BF16)
        act_ref[slot, :, :] = act
        slope_ref[slot, :, :] = slope.astype(BF16)
        act_ref.flush_part(slot)
        slope_ref.flush_part(slot)
        part = dot(act, weight[512:1024, :])
        if slot == 0 and fresh:
            total_ref[...] = part
        else:
            total_ref[...] += part


def feed_near_kernel(info_ref, normed_ref, w0, w1, act_ref, slope_ref, total_ref):
    feed_slots(normed_ref[...], (w0, w1), ((), ()), act_ref, slope_ref, total_ref, True)


def feed_kernel(
    info_ref, normed_ref, middle_ref, w0, w1, near_ref, bias_out_ref,
    gain_ref, offset_ref, projections,
    act_ref, slope_ref, stat_ref, stream_ref, next_ref, qkv_ref, core_ref, diag_ref, far_ref,
    total_ref,
):
    following = ((near_ref, middle_ref, bias_out_ref, gain_ref, offset_ref), (projections,))
    feed_slots(normed_ref[...], (w0, w1), following, act_ref, slope_ref, total_ref, True)
    ready(near_ref)
    ready(middle_ref, bias_out_ref, gain_ref, offset_ref)

    def finish(rows, totals):
        total_ref[rows, :] += near_ref[rows, :]
        stream, totals = add_branch(info_ref, rows, totals, total_ref, bias_out_ref[0:1, :], middle_ref)
        stream_ref[rows, :] = stream
        hat, _ = normalize(stream)
        next_ref[rows, :] = (hat * gain_ref[1, 0:1, :] + offset_ref[1, 0:1, :]).astype(BF16)
        return totals

    stat_ref[0:1, :], stat_ref[1:2, :] = by_rows(finish, 2)
    stream_ref.flush()
    next_ref.flush()
    project(
        next_ref[...], projections, info_ref, spread_table(True), step_inverse(),
        qkv_ref, core_ref, diag_ref, far_ref,
    )


def add_branch(info_ref, rows, totals, branch_ref, bias, middle_ref):
    branch = branch_ref[rows, :] + bias
    stream = middle_ref[rows, :] + branch
    valid = valid_rows(info_ref, rows)
    return stream, (
        fold(totals[0], jnp.where(valid, branch * branch, 0.0)),
        fold(totals[1], jnp.where(valid, stream * stream, 0.0)),
    )


def put_grads(target, matrix, value, at=0):
    low = value.astype(BF16)
    for piece in range(PIECES):
        target[piece, matrix * 64 : matrix * 64 + 64, at : at + value.shape[1]] = low[
            piece * 64 : piece * 64 + 64
        ]


def put_half(in_target, out_target, start, half, in_grad, out_grad):
    columns, _ = halves(half)
    low = in_grad.astype(BF16)
    for piece in range(PIECES):
        in_target[piece, :64, columns] = low[piece * 64 : piece * 64 + 64]
    low = out_grad.astype(BF16)
    for piece in range(PIECES // 2):
        place = half * (PIECES // 2) + piece
        out_target[place, start : start + 64, :] = low[piece * 64 : piece * 64 + 64]


def turn_kernel(
    info_ref, normed_ref, middle_ref, w0, w1, w2, w3, bias_out_ref, cotangent_ref, gain_ref,
    stream_ref, stat_ref, g0, g1, g2, g3, hidden_grad_ref, small_ref, grad_ref,
    total_ref, back_ref, low_ref, after,
):
    normed = normed_ref[...]
    following = ((w2,), (w3,), (middle_ref, bias_out_ref, gain_ref), after)

    def begin_grad(rows, totals):
        grad = jnp.where(valid_rows(info_ref, rows), cotangent_ref[0, rows, :].astype(F32), 0.0)
        low_ref[rows, :] = grad.astype(BF16)
        return (fold(totals[0], grad),)

    ready(cotangent_ref)
    (small_ref[2:3, :],) = by_rows(begin_grad, 1)
    grad_low = low_ref[...]
    total_ref[...] = jnp.zeros_like(total_ref)
    back_ref[...] = jnp.zeros_like(back_ref)
    for slot, weight in enumerate((w0, w1, w2, w3)):
        ready(weight)
        begin(*following[slot])
        target = (g0, g1, g2, g3)[slot]

        @pl.loop(0, 2)
        def _(half):
            columns, rows = halves(half)
            hidden = dot(normed, weight[:512, columns]) + weight[1024:1025, columns].astype(F32)
            act, slope = gelu_parts(hidden)
            act = act.astype(BF16)
            total_ref[...] += dot(act, weight[rows, :])
            hidden_grad = (dot_nt(grad_low, weight[rows, :]) * slope).astype(BF16)
            back_ref[...] += dot_nt(hidden_grad, weight[:512, columns])
            put_half(target, target, 64, half, dot_tn(normed, hidden_grad), dot_tn(act, grad_low))
            hidden_grad_ref[slot : slot + 1, columns] = jnp.sum(
                hidden_grad.astype(F32), axis=0, keepdims=True
            )

        target.flush()
    ready(middle_ref, bias_out_ref, gain_ref)

    def finish(rows, totals):
        stream, first = add_branch(
            info_ref, rows, totals[:2], total_ref, bias_out_ref[1:2, :], middle_ref
        )
        stream_ref[rows, :] = stream
        through, second = normalize_back(
            middle_ref[rows, :], gain_ref[1, 1:2, :], back_ref[rows, :], totals[2:]
        )
        grad = jnp.where(valid_rows(info_ref, rows), cotangent_ref[0, rows, :].astype(F32), 0.0) + through
        grad_ref[rows, :] = grad
        return first + second

    stat_ref[0:1, :], stat_ref[1:2, :], small_ref[0:1, :], small_ref[1:2, :] = by_rows(finish, 4)


def mix_back_kernel(
    info_ref, grad_ref, weights_ref, mixed_ref, inverse_ref, qkv_ref, ctx_ref,
    output_ref, local_ref, core_ref, diag_ref, far_ref,
    sum_ref, pair_ref, query_ref, context_ref, bias_ref, count_ref, spread_ref, spread_t_ref, step_ref,
):
    even = info_ref[1] == 1
    grad_low = grad_ref[...].astype(BF16)
    sum_ref[...] = dot_nt(grad_low, weights_ref[...])
    rows_grad = dot_tn(mixed_ref[...], grad_low).astype(BF16)
    for slot in range(SLOTS):
        for j in range(4):
            output_ref[slot, j * 128 : (j + 1) * 128, :] = rows_grad[
                slot * 128 : (slot + 1) * 128, j * 128 : (j + 1) * 128
            ]
    ready(mixed_ref, inverse_ref)

    def scale(rows, totals):
        scaled = sum_ref[rows, :].astype(BF16).astype(F32) * inverse_ref[rows, :]
        along = -scaled * mixed_ref[rows, :].astype(F32)
        for slot in range(SLOTS):
            columns = slice(slot * HEAD_PAIR, (slot + 1) * HEAD_PAIR)
            pair_ref[slot, rows, :HEAD_PAIR] = scaled[:, columns].astype(BF16)
            pair_ref[slot, rows, HEAD_PAIR:] = along[:, columns].astype(BF16)
        return totals

    by_rows(scale)
    for slot in range(SLOTS):
        pair_ref[slot, ROWS:, :] = dot(spread_t_ref[...], pair_ref[slot, :ROWS, :]).astype(BF16)

    output_ref.flush()
    ready(qkv_ref, ctx_ref)

    @pl.loop(0, SLOTS)
    def _(slot):
        held = None
        for query_row, context_row, keys, mask in TILES:
            queries = head_stack(qkv_ref[slot, query_row : query_row + TILE, :HEAD_PAIR])
            context = slice(context_row, context_row + keys)
            keyed = ctx_ref[slot, context, :HEAD_PAIR]
            scores = dot_nt(queries, keyed)
            weights = jnp.exp(scores + bias_ref[mask, :, :keys])
            values = jnp.concatenate(
                [ctx_ref[slot, context, HEAD_PAIR:], count_ref[context, :]], axis=1
            )
            upper = head_stack(pair_ref[slot, query_row : query_row + TILE, :])
            grad_scores = (dot_nt(upper, values) * weights).astype(BF16)
            query_ref[slot, query_row : query_row + TILE, :] = head_join(dot(grad_scores, keyed)) * 0.125
            key_part = dot_tn(grad_scores, queries)
            value_part = dot_tn(weights.astype(BF16), upper[:, :HEAD_PAIR])
            part = jnp.concatenate([key_part, value_part], axis=1)
            if context_row % TILE == 0 and context_row in (64, 128, 192) or context_row == 352:
                part = jnp.concatenate([part[:32] + held, part[32:]], axis=0)
            if context_row in (0, 64, 128, 288):
                held = part[TILE:]
                part = part[:TILE]
            context_ref[slot, context_row : context_row + part.shape[0], :] = part

    for slot in range(SLOTS):
        step_inv = step_ref[...]
        own = jnp.concatenate(
            [
                context_ref[slot, CTX_OWN[level] : CTX_OWN[level] + LEVEL_SIZE[level], :]
                for level in (1, 2, 3)
            ]
            + [jnp.zeros((32, 2 * HEAD_PAIR), F32)],
            axis=0,
        )
        coarse = jnp.concatenate(
            [query_ref[slot, ROWS:, :] * step_inv, own[:, :HEAD_PAIR] * step_inv, own[:, HEAD_PAIR:]],
            axis=1,
        ).astype(BF16)
        down = dot(spread_ref[...], coarse)
        local = query_ref[slot, :ROWS, :] + down[:, :HEAD_PAIR]
        local_ref[slot, :, :HEAD_PAIR] = local.astype(BF16)
        local = context_ref[slot, 16 : 16 + ROWS, :] + down[:, HEAD_PAIR:]
        local_ref[slot, :, HEAD_PAIR:] = local.astype(BF16)
        local_ref.flush_part(slot)
        for level in range(5):
            rows = slice(level * 16, level * 16 + 16)
            before = context_ref[slot, CTX_PREV[level] : CTX_PREV[level] + 16, :]
            after = context_ref[slot, CTX_NEXT[level] : CTX_NEXT[level] + 16, :]
            core_ref[slot, rows, :] = jnp.where(even, after, before).astype(BF16)
            diag_ref[slot, rows, :] = jnp.where(even, before, after).astype(BF16)
        diag_ref[slot, 80:96, :] = context_ref[slot, CTX_DIAG : CTX_DIAG + 16, :].astype(BF16)
        far_ref[slot, :, :] = context_ref[slot, CTX_Y : CTX_Y + 16, :].astype(BF16)
        for target in (core_ref, diag_ref, far_ref):
            target.flush_part(slot)


def back_tables(info_ref, bias_ref, count_ref, spread_ref, spread_t_ref, step_ref):
    fill_bias(bias_ref)
    fill_count(info_ref, count_ref)
    spread_ref[...] = spread_table()
    spread_t_ref[...] = spread_table(True)
    step_ref[...] = step_inverse()


def chained(body, inputs, outputs, scratch):
    def kernel(info_ref, *refs):
        refs = list(refs)
        parts = [[refs.pop(0) for _ in range(n)] for n in (inputs, 5, outputs, 5, scratch)]
        ins, back_ins, outs, back_outs, held = parts
        back_tables(info_ref, *refs[4:])
        body(info_ref, *ins, *outs, *held, tuple(back_ins))
        for result in outs:
            result.flush()
        mix_back_kernel(info_ref, outs[-1], *back_ins, *back_outs, *refs)

    return kernel


def project_back(
    info_ref, local_ref, core_ref, diag_ref, far_ref, normed, weights, targets, output_ref,
    low_ref, back_ref,
):
    keep = row_mask(info_ref, (ROWS, 3 * HEAD_PAIR))
    halo = halo_table(info_ref)
    scale = halo_step()
    for slot in range(SLOTS):
        arrived = jnp.concatenate(
            [core_ref[slot ^ 1, :, :], diag_ref[slot ^ 3, :, :], far_ref[slot ^ 2, :, :]], axis=0
        ).astype(F32)
        arrived = jnp.concatenate(
            [arrived[:, :HEAD_PAIR] * scale, arrived[:, HEAD_PAIR:]], axis=1
        ).astype(BF16)
        added = dot(halo, arrived)
        local = local_ref[slot, :, :].astype(F32)
        whole = jnp.concatenate([local[:, :HEAD_PAIR], local[:, HEAD_PAIR:] + added], axis=1)
        low_ref[:, slot * 384 : (slot + 1) * 384] = jnp.where(keep, whole, 0.0).astype(BF16)
    back_ref[...] = dot_nt(low_ref[...], weights[...])
    for slot in range(SLOTS):
        put_grads(targets[slot], 0, dot_tn(normed, low_ref[:, slot * 384 : (slot + 1) * 384]))
        put_grads(targets[slot], 0, output_ref[slot, :, :], 3 * HEAD_PAIR)


def between_kernel(
    info_ref, local_ref, core_ref, diag_ref, far_ref,
    normed_ref, projections, grad_in_ref, stream_ref, gain_ref,
    act_ref, slope_ref, second_ref, middle_ref, w0, w1, w2, w3, output_ref,
    a0, a1, a2, a3, g0, g1, g2, g3, o0, o1, o2, o3, hidden_grad_ref, small_ref, grad_ref,
    back_ref, mid_ref, low_ref, joint_ref, after,
):
    ready(local_ref, core_ref, diag_ref, far_ref, normed_ref, projections)
    begin(output_ref, grad_in_ref, stream_ref, gain_ref, w0, slope_ref, second_ref, act_ref)
    following = ((w2, middle_ref), (w3,), (), after)
    project_back(
        info_ref, local_ref, core_ref, diag_ref, far_ref,
        normed_ref[...], projections, (a0, a1, a2, a3), output_ref, joint_ref, back_ref,
    )
    for target in (a0, a1, a2, a3):
        target.flush()
    ready(grad_in_ref, stream_ref, gain_ref)

    def middle(rows, totals):
        through, first = normalize_back(
            stream_ref[rows, :], gain_ref[1, 0:1, :], back_ref[rows, :], totals[:2]
        )
        grad = grad_in_ref[rows, :] + through
        mid_ref[rows, :] = grad
        low = grad.astype(BF16)
        low_ref[rows, :] = low
        return first + (fold(totals[2], low.astype(F32)),)

    small_ref[0:1, :], small_ref[1:2, :], small_ref[4:5, :] = by_rows(middle, 3)
    grad_low = low_ref[...]
    second = second_ref[...]
    back_ref[...] = jnp.zeros_like(back_ref)
    ready(act_ref, slope_ref)
    begin(w1)
    for slot, weight in enumerate((w0, w1, w2, w3)):
        ready(weight)
        begin(*following[slot])
        in_target, out_target = (g0, g1, g2, g3)[slot], (o0, o1, o2, o3)[slot]

        @pl.loop(0, 2)
        def _(half):
            columns, rows = halves(half)
            slope = slope_ref[slot, :, columns].astype(F32)
            hidden_grad = (dot_nt(grad_low, weight[rows, :]) * slope).astype(BF16)
            back_ref[...] += dot_nt(hidden_grad, weight[:512, columns])
            put_half(
                in_target, out_target, 0, half, dot_tn(second, hidden_grad), dot_tn(act_ref[slot, :, columns], grad_low)
            )
            hidden_grad_ref[slot : slot + 1, columns] = jnp.sum(
                hidden_grad.astype(F32), axis=0, keepdims=True
            )

        in_target.flush()
        out_target.flush()
    ready(middle_ref)

    def finish(rows, totals):
        through, totals = normalize_back(
            middle_ref[rows, :], gain_ref[0, 1:2, :], back_ref[rows, :], totals
        )
        grad_ref[rows, :] = mid_ref[rows, :] + through
        return totals

    small_ref[2:3, :], small_ref[3:4, :] = by_rows(finish, 2)


def last_kernel(
    info_ref, local_ref, core_ref, diag_ref, far_ref,
    normed_ref, projections, grad_in_ref, stream_ref, gain_ref, output_ref,
    stat_a, stat_b, stat_c, stat_d, small_a, small_b, hidden_one, hidden_two,
    a0, a1, a2, a3, grad_ref,
    joint_ref, back_ref,
):
    targets = (a0, a1, a2, a3)
    ready(local_ref, core_ref, diag_ref, far_ref, normed_ref, projections)
    begin(
        output_ref, grad_in_ref, stream_ref, gain_ref, stat_a, stat_b, stat_c, stat_d, small_a, small_b,
        hidden_one, hidden_two,
    )
    project_back(
        info_ref, local_ref, core_ref, diag_ref, far_ref,
        normed_ref[...], projections, targets, output_ref, joint_ref, back_ref,
    )
    ready(grad_in_ref, stream_ref, gain_ref)

    def finish(rows, totals):
        through, totals = normalize_back(
            stream_ref[0, rows, :].astype(F32), gain_ref[0, 0:1, :], back_ref[rows, :], totals
        )
        grad_ref[rows, :] = grad_in_ref[rows, :] + through
        return totals

    gain_grad, offset_grad = by_rows(finish, 2)
    grad_ref.flush()
    position = lax.broadcasted_iota(jnp.int32, (1, WIDTH), 1)
    valid = jnp.where(position < jnp.minimum(info_ref[0], ROWS), 1.0, 0.0)
    lines = [
        gain_grad, offset_grad,
        small_b[0:1, :], small_b[1:2, :], small_b[2:3, :], small_b[3:4, :], small_b[4:5, :],
        small_a[0:1, :], small_a[1:2, :], small_a[2:3, :],
        stat_a[...], stat_b[0:1, :], stat_b[1:2, :], stat_c[...], stat_d[0:1, :], stat_d[1:2, :],
        valid,
    ]
    zero = jnp.zeros((1, WIDTH), F32)
    for slot in range(SLOTS):
        target = targets[slot]
        own = lines + [hidden_one[slot : slot + 1, :], hidden_two[slot : slot + 1, :]]
        own = own + [zero] * (8 * PIECES - len(own))
        for piece in range(PIECES):
            rows = jnp.concatenate(own[piece * 8 : piece * 8 + 8], axis=0)
            target[piece, 64:72, :] = rows.astype(BF16)


def far_sum_kernel(index_ref, keep_ref, arrived_ref, back_ref, stay_ref, go_ref):
    side = index_ref[0]
    for place in range(PIECES // 2):
        for target, which in ((stay_ref, side), (go_ref, 1 - side)):
            piece = 2 * place + which
            target[place] = (
                keep_ref[piece].astype(F32)
                + arrived_ref[piece].astype(F32)
                + back_ref[piece].astype(F32)
            ).astype(BF16)


def split_sum_kernel(bit, index_ref, stay_ref, arrived_ref, next_stay_ref, next_go_ref):
    side = index_ref[bit]
    for place in range(next_stay_ref.shape[0]):
        for target, which in ((next_stay_ref, side), (next_go_ref, 1 - side)):
            piece = 2 * place + which
            target[place] = (stay_ref[piece].astype(F32) + arrived_ref[piece].astype(F32)).astype(BF16)


def add_kernel(stay_ref, arrived_ref, sum_ref):
    sum_ref[...] = (stay_ref[...].astype(F32) + arrived_ref[...].astype(F32)).astype(BF16)


def join_kernel(bit, index_ref, own_ref, other_ref, block_ref):
    side = index_ref[bit]
    for place in range(own_ref.shape[0]):
        block_ref[2 * place + side] = own_ref[place]
        block_ref[2 * place + 1 - side] = other_ref[place]


def placed(info_ref, own, other):
    side = info_ref[3]
    for place in range(PIECES // 2):
        yield 2 * place + side, own, place
        yield 2 * place + 1 - side, other, place


def feed_result_kernel(
    info_ref, own_two, other_two, own_in, other_in, own_out, other_out, in_ref, out_ref
):
    ready(own_two, other_two, own_in, other_in, own_out, other_out)
    for layer, target, pair, start in (
        (1, in_ref, (own_two, other_two), 0), (1, out_ref, (own_two, other_two), 64),
        (0, in_ref, (own_in, other_in), 0), (0, out_ref, (own_out, other_out), 0),
    ):
        for piece, source, place in placed(info_ref, *pair):
            rows = pl.ds(pl.multiple_of(piece * 64, 64), 64)
            target[layer, rows, :] = source[place, start : start + 64, :].astype(F32)
        target.flush_part(layer)


def attn_result_kernel(
    info_ref, own_one, other_one, own_two, other_two,
    query_ref, key_ref, value_ref, output_ref, b_in_ref, gain_ref, offset_ref, b_out_ref, norm_ref,
    lines_ref,
):
    for layer, pair in ((1, (own_two, other_two)), (0, (own_one, other_one))):
        ready(*pair)
        for piece, source, place in placed(info_ref, *pair):
            rows = pl.ds(pl.multiple_of(piece * 64, 64), 64)
            part = source[place, :64, :].astype(F32)
            for i, target in enumerate((query_ref, key_ref, value_ref)):
                target[layer, rows, :] = part[:, i * HEAD_PAIR : (i + 1) * HEAD_PAIR]
            where = pl.ds(pl.multiple_of((piece % 2) * 64, 64), 64)
            columns = pl.ds(pl.multiple_of((piece // 2) * 128, 128), 128)
            output_ref[layer, where, columns] = part[:, 3 * HEAD_PAIR :]
            if layer == 0:
                rows = pl.ds(pl.multiple_of(piece * 8, 8), 8)
                lines_ref[rows, :] = source[place, 64:, :].astype(F32)
        for target in (query_ref, key_ref, value_ref, output_ref):
            target.flush_part(layer)
    for number, (target, place) in enumerate(
        (
            (gain_ref, (0, 0)), (offset_ref, (0, 0)), (gain_ref, (1, 0)), (offset_ref, (1, 0)),
            (gain_ref, (0, 1)), (offset_ref, (0, 1)), (b_out_ref, (0,)),
            (gain_ref, (1, 1)), (offset_ref, (1, 1)), (b_out_ref, (1,)),
        )
    ):
        line = lines_ref[number : number + 1, :]
        target[place[:-1] + (slice(place[-1], place[-1] + 1), slice(None))] = line
    b_in_ref[...] = lines_ref[17:19, :]
    squares = jnp.sum(lines_ref[10:18, :], axis=1, keepdims=True)
    count = jnp.sum(lines_ref[16:17, :], axis=1, keepdims=True)
    roots = jnp.sqrt(squares / (count * WIDTH))
    lane = iota((1, 128), 1)
    row = jnp.zeros((1, 128), F32)
    for i in range(3 * LAYERS):
        row = jnp.where(lane == i, roots[i : i + 1, :], row)
    norm_ref[...] = row[:, : 3 * LAYERS]


AFTER = []
ORDER = [None]


def in_order(value):
    before = [other for other in (ORDER[0], *AFTER) if other is not None]
    AFTER.clear()
    return tie(value, *before) if before else value


class Plan:
    def __init__(self, parts, dims, moves):
        self.parts, self.dims, self.moves = list(parts), dims, moves


def everything(value):
    return Plan([value], value.shape, [(0, None, None)])


def feed_plan(parts):
    if len(parts) == 1:
        return everything(parts[0])
    rows, width = parts[0].shape

    def half(number):
        def place(info_ref):
            side = info_ref[3] if number == 0 else 1 - info_ref[3]
            return pl.ds(pl.multiple_of(side * rows, 16), rows), slice(None)

        return place

    return Plan(parts, (2 * rows, width), [(i, None, half(i)) for i in range(2)])


def qkv_plan(slots):
    parts, moves = [], []
    for slot, group in enumerate(slots):
        rows = 512 // len(group)
        for i, part in enumerate(group):
            place = (slice(i * rows, (i + 1) * rows), slice(slot * 384, (slot + 1) * 384))
            moves.append((len(parts), (slice(None), slice(0, 384)), place))
            parts.append(part)
    return Plan(parts, (512, 384 * len(slots)), moves)


def output_plan(slots):
    parts, moves = [], []
    for slot, group in enumerate(slots):
        for j in range(4):
            rows = 4 // len(group)
            start = j % rows * 128
            source = (slice(start, start + 128), slice(384, 512))
            number = len(parts) + j // rows
            place = (slice(slot * 128, (slot + 1) * 128), slice(j * 128, (j + 1) * 128))
            moves.append((number, source, place))
        parts += group
    return Plan(parts, (512, 512), moves)


class Late:
    def __init__(self, arg):
        self.arg = arg


class Arriving:
    def __init__(self, ref, make, late):
        self.ref, self.make, self.copies = ref, make, None
        if not late:
            self.start()

    def start(self):
        if self.copies is None:
            self.copies = self.make()
            for copy in self.copies:
                copy.start()

    def wait(self):
        self.start()
        for copy in self.copies:
            copy.wait()
        self.copies = []

    def __getitem__(self, place):
        self.wait()
        return self.ref[place]


def begin(*arriving):
    for operand in arriving:
        operand.start()


class Leaving:
    def __init__(self, ref, target, sem):
        self.ref, self.target, self.sem, self.started = ref, target, sem, False
        self.copy = pltpu.make_async_copy(ref, target, sem)

    def flush(self):
        if not self.started:
            self.copy.start()
        self.started = True

    def flush_part(self, place):
        pltpu.make_async_copy(self.ref.at[place], self.target.at[place], self.sem).start()
        self.started = True

    def __getitem__(self, place):
        return self.ref[place]

    def __setitem__(self, place, value):
        self.ref[place] = value


def ready(*arriving):
    for operand in arriving:
        operand.wait()


def staged(body, name, out, args, scratch=(), flops=0):
    args = (in_order(args[0]),) + tuple(args[1:])
    late = [isinstance(arg, Late) for arg in args[1:]]
    plans = [arg.arg if isinstance(arg, Late) else arg for arg in args[1:]]
    plans = [plan if isinstance(plan, Plan) else everything(plan) for plan in plans]
    flat = [part for plan in plans for part in plan.parts]
    count = sum(len(plan.moves) for plan in plans)
    held = [pltpu.VMEM(plan.dims, plan.parts[0].dtype) for plan in plans]

    def kernel(*refs):
        info_ref, refs = refs[0], list(refs[1:])
        sources = [refs.pop(0) for _ in flat]
        targets = [refs.pop(0) for _ in out]
        inner = [refs.pop(0) for _ in held]
        outer = [refs.pop(0) for _ in out]
        sem_in = refs.pop()
        sem_out = refs.pop()
        arriving = []
        start, number = 0, 0
        for plan, ref, later in zip(plans, inner, late):

            def make(plan=plan, ref=ref, start=start, number=number):
                copies = []
                for i, (part, source_place, place) in enumerate(plan.moves):
                    source, target = sources[start + part], ref
                    if source_place is not None:
                        source = source.at[source_place]
                    if place is not None:
                        target = target.at[place(info_ref) if callable(place) else place]
                    copies.append(pltpu.make_async_copy(source, target, sem_in.at[number + i]))
                return copies

            arriving.append(Arriving(ref, make, later))
            start += len(plan.parts)
            number += len(plan.moves)
        leaving = [
            Leaving(ref, target, sem_out.at[i])
            for i, (ref, target) in enumerate(zip(outer, targets))
        ]
        body(info_ref, *arriving, *leaving, *refs)
        for operand in arriving:
            operand.wait()
        for result in leaving:
            result.flush()
        for result in leaving:
            result.copy.wait()

    result = pl.pallas_call(
        kernel,
        out_shape=tuple(out),
        in_specs=[pl.BlockSpec(memory_space=pltpu.SMEM)]
        + [pl.BlockSpec(memory_space=pl.ANY)] * len(flat),
        out_specs=tuple(pl.BlockSpec(memory_space=pl.ANY) for _ in out),
        scratch_shapes=held
        + [pltpu.VMEM(o.shape, o.dtype) for o in out]
        + list(scratch)
        + [pltpu.SemaphoreType.DMA((len(out),)), pltpu.SemaphoreType.DMA((count,))],
        cost_estimate=pl.CostEstimate(flops=1, bytes_accessed=1, transcendentals=0),
        name=name,
    )(args[0], *flat)
    ORDER[0] = result[-1]
    return result


def call(body, name, out, args, scalars=0):
    in_specs = [pl.BlockSpec(memory_space=pltpu.SMEM)] * scalars
    in_specs += [pl.BlockSpec(memory_space=pltpu.VMEM)] * (len(args) - scalars)
    args = (in_order(args[0]),) + tuple(args[1:])
    result = pl.pallas_call(
        body,
        out_shape=tuple(out),
        in_specs=in_specs,
        out_specs=tuple(pl.BlockSpec(memory_space=pltpu.VMEM) for _ in out),
        compiler_params=pltpu.CompilerParams(vmem_limit_bytes=4 << 20),
        cost_estimate=pl.CostEstimate(flops=1, bytes_accessed=1, transcendentals=0),
        name=name,
    )(*args)
    ORDER[0] = result[-1]
    return result


def start_attn(layer, wq, wk, wv, wo, block, sems):
    copies = []
    for i, source in enumerate((wq, wk, wv)):
        target = block.at[:, i * HEAD_PAIR : (i + 1) * HEAD_PAIR]
        copies.append(pltpu.make_async_copy(source.at[layer], target, sems.at[i]))
    for j in range(4):
        target = block.at[j * 128 : (j + 1) * 128, 3 * HEAD_PAIR :]
        source = wo.at[layer, :, j * 128 : (j + 1) * 128]
        copies.append(pltpu.make_async_copy(source, target, sems.at[3 + j]))
    for copy in copies:
        copy.start()
    return copies


def pack_first_kernel(wq, wk, wv, wo, own_ref, block, sems):
    for copy in start_attn(0, wq, wk, wv, wo, block, sems):
        copy.wait()
    copy = pltpu.make_async_copy(block, own_ref, sems.at[0])
    copy.start()
    copy.wait()


def pack_rest_kernel(
    info_ref, wq, wk, wv, wo, w_in, b_in, w_out,
    attn_two, feed_one, half_one, feed_two, half_two,
    attn, feeds, biases, sems, feed_sems, out_sems,
):
    side = info_ref[3]
    attn_copies = start_attn(1, wq, wk, wv, wo, attn, sems)
    feed_copies = []
    for layer in range(LAYERS):
        for i, source in enumerate((w_in, w_out)):
            copy = pltpu.make_async_copy(
                source.at[layer], feeds.at[layer, i * 512 : i * 512 + 512], feed_sems.at[layer * 2 + i]
            )
            copy.start()
            feed_copies.append(copy)
    bias_copy = pltpu.make_async_copy(b_in, biases, feed_sems.at[4])
    bias_copy.start()
    bias_copy.wait()
    row = iota((32, WIDTH), 0)
    for layer in range(LAYERS):
        line = jnp.broadcast_to(biases[layer : layer + 1, :].astype(F32), (32, WIDTH))
        feeds[layer, 1024:1056, :] = jnp.where(row == 0, line, 0.0).astype(BF16)
    place = pl.ds(pl.multiple_of(side * 528, 16), 528)
    sent = []
    for copies, parts in (
        (feed_copies[:2], [(feeds.at[0, place], half_one), (feeds.at[0], feed_one)]),
        (attn_copies, [(attn, attn_two)]),
        (feed_copies[2:], [(feeds.at[1, place], half_two), (feeds.at[1], feed_two)]),
    ):
        for copy in copies:
            copy.wait()
        for source, target in parts:
            sent.append(pltpu.make_async_copy(source, target, out_sems.at[len(sent)]))
            sent[-1].start()
    for copy in sent:
        copy.wait()


def pack_first(weights):
    return pl.pallas_call(
        pack_first_kernel,
        out_shape=shape((512, 512), BF16),
        in_specs=[pl.BlockSpec(memory_space=pl.ANY)] * 4,
        out_specs=pl.BlockSpec(memory_space=pl.ANY),
        scratch_shapes=[pltpu.VMEM((512, 512), BF16), pltpu.SemaphoreType.DMA((7,))],
        name="pack_first",
    )(*weights)


def pack_rest(info, weights):
    out = [(512, 512), (1056, 512), (528, 512), (1056, 512), (528, 512)]
    return pl.pallas_call(
        pack_rest_kernel,
        out_shape=tuple(shape(dims, BF16) for dims in out),
        in_specs=[pl.BlockSpec(memory_space=pltpu.SMEM)] + [pl.BlockSpec(memory_space=pl.ANY)] * 7,
        out_specs=tuple([pl.BlockSpec(memory_space=pl.ANY)] * 5),
        scratch_shapes=[
            pltpu.VMEM((512, 512), BF16),
            pltpu.VMEM((2, 1056, 512), BF16), pltpu.VMEM((2, 512), BF16),
            pltpu.SemaphoreType.DMA((7,)), pltpu.SemaphoreType.DMA((5,)), pltpu.SemaphoreType.DMA((5,)),
        ],
        name="pack_rest",
    )(info, *weights)


def shape(dims, dtype):
    return jax.ShapeDtypeStruct(dims, dtype)


def swap(value, axis, bit):
    size = lax.axis_size(axis)
    return lax.ppermute(value, axis, [(i, i ^ bit) for i in range(size)])


def halo_swap(core, diag, far):
    return swap(core, "tensor", 1), swap(diag, "tensor", 3), swap(far, "tensor", 2)


def tie(value, *others):
    return lax.optimization_barrier((value, *others))[0]


def far_sum(index, slots, arrived, back):
    pieces, rows = back.shape[:2]
    half = [shape((pieces // 2, rows, WIDTH), BF16)] * 2
    return call(far_sum_kernel, "far_sum", half, (index, slots[0], arrived[0], back), 1)


def core_swap(slots):
    far = swap(slots[3], "tensor", 1)
    return swap(slots[1], "tensor", 1), far


def core_sum(slots, arrived):
    return call(add_kernel, "core_sum", [shape(slots[2].shape, BF16)], (slots[2], arrived[1]))[0]


class Chain:
    def __init__(self, index, stay, go):
        self.index, self.stay, self.at = index, stay, 0
        self.arriving = swap(go, "dp", 1)

    def step(self):
        rest = self.stay.shape[1:]
        pieces = self.stay.shape[0]
        if self.at == 0:
            half = shape((pieces // 2,) + rest, BF16)
            self.stay, go = call(
                functools.partial(split_sum_kernel, 1), "split_sum", [half] * 2,
                (self.index, self.stay, self.arriving), 1,
            )
            self.arriving = swap(go, "dp", 2)
        elif self.at < 3:
            self.stay = call(
                add_kernel, "add", [shape(self.stay.shape, BF16)], (self.stay, self.arriving)
            )[0]
            if self.at == 2:
                bit = PIECES
                while bit < lax.axis_size("dp"):
                    self.stay = self.stay + swap(self.stay, "dp", bit)
                    bit *= 2
            self.arriving = swap(self.stay, "dp", 4 if self.at == 1 else 2)
        else:
            self.stay = call(
                functools.partial(join_kernel, 1), "join", [shape((pieces * 2,) + rest, BF16)],
                (self.index, self.stay, self.arriving), 1,
            )[0]
            self.arriving = swap(self.stay, "dp", 1)
        self.at += 1

    def result(self):
        assert self.at == 4
        return self.stay, self.arriving


class Flow:
    def __init__(self, index, slots, arrived, back=None, halos=()):
        self.index, self.slots, self.arrived, self.halos = index, slots, arrived, halos
        self.back, self.chain, self.at = back, None, 0 if back is None else 1

    def step(self):
        if self.at == 0:
            far = core_sum(self.slots, self.arrived)
            self.back = swap(tie(far, *self.halos) if self.halos else far, "tensor", 2)
        elif self.at == 1:
            self.chain = Chain(self.index, *far_sum(self.index, self.slots, self.arrived, self.back))
        elif self.at < 6:
            self.chain.step()
        else:
            AFTER.append(self.chain.arriving)
        self.at += 1


def on_device(
    inputs, lengths, cotangent, ln_gains, ln_biases,
    w_query, w_key, w_value, w_output, w_in, b_in, w_out, b_out,
):
    assert inputs.shape == (1, ROWS, WIDTH)
    assert lax.axis_size("tensor") == SLOTS and lax.axis_size("dp") % PIECES == 0
    rank = lax.axis_index("tensor")
    position = lax.axis_index("dp")
    side = position % 2
    index = jnp.stack([side, position // 2 % 2, position // 4 % 2]).astype(jnp.int32)
    near = (rank == 1) | (rank == 2)
    length = lengths[0]
    info = jnp.stack(
        [length - rank * ROWS, 1 - rank % 2, near.astype(jnp.int32), side, rank]
    ).astype(jnp.int32)

    def later(*values):
        return [Late(value) for value in values]

    ORDER[0] = None
    AFTER.clear()
    attn_own = pack_first((w_query, w_key, w_value, w_output))
    attn_two, feed_one, feed_one_half, feed_two, feed_two_half = pack_rest(
        tie(info, attn_own), (w_query, w_key, w_value, w_output, w_in, b_in, w_out)
    )
    own_far = swap(attn_own, "tensor", 2)
    own_core = swap(attn_own, "tensor", 1)
    slots = ((attn_own,), (own_core,))
    here_f1 = swap(feed_one_half, "tensor", 2)
    core_w = [swap(tie(own, own_core), "tensor", 1) for own in (feed_one, attn_two, feed_two)]

    qkv_shapes = [
        shape((SLOTS, 512, 384), BF16),
        shape((SLOTS, 80, 256), BF16),
        shape((SLOTS, 96, 256), BF16),
        shape((SLOTS, 16, 256), BF16),
    ]
    block_f32 = shape((ROWS, WIDTH), F32)
    block_low = shape((ROWS, WIDTH), BF16)

    sums = pltpu.VMEM((ROWS, WIDTH), F32)
    tables = [
        pltpu.VMEM((3, 128, 128), F32), pltpu.VMEM((CTX, 128), BF16), pltpu.VMEM((ROWS, ROWS), BF16)
    ]

    def mix(layer, qkv, halos, stream):
        return staged(
            functools.partial(mix_kernel, layer), "mix",
            [
                shape((SLOTS, CTX, 256), BF16), block_low, block_f32, block_f32, block_low, shape((1, WIDTH), F32),
            ],
            (
                info, qkv, *halos,
                *later(stream, ln_gains, ln_biases, output_weights[layer]),
            ),
            [pltpu.VMEM((SLOTS, 512, 256), F32), sums] + tables,
        )

    def with_mix_back(layer, body, name, out, args, held, saved, qkv):
        ctx, mixed, inverse = saved
        result = staged(
            chained(body, len(args), len(out), len(held)), name,
            list(out)
            + [
                shape((SLOTS, 512, 128), BF16),
                shape((SLOTS, ROWS, 384), BF16), shape((SLOTS, 80, 256), BF16),
                shape((SLOTS, 96, 256), BF16), shape((SLOTS, 16, 256), BF16),
            ],
            (info, *args, *later(output_weights[layer], mixed, inverse, qkv, ctx)),
            list(held)
            + [
                sums, pltpu.VMEM((SLOTS, 512, 256), BF16), pltpu.VMEM((SLOTS, 512, 128), F32),
                pltpu.VMEM((SLOTS, CTX, 256), F32),
            ]
            + tables
            + [pltpu.VMEM((ROWS, ROWS), BF16), pltpu.VMEM((ROWS, 128), F32)],
        )
        return result[: len(out)], result[len(out) :]

    near_shapes = [shape((2,) + dims.shape[1:], BF16) for dims in qkv_shapes]
    normed_one, stream_one, qkv_near, *pay_near = staged(
        first_near_kernel, "first_near", [block_low, block_f32] + near_shapes,
        (tie(info, feed_one_half), inputs, ln_gains, ln_biases, qkv_plan(slots[:2])),
    )
    own_diag = tuple(
        swap(part, "tensor", 1)
        for part in (tie(own_far, normed_one)[i * 256 : i * 256 + 256] for i in range(2))
    )
    slots += ((own_far,), own_diag)
    qkv_weights, output_weights = [qkv_plan(slots)], [output_plan(slots)]
    qkv_far, *pay = staged(
        first_kernel, "first", near_shapes[:1] + qkv_shapes[1:],
        (info, normed_one, qkv_plan(slots[2:]), *pay_near),
        [pltpu.VMEM(dims.shape, BF16) for dims in near_shapes[1:]],
    )
    qkv_one = Plan(
        (qkv_near, qkv_far), (SLOTS, 512, 384),
        [(0, None, (slice(0, 2),)), (1, None, (slice(2, 4),))],
    )
    halos = halo_swap(*pay)
    there_f1 = swap(tie(here_f1, halos[0]), "dp", 1)
    diag_f1 = swap(tie(here_f1, halos[0]), "tensor", 1)
    far_a2 = swap(tie(attn_two, here_f1, *halos), "tensor", 2)
    *saved_one, middle_one, second_one, stat_a = mix(0, qkv_one, halos, stream_one)
    here_f2 = swap(tie(feed_two_half, here_f1, stat_a), "tensor", 2)
    feed_weights = [[
        feed_plan(parts)
        for parts in (
            (feed_one,), (core_w[0],), (here_f1, there_f1),
            (diag_f1, swap(tie(there_f1, stat_a), "tensor", 1)),
        )
    ]]
    hidden = shape((SLOTS // 2, ROWS, 512), BF16)
    act_near, slope_near, total_near = staged(
        feed_near_kernel, "feed_near", [hidden, hidden, block_f32],
        (info, second_one, *feed_weights[0][:2]),
    )
    slots = (
        (attn_two,), (core_w[1],), (far_a2,), (swap(tie(far_a2, total_near), "tensor", 1),)
    )
    qkv_weights.append(qkv_plan(slots))
    output_weights.append(output_plan(slots))
    act_far, slope_far, stat_b, stream, normed_two, qkv_two, *pay = staged(
        feed_kernel, "feed",
        [hidden, hidden, shape((2, WIDTH), F32), block_f32, block_low] + qkv_shapes,
        (
            info, second_one, Late(middle_one), *feed_weights[0][2:],
            *later(total_near, b_out, ln_gains, ln_biases, qkv_weights[1]),
        ),
        [sums],
    )
    act, slope = (
        Plan(
            pair, (SLOTS, ROWS, 512),
            [(0, None, (slice(0, 2),)), (1, None, (slice(2, 4),))],
        )
        for pair in ((act_near, act_far), (slope_near, slope_far))
    )
    there_f2 = swap(tie(here_f2, there_f1, stat_b), "dp", 1)
    diag_f2 = swap(tie(here_f2, there_f1, stat_b), "tensor", 1)
    halos = halo_swap(*pay)
    *saved_two, middle_two, second_two, stat_c = mix(1, qkv_two, halos, stream)

    feed_weights.append([
        feed_plan(parts)
        for parts in (
            (feed_two,), (core_w[2],), (here_f2, there_f2),
            (diag_f2, swap(tie(there_f2, stat_c), "tensor", 1)),
        )
    ])

    def grads(matrices, extra=0):
        return [shape((PIECES, 64 * matrices + extra, WIDTH), BF16)] * SLOTS

    (result, stat_d, *f2, hidden_two, small_a, grad), (output_two, local, *pay) = with_mix_back(
        1, turn_kernel, "turn",
        [block_f32, shape((2, WIDTH), F32)] + grads(2)
        + [shape((SLOTS, WIDTH), F32), shape((3, WIDTH), F32), block_f32],
        (
            second_two, Late(middle_two), *feed_weights[1][:2], *later(*feed_weights[1][2:]),
            Late(b_out), cotangent, Late(ln_gains),
        ),
        [sums] * 2 + [pltpu.VMEM((ROWS, WIDTH), BF16)], saved_two, qkv_two,
    )
    halos = halo_swap(*pay)
    core_f2 = core_swap(f2)
    back_f2 = swap(tie(core_sum(f2, core_f2), *halos), "tensor", 2)
    (*both, hidden_one, small_b, grad), (output_one, local, *pay) = with_mix_back(
        0, between_kernel, "between",
        grads(1) * 3 + [shape((SLOTS, WIDTH), F32), shape((5, WIDTH), F32), block_f32],
        (
            local, *halos, normed_two, qkv_weights[1],
            *later(
                grad, stream, ln_gains, act, slope, second_one, middle_one, *feed_weights[0], output_two
            ),
        ),
        [sums] * 2 + [pltpu.VMEM((ROWS, WIDTH), BF16), pltpu.VMEM((ROWS, 384 * SLOTS), BF16)],
        saved_one, qkv_one,
    )
    a2, f1, g1 = both[:SLOTS], both[SLOTS : 2 * SLOTS], both[2 * SLOTS :]
    pay = [tie(part, back_f2) for part in pay]
    halos = halo_swap(*pay)
    core_f1 = core_swap(f1)
    core_a2 = core_swap(a2)
    core_g1 = core_swap(g1)
    f2 = Flow(index, f2, core_f2, back_f2)
    f1 = Flow(index, f1, core_f1, halos=halos)
    a2 = Flow(index, a2, core_a2, halos=halos)
    g1 = Flow(index, g1, core_g1, halos=halos)
    for flow in (f2, g1,):
        flow.step()
    *a1, input_grad = staged(
        last_kernel, "last",
        grads(1, 8) + [block_f32],
        (
            info, local, *halos, normed_one, qkv_weights[0],
            *later(
                grad, inputs, ln_gains, output_one, stat_a, stat_b, stat_c, stat_d, small_a, small_b,
                hidden_one, hidden_two,
            ),
        ),
        [pltpu.VMEM((ROWS, 384 * SLOTS), BF16), sums],
    )
    a1 = Flow(index, a1, core_swap(a1))
    for flow in (
        f1, f2, g1, a1, f1, f2, g1, a2, a1, f1, g1, f2,
        a2, a1, f1, f2, a1, f1, a2, g1, f1, a1, a2, g1,
        f2, f1, a1, g1,
    ):
        flow.step()
    for flow in (a2, a2,):
        flow.step()
    grad_in, grad_out = staged(
        feed_result_kernel, "feed_result", [shape((2, 512, 512), F32)] * 2,
        (info, *f2.chain.result(), *f1.chain.result(), *g1.chain.result()),
    )
    for flow in (a1, a2,):
        flow.step()
    (
        grad_query, grad_key, grad_value, grad_output, grad_b_in, gains, offsets, grad_b_out, norms
    ) = staged(
        attn_result_kernel, "attn_result",
        [shape((2, 512, 128), F32)] * 3
        + [
            shape((2, 128, 512), F32), shape((2, 512), F32), shape((2, 2, 512), F32),
            shape((2, 2, 512), F32), shape((2, 512), F32), shape((1, 3 * LAYERS), F32),
        ],
        (info, *a1.chain.result(), *a2.chain.result()),
        [pltpu.VMEM((8 * PIECES, WIDTH), F32)],
    )
    return (
        result[None], input_grad[None], gains, offsets,
        grad_query, grad_key, grad_value, grad_output, grad_in, grad_b_in, grad_out,
        grad_b_out, norms.reshape(3 * LAYERS),
    )


def solution(mesh):
    return jax.shard_map(
        on_device,
        mesh=mesh,
        in_specs=(
            P("dp", "tensor", None),
            P("dp"),
            P("dp", "tensor", None),
            P(),
            P(),
            P(None, None, "tensor"),
            P(None, None, "tensor"),
            P(None, None, "tensor"),
            P(None, "tensor", None),
            P(None, None, "tensor"),
            P(None, "tensor"),
            P(None, "tensor", None),
            P(),
        ),
        out_specs=(
            P("dp", "tensor", None),
            P("dp", "tensor", None),
            P(),
            P(),
            P(None, None, "tensor"),
            P(None, None, "tensor"),
            P(None, None, "tensor"),
            P(None, "tensor", None),
            P(None, None, "tensor"),
            P(None, "tensor"),
            P(None, "tensor", None),
            P(),
            P(),
        ),
        check_vma=False,
    )
```
